8 devices in a mesh: stage: 1 (over z), data: 8 (over y, x, core).
Axes of the slice: x: 2, y: 2, z: 1, core: 2. Of those that a mesh axis runs over, the one named last changes fastest.
Arguments:
- w_master: float32 [128, 512, 512], P('stage', 'data')
- momentum: float32 [128, 512, 512], P('stage', 'data')
- grads: bfloat16 [8, 128, 512, 512], P(('stage', 'data'))
Outputs:
- output 1: float32 [128, 512, 512], P('stage', 'data')
- output 2: float32 [128, 512, 512], P('stage', 'data')
All inputs are finite; a program needn't handle non-finite values.
Results may differ from the reference program's by a relative error of at most 0.0146391.
Values are sent between devices in bfloat16 or wider.
A program may use at most 1 GiB of HBM per device.

```python
import math
import jax
import jax.numpy as jnp
from jax import lax

GROUP_SIZE = 8
NUM_MATS = 128
MAT_ROWS = 512
MAT_COLS = 512
NS_ITERS = 5

MOMENTUM_COEF = 0.95
LEARN_RATE = 0.05
WEIGHT_DECAY = 0.2
NORM_EPS = 1e-7
COEF_A = 3.4445
COEF_B = -4.7750
COEF_C = 2.0315
RMS_SCALE = 0.2 * math.sqrt(max(MAT_ROWS, MAT_COLS))


def setup_inputs(seed: int = 0, part: int = 0) -> dict:
    base_key = jax.random.fold_in(jax.random.key(seed), part)
    sub_keys = jax.random.split(base_key, 6)
    mat_shape = (NUM_MATS, MAT_ROWS, MAT_COLS)
    w_master = 0.02 * jax.random.normal(sub_keys[0], mat_shape, jnp.float32)
    noise_base = jax.random.normal(sub_keys[1], mat_shape, jnp.float32)
    low_left = jax.random.normal(sub_keys[2], (NUM_MATS, MAT_ROWS, 4), jnp.float32)
    low_right = jax.random.normal(sub_keys[3], (NUM_MATS, 4, MAT_COLS), jnp.float32)
    shared = 0.25 * jnp.einsum('mrk,mkc->mrc', low_left, low_right)
    row_scale = jax.random.uniform(sub_keys[4], (NUM_MATS, MAT_ROWS, 1), jnp.float32, 0.5, 1.5)
    momentum = row_scale * (noise_base + shared)
    grads = (jax.random.normal(sub_keys[5], (GROUP_SIZE,) + mat_shape, jnp.float32) * GROUP_SIZE ** -0.5).astype(jnp.bfloat16)
    return {'w_master': w_master, 'momentum': momentum, 'grads': grads}


def newton_schulz(x_start):
    is_tall = MAT_ROWS > MAT_COLS
    x_cur = x_start.T if is_tall else x_start
    for _ in range(NS_ITERS):
        gram_mat = jnp.dot(x_cur, x_cur.T, preferred_element_type=jnp.float32).astype(jnp.bfloat16)
        gram_sq = jnp.dot(gram_mat, gram_mat, preferred_element_type=jnp.float32)
        poly_mat = (COEF_B * gram_mat.astype(jnp.float32) + COEF_C * gram_sq).astype(jnp.bfloat16)
        poly_x = jnp.dot(poly_mat, x_cur, preferred_element_type=jnp.float32)
        x_cur = (COEF_A * x_cur.astype(jnp.float32) + poly_x).astype(jnp.bfloat16)
    return x_cur.T if is_tall else x_cur


def reference(w_master, momentum, grads):
    grad_sum = jnp.sum(grads.astype(jnp.float32), axis=0)
    mom_new = MOMENTUM_COEF * momentum + grad_sum
    frob_norm = jnp.sqrt(jnp.sum(mom_new * mom_new, axis=(1, 2)))

    def one_matrix(mat_pair):
        mom_one, norm_one = mat_pair
        x_start = (mom_one.astype(jnp.bfloat16).astype(jnp.float32) / (norm_one + NORM_EPS)).astype(jnp.bfloat16)
        return newton_schulz(x_start)

    x_ortho = lax.map(one_matrix, (mom_new, frob_norm))
    w_new = w_master - LEARN_RATE * (x_ortho.astype(jnp.float32) * RMS_SCALE + WEIGHT_DECAY * w_master)
    return w_new, mom_new
```

```python
import functools
import math

import jax
import jax.numpy as jnp
from jax import lax
from jax.experimental import pallas as pl
from jax.experimental.pallas import tpu as pltpu
from jax.sharding import PartitionSpec as P

MOMENTUM_COEF = 0.95
LEARN_RATE = 0.05
WEIGHT_DECAY = 0.2
NORM_EPS = 1e-7
COEF_A = 3.4445
COEF_B = -4.7750
COEF_C = 2.0315
NS_ITERS = 5

NDEV = 8
CHUNK = 8
HALF = 4
AHEAD = 2
SLOTS = 3
XSLOTS = 5
HOLD = 2
RSLOTS = 6
PIECES = 4
MESH = pl.DeviceIdType.MESH


def muon_kernel(
    grad, mom, w, results, raw,
    inbuf, kept, part, momb, stage, owned, nstage, owned_n, xbuf, xin, gram, poly,
    raw_s, raw_r, part_s, part_r, own_s, own_r, nrm_s, nrm_r, back_s, back_r,
    in_sem, mom_in, w_in,
):
    n_mats, rows, cols = mom.shape
    rms_scale = 0.2 * math.sqrt(max(rows * NDEV, cols))
    w_out, mom_out = results.at[0], results.at[1]
    steps = n_mats // CHUNK
    me = lax.axis_index("data")
    y, x, c = me // 4, (me // 2) % 2, me % 2
    partner = y * 4 + x * 2 + (1 - c)
    x_nbr = y * 4 + (1 - x) * 2
    y_nbr = (1 - y) * 4 + x * 2

    def remote(src, dst, send, recv, dev):
        return pltpu.make_async_remote_copy(
            src_ref=src, dst_ref=dst, send_sem=send, recv_sem=recv,
            device_id={"data": dev}, device_id_type=MESH)

    barrier = pltpu.get_barrier_semaphore()
    for r in range(1, NDEV):
        pl.semaphore_signal(barrier, inc=1, device_id={"data": (me + r) % NDEV}, device_id_type=MESH)
    pl.semaphore_wait(barrier, NDEV - 1)

    def raw_copies(k):
        a = pl.ds(k * CHUNK, HALF)
        b = pl.ds(k * CHUNK + HALF, HALF)
        out = []
        for dc in range(2):
            out.append(remote(grad.at[a, :, 1 - x, dc], raw.at[k, 0, 1 + c],
                              raw_s.at[k, 0, 1 + dc], raw_r.at[k, 0, 1 + c], x_nbr + dc))
            out.append(remote(grad.at[b, 1 - y, :, dc], raw.at[k, 1, 1 + c],
                              raw_s.at[k, 1, 1 + dc], raw_r.at[k, 1, 1 + c], y_nbr + dc))
        out.append(remote(grad.at[a, :, x, 1 - c], raw.at[k, 0, 0], raw_s.at[k, 0, 0], raw_r.at[k, 0, 0], partner))
        out.append(remote(grad.at[b, y, :, 1 - c], raw.at[k, 1, 0], raw_s.at[k, 1, 0], raw_r.at[k, 1, 0], partner))
        return out

    def raw_arrival(k, s, i):
        return pltpu.make_async_copy(raw.at[k, s, i], raw.at[k, s, i], raw_r.at[k, s, i])

    def own_copy(k, s):
        if s == 0:
            src = grad.at[pl.ds(k * CHUNK, HALF), :, x, c]
        else:
            src = grad.at[pl.ds(k * CHUNK + HALF, HALF), y, :, c]
        return pltpu.make_async_copy(src, inbuf.at[s, 0], in_sem.at[s, 0])

    def raw_load(k, s, i):
        return pltpu.make_async_copy(raw.at[k, s, i], inbuf.at[s, 1 + i], in_sem.at[s, 1 + i])

    def part_copy(k, s):
        slot = k % SLOTS
        return remote(part.at[slot, s], mom_out.at[pl.ds(k * CHUNK + s * HALF, HALF)],
                      part_s.at[slot, s], part_r.at[k, s], (y_nbr if s == 0 else x_nbr) + c)

    def mom_load(k):
        return pltpu.make_async_copy(mom.at[pl.ds(k * CHUNK, CHUNK)], momb.at[k % SLOTS], mom_in.at[k % SLOTS])

    def w_load(k):
        rng = pl.ds(k * CHUNK, CHUNK)
        return pltpu.make_async_copy(w.at[rng], w_out.at[rng], w_in.at[k])

    def own_send(k, r):
        j = (me + r) % NDEV
        slot = k % SLOTS
        return remote(stage.at[slot, j], owned.at[k % RSLOTS, pl.ds(me * rows, rows)],
                      own_s.at[slot, r], own_r.at[k, r], j)

    def nrm_send(k, r):
        j = (me + r) % NDEV
        slot = k % SLOTS
        return remote(nstage.at[slot, j], owned_n.at[k, me], nrm_s.at[slot, r], nrm_r.at[k, r], j)

    def back_send(k, r):
        j = (me + r) % NDEV
        slot = k % XSLOTS
        return remote(xbuf.at[slot, pl.ds(j * rows, rows)], xin.at[k % RSLOTS, me],
                      back_s.at[slot, r], back_r.at[k, r], j)

    def sum_chunk(k):
        slot = k % SLOTS
        for s in range(2):
            for i in range(3):
                raw_arrival(k, s, i).wait()
                raw_load(k, s, i).start()

        @pl.when(k >= SLOTS)
        def _():
            for s in range(2):
                part_copy(k - SLOTS, s).wait_send()

        for s in range(2):
            own_copy(k, s).wait()
            for i in range(3):
                raw_load(k, s, i).wait()
            keep = y if s == 0 else x

            @pl.loop(0, HALF)
            def _(m):
                def total(e):
                    v = [inbuf[s, i, m, e].astype(jnp.float32) for i in range(4)]
                    return (v[0] + v[1]) + (v[2] + v[3])

                part[slot, s, m] = total(1 - keep)
                kept[k % 2, s * HALF + m] = total(keep)

            part_copy(k, s).start()

        @pl.when(k + 1 < steps)
        def _():
            for s in range(2):
                own_copy(k + 1, s).start()
        w_load(k).start()

    def finish_chunk(k):
        slot = k % SLOTS
        mom_load(k).wait()
        for s in range(2):
            part_copy(k, s).wait_recv()

        @pl.when(k >= SLOTS)
        def _():
            for r in range(1, NDEV):
                own_send(k - SLOTS, r).wait_send()
                nrm_send(k - SLOTS, r).wait_send()

        @pl.loop(0, CHUNK)
        def _(j):
            new = MOMENTUM_COEF * momb[slot, j] + (kept[k % 2, j] + mom_out[k * CHUNK + j])
            mom_out[k * CHUNK + j] = new
            stage[slot, j] = new.astype(jnp.bfloat16)
            sq = jnp.sum(new * new, axis=0, keepdims=True)
            nstage[slot, j] = (sq[:, :128] + sq[:, 128:256]) + (sq[:, 256:384] + sq[:, 384:])

        for r in range(1, NDEV):
            own_send(k, r).start()
            nrm_send(k, r).start()
        owned[k % RSLOTS, pl.ds(pl.multiple_of(me * rows, rows), rows)] = stage[slot, me]
        owned_n[k, me] = nstage[slot, me]

        @pl.when(k + 1 < steps)
        def _():
            mom_load(k + 1).start()

    def orthogonalize(k):
        slot = k % XSLOTS

        @pl.when(k >= XSLOTS)
        def _():
            for r in range(1, NDEV):
                back_send(k - XSLOTS, r).wait_send()

        for r in range(1, NDEV):
            own_send(k, r).wait_recv()
            nrm_send(k, r).wait_recv()
        sq = jnp.sum(owned_n[k], axis=0)
        nrm = jnp.sqrt(jnp.sum(sq, axis=1, keepdims=True))
        den = nrm + NORM_EPS

        @pl.loop(0, NDEV)
        def _(i):
            blk = pl.ds(pl.multiple_of(i * rows, rows), rows)
            xbuf[slot, blk] = (owned[k % RSLOTS, blk].astype(jnp.float32) / den).astype(jnp.bfloat16)

        @pl.loop(0, NS_ITERS)
        def _(_):
            cur = xbuf[slot]
            gram[...] = lax.dot_general(cur, cur, (((1,), (1,)), ((), ())),
                                        preferred_element_type=jnp.float32).astype(jnp.bfloat16)
            g = gram[...]
            sqr = jnp.dot(g, g, preferred_element_type=jnp.float32)
            poly[...] = (COEF_B * g.astype(jnp.float32) + COEF_C * sqr).astype(jnp.bfloat16)
            px = jnp.dot(poly[...], cur, preferred_element_type=jnp.float32)
            xbuf[slot] = (COEF_A * cur.astype(jnp.float32) + px).astype(jnp.bfloat16)

        xin[k % RSLOTS, me] = xbuf[slot, pl.ds(pl.multiple_of(me * rows, rows), rows)]

    def send_back(k):
        for r in range(1, NDEV):
            back_send(k, r).start()

    def update_weights(k):
        w_load(k).wait()
        for r in range(1, NDEV):
            j = (me + NDEV - r) % NDEV
            pltpu.make_async_copy(xin.at[k % RSLOTS, j], xin.at[k % RSLOTS, j], back_r.at[k, r]).wait()

        @pl.loop(0, CHUNK)
        def _(j):
            old = w_out[k * CHUNK + j]
            step = xin[k % RSLOTS, j].astype(jnp.float32) * rms_scale
            w_out[k * CHUNK + j] = old - LEARN_RATE * (step + WEIGHT_DECAY * old)

    for k in range(AHEAD):
        for copy in raw_copies(k):
            copy.start()
    for s in range(2):
        own_copy(0, s).start()
    mom_load(0).start()

    @pl.loop(0, steps)
    def _(t):
        @pl.when(t + AHEAD < steps)
        def _():
            for copy in raw_copies(t + AHEAD):
                copy.start()

        sum_chunk(t)

        @pl.when(t >= 2 + HOLD)
        def _():
            send_back(t - 2 - HOLD)

        @pl.when(t >= 1)
        def _():
            finish_chunk(t - 1)

        @pl.when(t >= 2)
        def _():
            orthogonalize(t - 2)

        @pl.when(t >= 4 + HOLD)
        def _():
            update_weights(t - 4 - HOLD)

    last = steps - 1
    send_back(last - 3)
    finish_chunk(last)
    send_back(last - 2)
    orthogonalize(last - 1)
    send_back(last - 1)
    orthogonalize(last)
    send_back(last)

    @pl.loop(steps - 4 - HOLD, steps)
    def _(k):
        update_weights(k)

    @pl.loop(0, steps)
    def _(k):
        for copy in raw_copies(k):
            copy.wait_send()

    @pl.loop(steps - SLOTS, steps)
    def _(k):
        for s in range(2):
            part_copy(k, s).wait_send()
        for r in range(1, NDEV):
            own_send(k, r).wait_send()
            nrm_send(k, r).wait_send()

    @pl.loop(steps - XSLOTS, steps)
    def _(k):
        for r in range(1, NDEV):
            back_send(k, r).wait_send()


def write_kernel(results, w_out, mom_out, sems):
    n = w_out.shape[0] // PIECES
    copies = []
    for i in range(PIECES):
        rng = pl.ds(i * n, n)
        copies.append(pltpu.make_async_copy(results.at[0, rng], w_out.at[rng], sems.at[0, i]))
        copies.append(pltpu.make_async_copy(results.at[1, rng], mom_out.at[rng], sems.at[1, i]))
    for copy in copies:
        copy.start()
    for copy in copies:
        copy.wait()


def solution(mesh):
    row_spec = P('stage', 'data', None)
    grad_spec = P(('stage', 'data'), None, None, None)

    def local_step(w_rows, mom_rows, grad_full):
        n_mats, rows, n_cols = w_rows.shape
        n_rows = rows * NDEV
        steps = n_mats // CHUNK
        grad_view = grad_full.reshape(n_mats, 2, 2, 2, rows, n_cols)
        f32, bf16 = jnp.float32, jnp.bfloat16
        dma = pltpu.SemaphoreType.DMA
        hbm = pl.BlockSpec(memory_space=pltpu.HBM)
        vmem = pl.BlockSpec(memory_space=pltpu.VMEM)
        results, _ = pl.pallas_call(
            muon_kernel,
            name="muon_step",
            out_shape=(
                pltpu.VMEM((2, n_mats, rows, n_cols), f32),
                jax.ShapeDtypeStruct((steps, 2, 3, HALF, 2, rows, n_cols), bf16),
            ),
            in_specs=[hbm] * 3,
            out_specs=(vmem, hbm),
            scratch_shapes=[
                pltpu.VMEM((2, 4, HALF, 2, rows, n_cols), bf16),
                pltpu.VMEM((2, CHUNK, rows, n_cols), f32),
                pltpu.VMEM((SLOTS, 2, HALF, rows, n_cols), f32),
                pltpu.VMEM((SLOTS, CHUNK, rows, n_cols), f32),
                pltpu.VMEM((SLOTS, CHUNK, rows, n_cols), bf16),
                pltpu.VMEM((RSLOTS, n_rows, n_cols), bf16),
                pltpu.VMEM((SLOTS, CHUNK, 1, 128), f32),
                pltpu.VMEM((steps, NDEV, 1, 128), f32),
                pltpu.VMEM((XSLOTS, n_rows, n_cols), bf16),
                pltpu.VMEM((RSLOTS, CHUNK, rows, n_cols), bf16),
                pltpu.VMEM((n_rows, n_rows), bf16),
                pltpu.VMEM((n_rows, n_rows), bf16),
                dma((steps, 2, 3)), dma((steps, 2, 3)),
                dma((SLOTS, 2)), dma((steps, 2)),
                dma((SLOTS, NDEV)), dma((steps, NDEV)),
                dma((SLOTS, NDEV)), dma((steps, NDEV)),
                dma((XSLOTS, NDEV)), dma((steps, NDEV)),
                dma((2, 4)), dma((SLOTS,)), dma((steps,)),
            ],
            compiler_params=pltpu.CompilerParams(
                collective_id=0, has_side_effects=True, vmem_limit_bytes=31 * 2 ** 20),
        )(grad_view, mom_rows, w_rows)
        return pl.pallas_call(
            write_kernel,
            name="write_results",
            out_shape=(jax.ShapeDtypeStruct(w_rows.shape, f32), jax.ShapeDtypeStruct(w_rows.shape, f32)),
            in_specs=[vmem],
            out_specs=(hbm, hbm),
            scratch_shapes=[dma((2, PIECES))],
            compiler_params=pltpu.CompilerParams(vmem_limit_bytes=2 ** 20),
        )(results)

    return jax.shard_map(local_step, mesh=mesh, in_specs=(row_spec, row_spec, grad_spec),
                         out_specs=(row_spec, row_spec), check_vma=False)
```

```python
import functools
import math

import jax
import jax.numpy as jnp
from jax import lax
from jax.experimental import pallas as pl
from jax.experimental.pallas import tpu as pltpu
from jax.sharding import PartitionSpec as P

MOMENTUM_COEF = 0.95
LEARN_RATE = 0.05
WEIGHT_DECAY = 0.2
NORM_EPS = 1e-7
COEF_A = 3.4445
COEF_B = -4.7750
COEF_C = 2.0315
NS_ITERS = 5

NDEV = 8
CHUNK = 8
HALF = 4
AHEAD = 2
SLOTS = 3
XSLOTS = 5
HOLD = 2
RSLOTS = 6
PIECES = 16
MESH = pl.DeviceIdType.MESH


def muon_kernel(
    grad, mom, w, results, raw,
    inbuf, kept, part, momb, stage, owned, nstage, owned_n, xbuf, xin, gram, poly,
    raw_s, raw_r, part_s, part_r, own_s, own_r, nrm_s, nrm_r, back_s, back_r,
    in_sem, mom_in, w_in,
):
    n_mats, rows, cols = mom.shape
    rms_scale = 0.2 * math.sqrt(max(rows * NDEV, cols))
    w_out, mom_out = results.at[0], results.at[1]
    steps = n_mats // CHUNK
    me = lax.axis_index("data")
    y, x, c = me // 4, (me // 2) % 2, me % 2
    partner = y * 4 + x * 2 + (1 - c)
    x_nbr = y * 4 + (1 - x) * 2
    y_nbr = (1 - y) * 4 + x * 2
    diagonal = (1 - y) * 4 + (1 - x) * 2
    peers = [base + core for base in (diagonal, x_nbr, y_nbr) for core in (c, 1 - c)] + [partner]

    def remote(src, dst, send, recv, dev):
        return pltpu.make_async_remote_copy(
            src_ref=src, dst_ref=dst, send_sem=send, recv_sem=recv,
            device_id={"data": dev}, device_id_type=MESH)

    barrier = pltpu.get_barrier_semaphore()
    for peer in peers:
        pl.semaphore_signal(barrier, inc=1, device_id={"data": peer}, device_id_type=MESH)
    pl.semaphore_wait(barrier, NDEV - 1)

    def raw_copies(k):
        a = pl.ds(k * CHUNK, HALF)
        b = pl.ds(k * CHUNK + HALF, HALF)
        out = []
        for dc in range(2):
            out.append(remote(grad.at[a, :, 1 - x, dc], raw.at[k, 0, 1 + c],
                              raw_s.at[k, 0, 1 + dc], raw_r.at[k, 0, 1 + c], x_nbr + dc))
            out.append(remote(grad.at[b, 1 - y, :, dc], raw.at[k, 1, 1 + c],
                              raw_s.at[k, 1, 1 + dc], raw_r.at[k, 1, 1 + c], y_nbr + dc))
        out.append(remote(grad.at[a, :, x, 1 - c], raw.at[k, 0, 0], raw_s.at[k, 0, 0], raw_r.at[k, 0, 0], partner))
        out.append(remote(grad.at[b, y, :, 1 - c], raw.at[k, 1, 0], raw_s.at[k, 1, 0], raw_r.at[k, 1, 0], partner))
        return out

    def raw_arrival(k, s, i):
        return pltpu.make_async_copy(raw.at[k, s, i], raw.at[k, s, i], raw_r.at[k, s, i])

    def own_copy(k, s):
        if s == 0:
            src = grad.at[pl.ds(k * CHUNK, HALF), :, x, c]
        else:
            src = grad.at[pl.ds(k * CHUNK + HALF, HALF), y, :, c]
        return pltpu.make_async_copy(src, inbuf.at[s, 0], in_sem.at[s, 0])

    def raw_load(k, s, i):
        return pltpu.make_async_copy(raw.at[k, s, i], inbuf.at[s, 1 + i], in_sem.at[s, 1 + i])

    def part_copy(k, s):
        slot = k % SLOTS
        return remote(part.at[slot, s], mom_out.at[pl.ds(k * CHUNK + s * HALF, HALF)],
                      part_s.at[slot, s], part_r.at[k, s], (y_nbr if s == 0 else x_nbr) + c)

    def mom_load(k):
        return pltpu.make_async_copy(mom.at[pl.ds(k * CHUNK, CHUNK)], momb.at[k % SLOTS], mom_in.at[k % SLOTS])

    def w_load(k):
        rng = pl.ds(k * CHUNK, CHUNK)
        return pltpu.make_async_copy(w.at[rng], w_out.at[rng], w_in.at[k])

    def own_send(k, r):
        j = peers[r]
        slot = k % SLOTS
        return remote(stage.at[slot, j], owned.at[k % RSLOTS, pl.ds(me * rows, rows)],
                      own_s.at[slot, r], own_r.at[k, r], j)

    def nrm_send(k, r):
        j = peers[r]
        slot = k % SLOTS
        return remote(nstage.at[slot, j], owned_n.at[k, me], nrm_s.at[slot, r], nrm_r.at[k, r], j)

    def back_send(k, r):
        j = peers[r]
        slot = k % XSLOTS
        return remote(xbuf.at[slot, pl.ds(j * rows, rows)], xin.at[k % RSLOTS, me],
                      back_s.at[slot, r], back_r.at[k, r], j)

    def sum_chunk(k):
        slot = k % SLOTS
        for s in range(2):
            for i in range(3):
                raw_arrival(k, s, i).wait()
                raw_load(k, s, i).start()

        @pl.when(k >= SLOTS)
        def _():
            for s in range(2):
                part_copy(k - SLOTS, s).wait_send()

        for s in range(2):
            own_copy(k, s).wait()
            for i in range(3):
                raw_load(k, s, i).wait()
            keep = y if s == 0 else x

            @pl.loop(0, HALF)
            def _(m):
                def total(e):
                    v = [inbuf[s, i, m, e].astype(jnp.float32) for i in range(4)]
                    return (v[0] + v[1]) + (v[2] + v[3])

                part[slot, s, m] = total(1 - keep)
                kept[k % 2, s * HALF + m] = total(keep)

            part_copy(k, s).start()

        @pl.when(k + 1 < steps)
        def _():
            for s in range(2):
                own_copy(k + 1, s).start()
        w_load(k).start()

    def finish_chunk(k):
        slot = k % SLOTS
        mom_load(k).wait()
        for s in range(2):
            part_copy(k, s).wait_recv()

        @pl.when(k >= SLOTS)
        def _():
            for r in range(NDEV - 1):
                own_send(k - SLOTS, r).wait_send()
                nrm_send(k - SLOTS, r).wait_send()

        @pl.loop(0, CHUNK)
        def _(j):
            new = MOMENTUM_COEF * momb[slot, j] + (kept[k % 2, j] + mom_out[k * CHUNK + j])
            mom_out[k * CHUNK + j] = new
            stage[slot, j] = new.astype(jnp.bfloat16)
            sq = jnp.sum(new * new, axis=0, keepdims=True)
            nstage[slot, j] = (sq[:, :128] + sq[:, 128:256]) + (sq[:, 256:384] + sq[:, 384:])

        for r in range(NDEV - 1):
            own_send(k, r).start()
            nrm_send(k, r).start()
        owned[k % RSLOTS, pl.ds(pl.multiple_of(me * rows, rows), rows)] = stage[slot, me]
        owned_n[k, me] = nstage[slot, me]

        @pl.when(k + 1 < steps)
        def _():
            mom_load(k + 1).start()

    def orthogonalize(k):
        slot = k % XSLOTS

        @pl.when(k >= XSLOTS)
        def _():
            for r in range(NDEV - 1):
                back_send(k - XSLOTS, r).wait_send()

        for r in range(NDEV - 1):
            own_send(k, r).wait_recv()
            nrm_send(k, r).wait_recv()
        sq = jnp.sum(owned_n[k], axis=0)
        nrm = jnp.sqrt(jnp.sum(sq, axis=1, keepdims=True))
        den = nrm + NORM_EPS

        @pl.loop(0, NDEV)
        def _(i):
            blk = pl.ds(pl.multiple_of(i * rows, rows), rows)
            xbuf[slot, blk] = (owned[k % RSLOTS, blk].astype(jnp.float32) / den).astype(jnp.bfloat16)

        @pl.loop(0, NS_ITERS)
        def _(_):
            cur = xbuf[slot]
            gram[...] = lax.dot_general(cur, cur, (((1,), (1,)), ((), ())),
                                        preferred_element_type=jnp.float32).astype(jnp.bfloat16)
            g = gram[...]
            sqr = jnp.dot(g, g, preferred_element_type=jnp.float32)
            poly[...] = (COEF_B * g.astype(jnp.float32) + COEF_C * sqr).astype(jnp.bfloat16)
            px = jnp.dot(poly[...], cur, preferred_element_type=jnp.float32)
            xbuf[slot] = (COEF_A * cur.astype(jnp.float32) + px).astype(jnp.bfloat16)

        xin[k % RSLOTS, me] = xbuf[slot, pl.ds(pl.multiple_of(me * rows, rows), rows)]

    def send_back(k):
        for r in range(NDEV - 1):
            back_send(k, r).start()

    def update_weights(k):
        w_load(k).wait()
        for r in range(-1, NDEV - 1):
            j = me if r < 0 else peers[r]
            if r >= 0:
                pltpu.make_async_copy(xin.at[k % RSLOTS, j], xin.at[k % RSLOTS, j], back_r.at[k, r]).wait()
            old = w_out[k * CHUNK + j]
            step = xin[k % RSLOTS, j].astype(jnp.float32) * rms_scale
            w_out[k * CHUNK + j] = old - LEARN_RATE * (step + WEIGHT_DECAY * old)

    for k in range(AHEAD):
        for copy in raw_copies(k):
            copy.start()
    for s in range(2):
        own_copy(0, s).start()
    mom_load(0).start()

    @pl.loop(0, steps)
    def _(t):
        @pl.when(t + AHEAD < steps)
        def _():
            for copy in raw_copies(t + AHEAD):
                copy.start()

        sum_chunk(t)

        @pl.when(t >= 2 + HOLD)
        def _():
            send_back(t - 2 - HOLD)

        @pl.when(t >= 1)
        def _():
            finish_chunk(t - 1)

        @pl.when(t >= 2)
        def _():
            orthogonalize(t - 2)

        @pl.when(t >= 4 + HOLD)
        def _():
            update_weights(t - 4 - HOLD)

    last = steps - 1
    send_back(last - 3)
    finish_chunk(last)
    send_back(last - 2)
    orthogonalize(last - 1)
    send_back(last - 1)
    orthogonalize(last)
    send_back(last)

    @pl.loop(0, steps)
    def _(k):
        for copy in raw_copies(k):
            copy.wait_send()

    @pl.loop(steps - SLOTS, steps)
    def _(k):
        for s in range(2):
            part_copy(k, s).wait_send()
        for r in range(NDEV - 1):
            own_send(k, r).wait_send()
            nrm_send(k, r).wait_send()

    @pl.loop(steps - 4 - HOLD, steps)
    def _(k):
        update_weights(k)

    @pl.loop(steps - XSLOTS, steps)
    def _(k):
        for r in range(NDEV - 1):
            back_send(k, r).wait_send()


def write_kernel(results, w_out, mom_out, sems):
    n = w_out.shape[0] // PIECES
    copies = []
    for i in range(PIECES):
        rng = pl.ds(i * n, n)
        copies.append(pltpu.make_async_copy(results.at[0, rng], w_out.at[rng], sems.at[0, i]))
        copies.append(pltpu.make_async_copy(results.at[1, rng], mom_out.at[rng], sems.at[1, i]))
    for copy in copies:
        copy.start()
    for copy in copies:
        copy.wait()


def solution(mesh):
    row_spec = P('stage', 'data', None)
    grad_spec = P(('stage', 'data'), None, None, None)

    def local_step(w_rows, mom_rows, grad_full):
        n_mats, rows, n_cols = w_rows.shape
        n_rows = rows * NDEV
        steps = n_mats // CHUNK
        grad_view = grad_full.reshape(n_mats, 2, 2, 2, rows, n_cols)
        f32, bf16 = jnp.float32, jnp.bfloat16
        dma = pltpu.SemaphoreType.DMA
        hbm = pl.BlockSpec(memory_space=pltpu.HBM)
        vmem = pl.BlockSpec(memory_space=pltpu.VMEM)
        results, _ = pl.pallas_call(
            muon_kernel,
            name="muon_step",
            out_shape=(
                pltpu.VMEM((2, n_mats, rows, n_cols), f32),
                jax.ShapeDtypeStruct((steps, 2, 3, HALF, 2, rows, n_cols), bf16),
            ),
            in_specs=[hbm] * 3,
            out_specs=(vmem, hbm),
            scratch_shapes=[
                pltpu.VMEM((2, 4, HALF, 2, rows, n_cols), bf16),
                pltpu.VMEM((2, CHUNK, rows, n_cols), f32),
                pltpu.VMEM((SLOTS, 2, HALF, rows, n_cols), f32),
                pltpu.VMEM((SLOTS, CHUNK, rows, n_cols), f32),
                pltpu.VMEM((SLOTS, CHUNK, rows, n_cols), bf16),
                pltpu.VMEM((RSLOTS, n_rows, n_cols), bf16),
                pltpu.VMEM((SLOTS, CHUNK, 1, 128), f32),
                pltpu.VMEM((steps, NDEV, 1, 128), f32),
                pltpu.VMEM((XSLOTS, n_rows, n_cols), bf16),
                pltpu.VMEM((RSLOTS, CHUNK, rows, n_cols), bf16),
                pltpu.VMEM((n_rows, n_rows), bf16),
                pltpu.VMEM((n_rows, n_rows), bf16),
                dma((steps, 2, 3)), dma((steps, 2, 3)),
                dma((SLOTS, 2)), dma((steps, 2)),
                dma((SLOTS, NDEV)), dma((steps, NDEV)),
                dma((SLOTS, NDEV)), dma((steps, NDEV)),
                dma((XSLOTS, NDEV)), dma((steps, NDEV)),
                dma((2, 4)), dma((SLOTS,)), dma((steps,)),
            ],
            compiler_params=pltpu.CompilerParams(
                collective_id=0, has_side_effects=True, vmem_limit_bytes=31 * 2 ** 20),
        )(grad_view, mom_rows, w_rows)
        return pl.pallas_call(
            write_kernel,
            name="write_results",
            out_shape=(jax.ShapeDtypeStruct(w_rows.shape, f32), jax.ShapeDtypeStruct(w_rows.shape, f32)),
            in_specs=[vmem],
            out_specs=(hbm, hbm),
            scratch_shapes=[dma((2, PIECES))],
            compiler_params=pltpu.CompilerParams(vmem_limit_bytes=2 ** 20),
        )(results)

    return jax.shard_map(local_step, mesh=mesh, in_specs=(row_spec, row_spec, grad_spec),
                         out_specs=(row_spec, row_spec), check_vma=False)
```

```python
import functools
import math

import jax
import jax.numpy as jnp
from jax import lax
from jax.experimental import pallas as pl
from jax.experimental.pallas import tpu as pltpu
from jax.sharding import PartitionSpec as P

MOMENTUM_COEF = 0.95
LEARN_RATE = 0.05
WEIGHT_DECAY = 0.2
NORM_EPS = 1e-7
COEF_A = 3.4445
COEF_B = -4.7750
COEF_C = 2.0315
NS_ITERS = 5

NDEV = 8
CHUNK = 8
HALF = 4
PAIR = 2
AHEAD = 2
SLOTS = 3
XSLOTS = 5
HOLD = 2
RSLOTS = 6
PIECES = 16
MESH = pl.DeviceIdType.MESH


def muon_kernel(
    grad, mom, w, results, raw,
    inbuf, kept, part, momb, stage, owned, nstage, owned_n, xbuf, xin, gram, poly,
    raw_s, raw_r, part_s, part_r, own_s, own_r, nrm_s, nrm_r, back_s, back_r,
    in_sem, mom_in, w_in,
):
    n_mats, rows, cols = mom.shape
    rms_scale = 0.2 * math.sqrt(max(rows * NDEV, cols))
    w_out, mom_out = results.at[0], results.at[1]
    steps = n_mats // CHUNK
    me = lax.axis_index("data")
    y, x, c = me // 4, (me // 2) % 2, me % 2
    partner = y * 4 + x * 2 + (1 - c)
    x_nbr = y * 4 + (1 - x) * 2
    y_nbr = (1 - y) * 4 + x * 2
    diagonal = (1 - y) * 4 + (1 - x) * 2
    peers = [base + core for base in (diagonal, x_nbr, y_nbr) for core in (c, 1 - c)] + [partner]

    def remote(src, dst, send, recv, dev):
        return pltpu.make_async_remote_copy(
            src_ref=src, dst_ref=dst, send_sem=send, recv_sem=recv,
            device_id={"data": dev}, device_id_type=MESH)

    barrier = pltpu.get_barrier_semaphore()
    for peer in peers:
        pl.semaphore_signal(barrier, inc=1, device_id={"data": peer}, device_id_type=MESH)
    pl.semaphore_wait(barrier, NDEV - 1)

    def raw_copies(q):
        rng = pl.ds(q * PAIR, PAIR)
        out = []
        for dc in range(2):
            out.append(remote(grad.at[rng, 0, :, :, 1 - x, dc], raw.at[q, 0, 1 + c],
                              raw_s.at[q, 0, 1 + dc], raw_r.at[q, 0, 1 + c], x_nbr + dc))
            out.append(remote(grad.at[rng, 1, :, 1 - y, :, dc], raw.at[q, 1, 1 + c],
                              raw_s.at[q, 1, 1 + dc], raw_r.at[q, 1, 1 + c], y_nbr + dc))
        out.append(remote(grad.at[rng, 0, :, :, x, 1 - c], raw.at[q, 0, 0], raw_s.at[q, 0, 0], raw_r.at[q, 0, 0], partner))
        out.append(remote(grad.at[rng, 1, :, y, :, 1 - c], raw.at[q, 1, 0], raw_s.at[q, 1, 0], raw_r.at[q, 1, 0], partner))
        return out

    def raw_arrival(q, s, i):
        return pltpu.make_async_copy(raw.at[q, s, i], raw.at[q, s, i], raw_r.at[q, s, i])

    def own_copy(k, s):
        src = grad.at[k, 0, :, :, x, c] if s == 0 else grad.at[k, 1, :, y, :, c]
        return pltpu.make_async_copy(src, inbuf.at[s, 0], in_sem.at[s, 0])

    def raw_load(k, s, i):
        return pltpu.make_async_copy(raw.at[k // PAIR, s, i, k % PAIR], inbuf.at[s, 1 + i], in_sem.at[s, 1 + i])

    def part_copy(k, s):
        slot = k % SLOTS
        return remote(part.at[slot, s], mom_out.at[pl.ds(k * CHUNK + s * HALF, HALF)],
                      part_s.at[slot, s], part_r.at[k, s], (y_nbr if s == 0 else x_nbr) + c)

    def mom_load(k):
        return pltpu.make_async_copy(mom.at[pl.ds(k * CHUNK, CHUNK)], momb.at[k % SLOTS], mom_in.at[k % SLOTS])

    def w_load(k):
        rng = pl.ds(k * CHUNK, CHUNK)
        return pltpu.make_async_copy(w.at[rng], w_out.at[rng], w_in.at[k])

    def own_send(k, r):
        j = peers[r]
        slot = k % SLOTS
        return remote(stage.at[slot, j], owned.at[k % RSLOTS, pl.ds(me * rows, rows)],
                      own_s.at[slot, r], own_r.at[k, r], j)

    def nrm_send(k, r):
        j = peers[r]
        slot = k % SLOTS
        return remote(nstage.at[slot, j], owned_n.at[k, me], nrm_s.at[slot, r], nrm_r.at[k, r], j)

    def back_send(k, r):
        j = peers[r]
        slot = k % XSLOTS
        return remote(xbuf.at[slot, pl.ds(j * rows, rows)], xin.at[k % RSLOTS, me],
                      back_s.at[slot, r], back_r.at[k, r], j)

    def sum_chunk(k):
        slot = k % SLOTS
        @pl.when(k % PAIR == 0)
        def _():
            for s in range(2):
                for i in range(3):
                    raw_arrival(k // PAIR, s, i).wait()

        for s in range(2):
            for i in range(3):
                raw_load(k, s, i).start()

        @pl.when(k >= SLOTS)
        def _():
            for s in range(2):
                part_copy(k - SLOTS, s).wait_send()

        for s in range(2):
            own_copy(k, s).wait()
            for i in range(3):
                raw_load(k, s, i).wait()
            keep = y if s == 0 else x

            @pl.loop(0, HALF)
            def _(m):
                def total(e):
                    v = [inbuf[s, i, m, e].astype(jnp.float32) for i in range(4)]
                    return (v[0] + v[1]) + (v[2] + v[3])

                part[slot, s, m] = total(1 - keep)
                kept[k % 2, s * HALF + m] = total(keep)

            part_copy(k, s).start()

        @pl.when(k + 1 < steps)
        def _():
            for s in range(2):
                own_copy(k + 1, s).start()
        w_load(k).start()

    def finish_chunk(k):
        slot = k % SLOTS
        mom_load(k).wait()
        for s in range(2):
            part_copy(k, s).wait_recv()

        @pl.when(k >= SLOTS)
        def _():
            for r in range(NDEV - 1):
                own_send(k - SLOTS, r).wait_send()
                nrm_send(k - SLOTS, r).wait_send()

        @pl.loop(0, CHUNK)
        def _(j):
            new = MOMENTUM_COEF * momb[slot, j] + (kept[k % 2, j] + mom_out[k * CHUNK + j])
            mom_out[k * CHUNK + j] = new
            stage[slot, j] = new.astype(jnp.bfloat16)
            sq = jnp.sum(new * new, axis=0, keepdims=True)
            nstage[slot, j] = (sq[:, :128] + sq[:, 128:256]) + (sq[:, 256:384] + sq[:, 384:])

        for r in range(NDEV - 1):
            own_send(k, r).start()
            nrm_send(k, r).start()
        owned[k % RSLOTS, pl.ds(pl.multiple_of(me * rows, rows), rows)] = stage[slot, me]
        owned_n[k, me] = nstage[slot, me]

        @pl.when(k + 1 < steps)
        def _():
            mom_load(k + 1).start()

    def orthogonalize(k):
        slot = k % XSLOTS

        @pl.when(k >= XSLOTS)
        def _():
            for r in range(NDEV - 1):
                back_send(k - XSLOTS, r).wait_send()

        for r in range(NDEV - 1):
            own_send(k, r).wait_recv()
            nrm_send(k, r).wait_recv()
        sq = jnp.sum(owned_n[k], axis=0)
        nrm = jnp.sqrt(jnp.sum(sq, axis=1, keepdims=True))
        den = nrm + NORM_EPS

        @pl.loop(0, NDEV)
        def _(i):
            blk = pl.ds(pl.multiple_of(i * rows, rows), rows)
            xbuf[slot, blk] = (owned[k % RSLOTS, blk].astype(jnp.float32) / den).astype(jnp.bfloat16)

        @pl.loop(0, NS_ITERS)
        def _(_):
            cur = xbuf[slot]
            gram[...] = lax.dot_general(cur, cur, (((1,), (1,)), ((), ())),
                                        preferred_element_type=jnp.float32).astype(jnp.bfloat16)
            g = gram[...]
            sqr = jnp.dot(g, g, preferred_element_type=jnp.float32)
            poly[...] = (COEF_B * g.astype(jnp.float32) + COEF_C * sqr).astype(jnp.bfloat16)
            px = jnp.dot(poly[...], cur, preferred_element_type=jnp.float32)
            xbuf[slot] = (COEF_A * cur.astype(jnp.float32) + px).astype(jnp.bfloat16)

        xin[k % RSLOTS, me] = xbuf[slot, pl.ds(pl.multiple_of(me * rows, rows), rows)]

    def send_back(k):
        for r in range(NDEV - 1):
            back_send(k, r).start()

    def update_weights(k):
        w_load(k).wait()
        for r in range(-1, NDEV - 1):
            j = me if r < 0 else peers[r]
            if r >= 0:
                pltpu.make_async_copy(xin.at[k % RSLOTS, j], xin.at[k % RSLOTS, j], back_r.at[k, r]).wait()
            old = w_out[k * CHUNK + j]
            step = xin[k % RSLOTS, j].astype(jnp.float32) * rms_scale
            w_out[k * CHUNK + j] = old - LEARN_RATE * (step + WEIGHT_DECAY * old)

    for q in range(AHEAD // PAIR):
        for copy in raw_copies(q):
            copy.start()
    for s in range(2):
        own_copy(0, s).start()
    mom_load(0).start()

    @pl.loop(0, steps)
    def _(t):
        @pl.when((t % PAIR == 0) & (t + AHEAD < steps))
        def _():
            for copy in raw_copies((t + AHEAD) // PAIR):
                copy.start()

        sum_chunk(t)

        @pl.when(t >= 2 + HOLD)
        def _():
            send_back(t - 2 - HOLD)

        @pl.when(t >= 1)
        def _():
            finish_chunk(t - 1)

        @pl.when(t >= 2)
        def _():
            orthogonalize(t - 2)

        @pl.when(t >= 4 + HOLD)
        def _():
            update_weights(t - 4 - HOLD)

    last = steps - 1
    send_back(last - 3)
    finish_chunk(last)
    send_back(last - 2)
    orthogonalize(last - 1)
    send_back(last - 1)
    orthogonalize(last)
    send_back(last)

    @pl.loop(0, steps // PAIR)
    def _(q):
        for copy in raw_copies(q):
            copy.wait_send()

    @pl.loop(steps - SLOTS, steps)
    def _(k):
        for s in range(2):
            part_copy(k, s).wait_send()
        for r in range(NDEV - 1):
            own_send(k, r).wait_send()
            nrm_send(k, r).wait_send()

    @pl.loop(steps - 4 - HOLD, steps)
    def _(k):
        update_weights(k)

    @pl.loop(steps - XSLOTS, steps)
    def _(k):
        for r in range(NDEV - 1):
            back_send(k, r).wait_send()


def write_kernel(results, w_out, mom_out, sems):
    n = w_out.shape[0] // PIECES
    copies = []
    for i in range(PIECES):
        rng = pl.ds(i * n, n)
        copies.append(pltpu.make_async_copy(results.at[0, rng], w_out.at[rng], sems.at[0, i]))
        copies.append(pltpu.make_async_copy(results.at[1, rng], mom_out.at[rng], sems.at[1, i]))
    for copy in copies:
        copy.start()
    for copy in copies:
        copy.wait()


def solution(mesh):
    row_spec = P('stage', 'data', None)
    grad_spec = P(('stage', 'data'), None, None, None)

    def local_step(w_rows, mom_rows, grad_full):
        n_mats, rows, n_cols = w_rows.shape
        n_rows = rows * NDEV
        steps = n_mats // CHUNK
        grad_view = grad_full.reshape(steps, 2, HALF, 2, 2, 2, rows, n_cols)
        f32, bf16 = jnp.float32, jnp.bfloat16
        dma = pltpu.SemaphoreType.DMA
        hbm = pl.BlockSpec(memory_space=pltpu.HBM)
        vmem = pl.BlockSpec(memory_space=pltpu.VMEM)
        results, _ = pl.pallas_call(
            muon_kernel,
            name="muon_step",
            out_shape=(
                pltpu.VMEM((2, n_mats, rows, n_cols), f32),
                jax.ShapeDtypeStruct((steps // PAIR, 2, 3, PAIR, HALF, 2, rows, n_cols), bf16),
            ),
            in_specs=[hbm] * 3,
            out_specs=(vmem, hbm),
            scratch_shapes=[
                pltpu.VMEM((2, 4, HALF, 2, rows, n_cols), bf16),
                pltpu.VMEM((2, CHUNK, rows, n_cols), f32),
                pltpu.VMEM((SLOTS, 2, HALF, rows, n_cols), f32),
                pltpu.VMEM((SLOTS, CHUNK, rows, n_cols), f32),
                pltpu.VMEM((SLOTS, CHUNK, rows, n_cols), bf16),
                pltpu.VMEM((RSLOTS, n_rows, n_cols), bf16),
                pltpu.VMEM((SLOTS, CHUNK, 1, 128), f32),
                pltpu.VMEM((steps, NDEV, 1, 128), f32),
                pltpu.VMEM((XSLOTS, n_rows, n_cols), bf16),
                pltpu.VMEM((RSLOTS, CHUNK, rows, n_cols), bf16),
                pltpu.VMEM((n_rows, n_rows), bf16),
                pltpu.VMEM((n_rows, n_rows), bf16),
                dma((steps // PAIR, 2, 3)), dma((steps // PAIR, 2, 3)),
                dma((SLOTS, 2)), dma((steps, 2)),
                dma((SLOTS, NDEV)), dma((steps, NDEV)),
                dma((SLOTS, NDEV)), dma((steps, NDEV)),
                dma((XSLOTS, NDEV)), dma((steps, NDEV)),
                dma((2, 4)), dma((SLOTS,)), dma((steps,)),
            ],
            compiler_params=pltpu.CompilerParams(
                collective_id=0, has_side_effects=True, vmem_limit_bytes=31 * 2 ** 20),
        )(grad_view, mom_rows, w_rows)
        return pl.pallas_call(
            write_kernel,
            name="write_results",
            out_shape=(jax.ShapeDtypeStruct(w_rows.shape, f32), jax.ShapeDtypeStruct(w_rows.shape, f32)),
            in_specs=[vmem],
            out_specs=(hbm, hbm),
            scratch_shapes=[dma((2, PIECES))],
            compiler_params=pltpu.CompilerParams(vmem_limit_bytes=2 ** 20),
        )(results)

    return jax.shard_map(local_step, mesh=mesh, in_specs=(row_spec, row_spec, grad_spec),
                         out_specs=(row_spec, row_spec), check_vma=False)
```

```python
import functools
import math

import jax
import jax.numpy as jnp
from jax import lax
from jax.experimental import pallas as pl
from jax.experimental.pallas import tpu as pltpu
from jax.sharding import PartitionSpec as P

MOMENTUM_COEF = 0.95
LEARN_RATE = 0.05
WEIGHT_DECAY = 0.2
NORM_EPS = 1e-7
COEF_A = 3.4445
COEF_B = -4.7750
COEF_C = 2.0315
NS_ITERS = 5

NDEV = 8
CHUNK = 8
HALF = 4
PAIR = 2
AHEAD = 2
SLOTS = 3
GROUP = 2
GSLOTS = 2
OSLOTS = 2
XSLOTS = 3
RSLOTS = 3
HOLD = 2
PIECES = 16
MESH = pl.DeviceIdType.MESH


def muon_kernel(
    grad, mom, w, results, raw,
    inbuf, kept, part, momb, stage, owned, nstage, owned_n, xbuf, xin, gram, poly,
    raw_s, raw_r, part_s, part_r, own_s, own_r, nrm_s, nrm_r, back_s, back_r,
    in_sem, mom_in, w_in,
):
    n_mats, rows, cols = mom.shape
    rms_scale = 0.2 * math.sqrt(max(rows * NDEV, cols))
    w_out, mom_out = results.at[0], results.at[1]
    steps = n_mats // CHUNK
    me = lax.axis_index("data")
    y, x, c = me // 4, (me // 2) % 2, me % 2
    partner = y * 4 + x * 2 + (1 - c)
    x_nbr = y * 4 + (1 - x) * 2
    y_nbr = (1 - y) * 4 + x * 2
    diagonal = (1 - y) * 4 + (1 - x) * 2
    peers = [base + core for base in (diagonal, x_nbr, y_nbr) for core in (c, 1 - c)] + [partner]

    def remote(src, dst, send, recv, dev):
        return pltpu.make_async_remote_copy(
            src_ref=src, dst_ref=dst, send_sem=send, recv_sem=recv,
            device_id={"data": dev}, device_id_type=MESH)

    barrier = pltpu.get_barrier_semaphore()
    for peer in peers:
        pl.semaphore_signal(barrier, inc=1, device_id={"data": peer}, device_id_type=MESH)
    pl.semaphore_wait(barrier, NDEV - 1)

    def raw_copies(q):
        rng = pl.ds(q * PAIR, PAIR)
        out = []
        for dc in range(2):
            out.append(remote(grad.at[rng, 0, :, :, 1 - x, dc], raw.at[q, 0, 1 + c],
                              raw_s.at[q, 0, 1 + dc], raw_r.at[q, 0, 1 + c], x_nbr + dc))
            out.append(remote(grad.at[rng, 1, :, 1 - y, :, dc], raw.at[q, 1, 1 + c],
                              raw_s.at[q, 1, 1 + dc], raw_r.at[q, 1, 1 + c], y_nbr + dc))
        out.append(remote(grad.at[rng, 0, :, :, x, 1 - c], raw.at[q, 0, 0], raw_s.at[q, 0, 0], raw_r.at[q, 0, 0], partner))
        out.append(remote(grad.at[rng, 1, :, y, :, 1 - c], raw.at[q, 1, 0], raw_s.at[q, 1, 0], raw_r.at[q, 1, 0], partner))
        return out

    def raw_arrival(q, s, i):
        return pltpu.make_async_copy(raw.at[q, s, i], raw.at[q, s, i], raw_r.at[q, s, i])

    def own_copy(k, s):
        src = grad.at[k, 0, :, :, x, c] if s == 0 else grad.at[k, 1, :, y, :, c]
        return pltpu.make_async_copy(src, inbuf.at[s, 0], in_sem.at[s, 0])

    def raw_load(k, s, i):
        return pltpu.make_async_copy(raw.at[k // PAIR, s, i, k % PAIR], inbuf.at[s, 1 + i], in_sem.at[s, 1 + i])

    def part_copy(k, s):
        slot = k % SLOTS
        return remote(part.at[slot, s], mom_out.at[pl.ds(k * CHUNK + s * HALF, HALF)],
                      part_s.at[slot, s], part_r.at[k, s], (y_nbr if s == 0 else x_nbr) + c)

    def mom_load(k):
        return pltpu.make_async_copy(mom.at[pl.ds(k * CHUNK, CHUNK)], momb.at[k % SLOTS], mom_in.at[k % SLOTS])

    def w_load(k):
        rng = pl.ds(k * CHUNK, CHUNK)
        return pltpu.make_async_copy(w.at[rng], w_out.at[rng], w_in.at[k])

    def own_send(g, r):
        slot = g % GSLOTS
        return remote(stage.at[slot, peers[r]], owned.at[g % OSLOTS, :, pl.ds(me * rows, rows)],
                      own_s.at[slot, r], own_r.at[g, r], peers[r])

    def nrm_send(g, r):
        slot = g % GSLOTS
        return remote(nstage.at[slot, peers[r]], owned_n.at[g, me], nrm_s.at[slot, r], nrm_r.at[g, r], peers[r])

    def back_send(g, r):
        slot = g % XSLOTS
        return remote(xbuf.at[slot, :, pl.ds(peers[r] * rows, rows)], xin.at[g % RSLOTS, me],
                      back_s.at[slot, r], back_r.at[g, r], peers[r])

    def sum_chunk(k):
        slot = k % SLOTS
        @pl.when(k % PAIR == 0)
        def _():
            for s in range(2):
                for i in range(3):
                    raw_arrival(k // PAIR, s, i).wait()

        for s in range(2):
            for i in range(3):
                raw_load(k, s, i).start()

        @pl.when(k >= SLOTS)
        def _():
            for s in range(2):
                part_copy(k - SLOTS, s).wait_send()

        for s in range(2):
            own_copy(k, s).wait()
            for i in range(3):
                raw_load(k, s, i).wait()
            keep = y if s == 0 else x

            @pl.loop(0, HALF)
            def _(m):
                def total(e):
                    v = [inbuf[s, i, m, e].astype(jnp.float32) for i in range(4)]
                    return (v[0] + v[1]) + (v[2] + v[3])

                part[slot, s, m] = total(1 - keep)
                kept[k % 2, s * HALF + m] = total(keep)

            part_copy(k, s).start()

        @pl.when(k + 1 < steps)
        def _():
            for s in range(2):
                own_copy(k + 1, s).start()
        w_load(k).start()

    def finish_chunk(k):
        slot = k % SLOTS
        g, i = k // GROUP, k % GROUP
        gslot = g % GSLOTS
        mom_load(k).wait()
        for s in range(2):
            part_copy(k, s).wait_recv()

        @pl.when((i == 0) & (g >= GSLOTS))
        def _():
            for r in range(NDEV - 1):
                own_send(g - GSLOTS, r).wait_send()
                nrm_send(g - GSLOTS, r).wait_send()

        @pl.loop(0, CHUNK)
        def _(j):
            new = MOMENTUM_COEF * momb[slot, j] + (kept[k % 2, j] + mom_out[k * CHUNK + j])
            mom_out[k * CHUNK + j] = new
            stage[gslot, j, i] = new.astype(jnp.bfloat16)
            sq = jnp.sum(new * new, axis=0, keepdims=True)
            nstage[gslot, j, i] = (sq[:, :128] + sq[:, 128:256]) + (sq[:, 256:384] + sq[:, 384:])

        @pl.when(i == GROUP - 1)
        def _():
            for r in range(NDEV - 1):
                own_send(g, r).start()
                nrm_send(g, r).start()

        owned[g % OSLOTS, i, pl.ds(pl.multiple_of(me * rows, rows), rows)] = stage[gslot, me, i]
        owned_n[g, me, i] = nstage[gslot, me, i]

        @pl.when(k + 1 < steps)
        def _():
            mom_load(k + 1).start()

    def orthogonalize(g):
        slot = g % XSLOTS

        @pl.when(g >= XSLOTS)
        def _():
            for r in range(NDEV - 1):
                back_send(g - XSLOTS, r).wait_send()

        for r in range(NDEV - 1):
            own_send(g, r).wait_recv()
            nrm_send(g, r).wait_recv()

        @pl.loop(0, GROUP)
        def _(i):
            sq = owned_n[g, 0, i]
            for j in range(1, NDEV):
                sq = sq + owned_n[g, j, i]
            den = jnp.sqrt(jnp.sum(sq, axis=1, keepdims=True)) + NORM_EPS

            @pl.loop(0, NDEV)
            def _(j):
                blk = pl.ds(pl.multiple_of(j * rows, rows), rows)
                xbuf[slot, i, blk] = (owned[g % OSLOTS, i, blk].astype(jnp.float32) / den).astype(jnp.bfloat16)

            @pl.loop(0, NS_ITERS)
            def _(_):
                cur = xbuf[slot, i]
                gram[...] = lax.dot_general(cur, cur, (((1,), (1,)), ((), ())),
                                            preferred_element_type=jnp.float32).astype(jnp.bfloat16)
                gm = gram[...]
                sqr = jnp.dot(gm, gm, preferred_element_type=jnp.float32)
                poly[...] = (COEF_B * gm.astype(jnp.float32) + COEF_C * sqr).astype(jnp.bfloat16)
                px = jnp.dot(poly[...], cur, preferred_element_type=jnp.float32)
                xbuf[slot, i] = (COEF_A * cur.astype(jnp.float32) + px).astype(jnp.bfloat16)

            xin[g % RSLOTS, me, i] = xbuf[slot, i, pl.ds(pl.multiple_of(me * rows, rows), rows)]

    def send_back(g):
        for r in range(NDEV - 1):
            back_send(g, r).start()

    def update_weights(g):
        for i in range(GROUP):
            w_load(g * GROUP + i).wait()
        for r in range(-1, NDEV - 1):
            j = me if r < 0 else peers[r]
            if r >= 0:
                pltpu.make_async_copy(xin.at[g % RSLOTS, j], xin.at[g % RSLOTS, j], back_r.at[g, r]).wait()

            @pl.loop(0, GROUP)
            def _(i):
                m = (g * GROUP + i) * CHUNK + j
                old = w_out[m]
                step = xin[g % RSLOTS, j, i].astype(jnp.float32) * rms_scale
                w_out[m] = old - LEARN_RATE * (step + WEIGHT_DECAY * old)

    for q in range(AHEAD // PAIR):
        for copy in raw_copies(q):
            copy.start()
    for s in range(2):
        own_copy(0, s).start()
    mom_load(0).start()

    @pl.loop(0, steps)
    def _(t):
        @pl.when((t % PAIR == 0) & (t + AHEAD < steps))
        def _():
            for copy in raw_copies((t + AHEAD) // PAIR):
                copy.start()

        sum_chunk(t)

        def at(lag, work):
            @pl.when(((t - lag) % GROUP == 0) & (t >= lag + GROUP))
            def _():
                work((t - lag) // GROUP - 1)

        at(1 + HOLD, send_back)

        @pl.when(t >= 1)
        def _():
            finish_chunk(t - 1)

        at(1, orthogonalize)
        at(3 + HOLD, update_weights)

    groups = steps // GROUP
    finish_chunk(steps - 1)
    send_back(groups - 2)
    orthogonalize(groups - 1)
    send_back(groups - 1)

    @pl.loop(0, steps // PAIR)
    def _(q):
        for copy in raw_copies(q):
            copy.wait_send()

    @pl.loop(steps - SLOTS, steps)
    def _(k):
        for s in range(2):
            part_copy(k, s).wait_send()

    @pl.loop(groups - GSLOTS, groups)
    def _(g):
        for r in range(NDEV - 1):
            own_send(g, r).wait_send()
            nrm_send(g, r).wait_send()

    @pl.loop((steps - 1 - 3 - HOLD) // GROUP, groups)
    def _(g):
        update_weights(g)

    @pl.loop(groups - XSLOTS, groups)
    def _(g):
        for r in range(NDEV - 1):
            back_send(g, r).wait_send()


def write_kernel(results, w_out, mom_out, sems):
    n = w_out.shape[0] // PIECES
    copies = []
    for i in range(PIECES):
        rng = pl.ds(i * n, n)
        copies.append(pltpu.make_async_copy(results.at[0, rng], w_out.at[rng], sems.at[0, i]))
        copies.append(pltpu.make_async_copy(results.at[1, rng], mom_out.at[rng], sems.at[1, i]))
    for copy in copies:
        copy.start()
    for copy in copies:
        copy.wait()


def solution(mesh):
    row_spec = P('stage', 'data', None)
    grad_spec = P(('stage', 'data'), None, None, None)

    def local_step(w_rows, mom_rows, grad_full):
        n_mats, rows, n_cols = w_rows.shape
        n_rows = rows * NDEV
        steps = n_mats // CHUNK
        groups = steps // GROUP
        grad_view = grad_full.reshape(steps, 2, HALF, 2, 2, 2, rows, n_cols)
        f32, bf16 = jnp.float32, jnp.bfloat16
        dma = pltpu.SemaphoreType.DMA
        hbm = pl.BlockSpec(memory_space=pltpu.HBM)
        vmem = pl.BlockSpec(memory_space=pltpu.VMEM)
        results, _ = pl.pallas_call(
            muon_kernel,
            name="muon_step",
            out_shape=(
                pltpu.VMEM((2, n_mats, rows, n_cols), f32),
                jax.ShapeDtypeStruct((steps // PAIR, 2, 3, PAIR, HALF, 2, rows, n_cols), bf16),
            ),
            in_specs=[hbm] * 3,
            out_specs=(vmem, hbm),
            scratch_shapes=[
                pltpu.VMEM((2, 4, HALF, 2, rows, n_cols), bf16),
                pltpu.VMEM((2, CHUNK, rows, n_cols), f32),
                pltpu.VMEM((SLOTS, 2, HALF, rows, n_cols), f32),
                pltpu.VMEM((SLOTS, CHUNK, rows, n_cols), f32),
                pltpu.VMEM((GSLOTS, NDEV, GROUP, rows, n_cols), bf16),
                pltpu.VMEM((OSLOTS, GROUP, n_rows, n_cols), bf16),
                pltpu.VMEM((GSLOTS, NDEV, GROUP, 1, 128), f32),
                pltpu.VMEM((groups, NDEV, GROUP, 1, 128), f32),
                pltpu.VMEM((XSLOTS, GROUP, n_rows, n_cols), bf16),
                pltpu.VMEM((RSLOTS, NDEV, GROUP, rows, n_cols), bf16),
                pltpu.VMEM((n_rows, n_rows), bf16),
                pltpu.VMEM((n_rows, n_rows), bf16),
                dma((steps // PAIR, 2, 3)), dma((steps // PAIR, 2, 3)),
                dma((SLOTS, 2)), dma((steps, 2)),
                dma((GSLOTS, NDEV)), dma((groups, NDEV)),
                dma((GSLOTS, NDEV)), dma((groups, NDEV)),
                dma((XSLOTS, NDEV)), dma((groups, NDEV)),
                dma((2, 4)), dma((SLOTS,)), dma((steps,)),
            ],
            compiler_params=pltpu.CompilerParams(
                collective_id=0, has_side_effects=True, vmem_limit_bytes=31 * 2 ** 20),
        )(grad_view, mom_rows, w_rows)
        return pl.pallas_call(
            write_kernel,
            name="write_results",
            out_shape=(jax.ShapeDtypeStruct(w_rows.shape, f32), jax.ShapeDtypeStruct(w_rows.shape, f32)),
            in_specs=[vmem],
            out_specs=(hbm, hbm),
            scratch_shapes=[dma((2, PIECES))],
            compiler_params=pltpu.CompilerParams(vmem_limit_bytes=2 ** 20),
        )(results)

    return jax.shard_map(local_step, mesh=mesh, in_specs=(row_spec, row_spec, grad_spec),
                         out_specs=(row_spec, row_spec), check_vma=False)
```

```python
import functools
import math

import jax
import jax.numpy as jnp
from jax import lax
from jax.experimental import pallas as pl
from jax.experimental.pallas import tpu as pltpu
from jax.sharding import PartitionSpec as P

MOMENTUM_COEF = 0.95
LEARN_RATE = 0.05
WEIGHT_DECAY = 0.2
NORM_EPS = 1e-7
COEF_A = 3.4445
COEF_B = -4.7750
COEF_C = 2.0315
NS_ITERS = 5

NDEV = 8
CHUNK = 8
HALF = 4
PAIR = 2
AHEAD = 2
SLOTS = 3
GROUP = 4
GSLOTS = 2
OSLOTS = 2
XSLOTS = 2
RSLOTS = 2
HOLD = 3
PIECES = 16
MESH = pl.DeviceIdType.MESH


def muon_kernel(
    grad, mom, w, results, raw,
    inbuf, kept, part, momb, stage, owned, nstage, owned_n, xbuf, xin, gram, poly,
    raw_s, raw_r, part_s, part_r, own_s, own_r, nrm_s, nrm_r, back_s, back_r, tail_s, tail_r,
    in_sem, mom_in, w_in,
):
    n_mats, rows, cols = mom.shape
    rms_scale = 0.2 * math.sqrt(max(rows * NDEV, cols))
    w_out, mom_out = results.at[0], results.at[1]
    steps = n_mats // CHUNK
    me = lax.axis_index("data")
    y, x, c = me // 4, (me // 2) % 2, me % 2
    partner = y * 4 + x * 2 + (1 - c)
    x_nbr = y * 4 + (1 - x) * 2
    y_nbr = (1 - y) * 4 + x * 2
    diagonal = (1 - y) * 4 + (1 - x) * 2
    peers = [base + core for base in (diagonal, x_nbr, y_nbr) for core in (c, 1 - c)] + [partner]

    def remote(src, dst, send, recv, dev):
        return pltpu.make_async_remote_copy(
            src_ref=src, dst_ref=dst, send_sem=send, recv_sem=recv,
            device_id={"data": dev}, device_id_type=MESH)

    barrier = pltpu.get_barrier_semaphore()
    for peer in peers:
        pl.semaphore_signal(barrier, inc=1, device_id={"data": peer}, device_id_type=MESH)
    pl.semaphore_wait(barrier, NDEV - 1)

    def raw_copies(q):
        rng = pl.ds(q * PAIR, PAIR)
        out = []
        for dc in range(2):
            out.append(remote(grad.at[rng, 0, :, :, 1 - x, dc], raw.at[q, 0, 1 + c],
                              raw_s.at[q, 0, 1 + dc], raw_r.at[q, 0, 1 + c], x_nbr + dc))
            out.append(remote(grad.at[rng, 1, :, 1 - y, :, dc], raw.at[q, 1, 1 + c],
                              raw_s.at[q, 1, 1 + dc], raw_r.at[q, 1, 1 + c], y_nbr + dc))
        out.append(remote(grad.at[rng, 0, :, :, x, 1 - c], raw.at[q, 0, 0], raw_s.at[q, 0, 0], raw_r.at[q, 0, 0], partner))
        out.append(remote(grad.at[rng, 1, :, y, :, 1 - c], raw.at[q, 1, 0], raw_s.at[q, 1, 0], raw_r.at[q, 1, 0], partner))
        return out

    def raw_arrival(q, s, i):
        return pltpu.make_async_copy(raw.at[q, s, i], raw.at[q, s, i], raw_r.at[q, s, i])

    def own_copy(k, s):
        src = grad.at[k, 0, :, :, x, c] if s == 0 else grad.at[k, 1, :, y, :, c]
        return pltpu.make_async_copy(src, inbuf.at[s, 0], in_sem.at[s, 0])

    def raw_load(k, s, i):
        return pltpu.make_async_copy(raw.at[k // PAIR, s, i, k % PAIR], inbuf.at[s, 1 + i], in_sem.at[s, 1 + i])

    def part_copy(k, s):
        slot = k % SLOTS
        return remote(part.at[slot, s], mom_out.at[pl.ds(k * CHUNK + s * HALF, HALF)],
                      part_s.at[slot, s], part_r.at[k, s], (y_nbr if s == 0 else x_nbr) + c)

    def mom_load(k):
        return pltpu.make_async_copy(mom.at[pl.ds(k * CHUNK, CHUNK)], momb.at[k % SLOTS], mom_in.at[k % SLOTS])

    def w_load(k):
        rng = pl.ds(k * CHUNK, CHUNK)
        return pltpu.make_async_copy(w.at[rng], w_out.at[rng], w_in.at[k])

    def own_send(g, r):
        slot = g % GSLOTS
        return remote(stage.at[slot, peers[r]], owned.at[g % OSLOTS, :, pl.ds(me * rows, rows)],
                      own_s.at[slot, r], own_r.at[g, r], peers[r])

    def nrm_send(g, r):
        slot = g % GSLOTS
        return remote(nstage.at[slot, peers[r]], owned_n.at[g, me], nrm_s.at[slot, r], nrm_r.at[g, r], peers[r])

    def back_send(g, r):
        slot = g % XSLOTS
        return remote(xbuf.at[slot, :, pl.ds(peers[r] * rows, rows)], xin.at[g % RSLOTS, me],
                      back_s.at[slot, r], back_r.at[g, r], peers[r])

    def tail_send(g, i, r):
        slot = g % XSLOTS
        return remote(xbuf.at[slot, i, pl.ds(peers[r] * rows, rows)], xin.at[g % RSLOTS, me, i],
                      tail_s.at[i, r], tail_r.at[i, r], peers[r])

    def sum_chunk(k):
        slot = k % SLOTS
        @pl.when(k % PAIR == 0)
        def _():
            for s in range(2):
                for i in range(3):
                    raw_arrival(k // PAIR, s, i).wait()

        for s in range(2):
            for i in range(3):
                raw_load(k, s, i).start()

        @pl.when(k >= SLOTS)
        def _():
            for s in range(2):
                part_copy(k - SLOTS, s).wait_send()

        for s in range(2):
            own_copy(k, s).wait()
            for i in range(3):
                raw_load(k, s, i).wait()
            keep = y if s == 0 else x

            @pl.loop(0, HALF)
            def _(m):
                def total(e):
                    v = [inbuf[s, i, m, e].astype(jnp.float32) for i in range(4)]
                    return (v[0] + v[1]) + (v[2] + v[3])

                part[slot, s, m] = total(1 - keep)
                kept[k % 2, s * HALF + m] = total(keep)

            part_copy(k, s).start()

        @pl.when(k + 1 < steps)
        def _():
            for s in range(2):
                own_copy(k + 1, s).start()
        w_load(k).start()

    def finish_chunk(k):
        slot = k % SLOTS
        g, i = k // GROUP, k % GROUP
        gslot = g % GSLOTS
        mom_load(k).wait()
        for s in range(2):
            part_copy(k, s).wait_recv()

        @pl.when((i == 0) & (g >= GSLOTS))
        def _():
            for r in range(NDEV - 1):
                own_send(g - GSLOTS, r).wait_send()
                nrm_send(g - GSLOTS, r).wait_send()

        @pl.loop(0, CHUNK)
        def _(j):
            new = MOMENTUM_COEF * momb[slot, j] + (kept[k % 2, j] + mom_out[k * CHUNK + j])
            mom_out[k * CHUNK + j] = new
            stage[gslot, j, i] = new.astype(jnp.bfloat16)
            sq = jnp.sum(new * new, axis=0, keepdims=True)
            nstage[gslot, j, i] = (sq[:, :128] + sq[:, 128:256]) + (sq[:, 256:384] + sq[:, 384:])

        @pl.when(i == GROUP - 1)
        def _():
            for r in range(NDEV - 1):
                own_send(g, r).start()
                nrm_send(g, r).start()

        owned[g % OSLOTS, i, pl.ds(pl.multiple_of(me * rows, rows), rows)] = stage[gslot, me, i]
        owned_n[g, me, i] = nstage[gslot, me, i]

        @pl.when(k + 1 < steps)
        def _():
            mom_load(k + 1).start()

    def orthogonalize(g, after=lambda i: None):
        slot = g % XSLOTS

        @pl.when(g >= XSLOTS)
        def _():
            for r in range(NDEV - 1):
                back_send(g - XSLOTS, r).wait_send()

        for r in range(NDEV - 1):
            own_send(g, r).wait_recv()
            nrm_send(g, r).wait_recv()

        @pl.loop(0, GROUP)
        def _(i):
            sq = owned_n[g, 0, i]
            for j in range(1, NDEV):
                sq = sq + owned_n[g, j, i]
            den = jnp.sqrt(jnp.sum(sq, axis=1, keepdims=True)) + NORM_EPS

            @pl.loop(0, NDEV)
            def _(j):
                blk = pl.ds(pl.multiple_of(j * rows, rows), rows)
                xbuf[slot, i, blk] = (owned[g % OSLOTS, i, blk].astype(jnp.float32) / den).astype(jnp.bfloat16)

            @pl.loop(0, NS_ITERS)
            def _(_):
                cur = xbuf[slot, i]
                gram[...] = lax.dot_general(cur, cur, (((1,), (1,)), ((), ())),
                                            preferred_element_type=jnp.float32).astype(jnp.bfloat16)
                gm = gram[...]
                sqr = jnp.dot(gm, gm, preferred_element_type=jnp.float32)
                poly[...] = (COEF_B * gm.astype(jnp.float32) + COEF_C * sqr).astype(jnp.bfloat16)
                px = jnp.dot(poly[...], cur, preferred_element_type=jnp.float32)
                xbuf[slot, i] = (COEF_A * cur.astype(jnp.float32) + px).astype(jnp.bfloat16)

            after(i)
            xin[g % RSLOTS, me, i] = xbuf[slot, i, pl.ds(pl.multiple_of(me * rows, rows), rows)]

    def send_back(g, part=range(NDEV - 1)):
        for r in part:
            back_send(g, r).start()

    def update_rows(g, i, j):
        m = (g * GROUP + i) * CHUNK + j
        old = w_out[m]
        step = xin[g % RSLOTS, j, i].astype(jnp.float32) * rms_scale
        w_out[m] = old - LEARN_RATE * (step + WEIGHT_DECAY * old)

    def update_weights(g):
        for i in range(GROUP):
            w_load(g * GROUP + i).wait()
        for r in range(NDEV):
            j = peers[r] if r < NDEV - 1 else me
            if r < NDEV - 1:
                pltpu.make_async_copy(xin.at[g % RSLOTS, j], xin.at[g % RSLOTS, j], back_r.at[g, r]).wait()

            @pl.loop(0, GROUP)
            def _(i):
                update_rows(g, i, j)

    def update_last(g):
        @pl.loop(0, GROUP)
        def _(i):
            w_load(g * GROUP + i).wait()
            update_rows(g, i, me)
            for r in range(NDEV - 1):
                pltpu.make_async_copy(xin.at[g % RSLOTS, peers[r], i], xin.at[g % RSLOTS, peers[r], i],
                                      tail_r.at[i, r]).wait()
                update_rows(g, i, peers[r])

    for q in range(AHEAD // PAIR):
        for copy in raw_copies(q):
            copy.start()
    for s in range(2):
        own_copy(0, s).start()
    mom_load(0).start()

    @pl.loop(0, steps)
    def _(t):
        @pl.when((t % PAIR == 0) & (t + AHEAD < steps))
        def _():
            for copy in raw_copies((t + AHEAD) // PAIR):
                copy.start()

        sum_chunk(t)

        def at(lag, work):
            @pl.when(((t - lag) % GROUP == 0) & (t >= lag + GROUP))
            def _():
                work((t - lag) // GROUP - 1)

        at(1 + HOLD, send_back)

        @pl.when(t >= 1)
        def _():
            finish_chunk(t - 1)

        at(1, orthogonalize)
        at(3 + HOLD, update_weights)

    groups = steps // GROUP
    last = groups - 1

    def send_rows(i):
        for r in range(NDEV - 1):
            tail_send(last, i, r).start()

    if GROUP > 2:
        send_back(last - 1, range(0, NDEV - 1, 2))
    finish_chunk(steps - 1)
    send_back(last - 1, range(1, NDEV - 1, 2) if GROUP > 2 else range(NDEV - 1))
    orthogonalize(last, send_rows)

    @pl.loop(0, steps // PAIR)
    def _(q):
        for copy in raw_copies(q):
            copy.wait_send()

    @pl.loop(steps - SLOTS, steps)
    def _(k):
        for s in range(2):
            part_copy(k, s).wait_send()

    @pl.loop(groups - GSLOTS, groups)
    def _(g):
        for r in range(NDEV - 1):
            own_send(g, r).wait_send()
            nrm_send(g, r).wait_send()

    @pl.loop((steps - 1 - 3 - HOLD) // GROUP, last)
    def _(g):
        update_weights(g)

    update_last(last)

    for r in range(NDEV - 1):
        for g in range(groups - XSLOTS, last):
            back_send(g, r).wait_send()
        for i in range(GROUP):
            tail_send(last, i, r).wait_send()


def write_kernel(results, w_out, mom_out, sems):
    n = w_out.shape[0] // PIECES
    copies = []
    for i in range(PIECES):
        rng = pl.ds(i * n, n)
        copies.append(pltpu.make_async_copy(results.at[0, rng], w_out.at[rng], sems.at[0, i]))
        copies.append(pltpu.make_async_copy(results.at[1, rng], mom_out.at[rng], sems.at[1, i]))
    for copy in copies:
        copy.start()
    for copy in copies:
        copy.wait()


def solution(mesh):
    row_spec = P('stage', 'data', None)
    grad_spec = P(('stage', 'data'), None, None, None)

    def local_step(w_rows, mom_rows, grad_full):
        n_mats, rows, n_cols = w_rows.shape
        n_rows = rows * NDEV
        steps = n_mats // CHUNK
        groups = steps // GROUP
        grad_view = grad_full.reshape(steps, 2, HALF, 2, 2, 2, rows, n_cols)
        f32, bf16 = jnp.float32, jnp.bfloat16
        dma = pltpu.SemaphoreType.DMA
        hbm = pl.BlockSpec(memory_space=pltpu.HBM)
        vmem = pl.BlockSpec(memory_space=pltpu.VMEM)
        results, _ = pl.pallas_call(
            muon_kernel,
            name="muon_step",
            out_shape=(
                pltpu.VMEM((2, n_mats, rows, n_cols), f32),
                jax.ShapeDtypeStruct((steps // PAIR, 2, 3, PAIR, HALF, 2, rows, n_cols), bf16),
            ),
            in_specs=[hbm] * 3,
            out_specs=(vmem, hbm),
            scratch_shapes=[
                pltpu.VMEM((2, 4, HALF, 2, rows, n_cols), bf16),
                pltpu.VMEM((2, CHUNK, rows, n_cols), f32),
                pltpu.VMEM((SLOTS, 2, HALF, rows, n_cols), f32),
                pltpu.VMEM((SLOTS, CHUNK, rows, n_cols), f32),
                pltpu.VMEM((GSLOTS, NDEV, GROUP, rows, n_cols), bf16),
                pltpu.VMEM((OSLOTS, GROUP, n_rows, n_cols), bf16),
                pltpu.VMEM((GSLOTS, NDEV, GROUP, 1, 128), f32),
                pltpu.VMEM((groups, NDEV, GROUP, 1, 128), f32),
                pltpu.VMEM((XSLOTS, GROUP, n_rows, n_cols), bf16),
                pltpu.VMEM((RSLOTS, NDEV, GROUP, rows, n_cols), bf16),
                pltpu.VMEM((n_rows, n_rows), bf16),
                pltpu.VMEM((n_rows, n_rows), bf16),
                dma((steps // PAIR, 2, 3)), dma((steps // PAIR, 2, 3)),
                dma((SLOTS, 2)), dma((steps, 2)),
                dma((GSLOTS, NDEV)), dma((groups, NDEV)),
                dma((GSLOTS, NDEV)), dma((groups, NDEV)),
                dma((XSLOTS, NDEV)), dma((groups, NDEV)),
                dma((GROUP, NDEV)), dma((GROUP, NDEV)),
                dma((2, 4)), dma((SLOTS,)), dma((steps,)),
            ],
            compiler_params=pltpu.CompilerParams(
                collective_id=0, has_side_effects=True, vmem_limit_bytes=31 * 2 ** 20),
        )(grad_view, mom_rows, w_rows)
        return pl.pallas_call(
            write_kernel,
            name="write_results",
            out_shape=(jax.ShapeDtypeStruct(w_rows.shape, f32), jax.ShapeDtypeStruct(w_rows.shape, f32)),
            in_specs=[vmem],
            out_specs=(hbm, hbm),
            scratch_shapes=[dma((2, PIECES))],
            compiler_params=pltpu.CompilerParams(vmem_limit_bytes=2 ** 20),
        )(results)

    return jax.shard_map(local_step, mesh=mesh, in_specs=(row_spec, row_spec, grad_spec),
                         out_specs=(row_spec, row_spec), check_vma=False)
```

```python
import functools
import math

import jax
import jax.numpy as jnp
from jax import lax
from jax.experimental import pallas as pl
from jax.experimental.pallas import tpu as pltpu
from jax.sharding import PartitionSpec as P

MOMENTUM_COEF = 0.95
LEARN_RATE = 0.05
WEIGHT_DECAY = 0.2
NORM_EPS = 1e-7
COEF_A = 3.4445
COEF_B = -4.7750
COEF_C = 2.0315
NS_ITERS = 5

NDEV = 8
CHUNK = 8
HALF = 4
PAIR = 2
AHEAD = 2
SLOTS = 3
GROUP = 2
GSLOTS = 2
OSLOTS = 3
XSLOTS = 3
RSLOTS = 3
PIECES = 16
MESH = pl.DeviceIdType.MESH


def muon_kernel(
    grad, mom, w, results, raw,
    inbuf, kept, part, momb, stage, owned, nstage, owned_n, xbuf, xin, gram, poly,
    raw_s, raw_r, part_s, part_r, own_s, own_r, nrm_s, nrm_r, back_s, back_r, tail_s, tail_r,
    in_sem, mom_in, w_in,
):
    n_mats, rows, cols = mom.shape
    rms_scale = 0.2 * math.sqrt(max(rows * NDEV, cols))
    w_out, mom_out = results.at[0], results.at[1]
    steps = n_mats // CHUNK
    me = lax.axis_index("data")
    y, x, c = me // 4, (me // 2) % 2, me % 2
    partner = y * 4 + x * 2 + (1 - c)
    x_nbr = y * 4 + (1 - x) * 2
    y_nbr = (1 - y) * 4 + x * 2
    diagonal = (1 - y) * 4 + (1 - x) * 2
    peers = [base + core for base in (diagonal, x_nbr, y_nbr) for core in (c, 1 - c)] + [partner]

    def remote(src, dst, send, recv, dev):
        return pltpu.make_async_remote_copy(
            src_ref=src, dst_ref=dst, send_sem=send, recv_sem=recv,
            device_id={"data": dev}, device_id_type=MESH)

    barrier = pltpu.get_barrier_semaphore()
    for peer in peers:
        pl.semaphore_signal(barrier, inc=1, device_id={"data": peer}, device_id_type=MESH)
    pl.semaphore_wait(barrier, NDEV - 1)

    def raw_copies(q):
        rng = pl.ds(q * PAIR, PAIR)
        out = []
        for dc in range(2):
            out.append(remote(grad.at[rng, 0, :, :, 1 - x, dc], raw.at[q, 0, 1 + c],
                              raw_s.at[q, 0, 1 + dc], raw_r.at[q, 0, 1 + c], x_nbr + dc))
            out.append(remote(grad.at[rng, 1, :, 1 - y, :, dc], raw.at[q, 1, 1 + c],
                              raw_s.at[q, 1, 1 + dc], raw_r.at[q, 1, 1 + c], y_nbr + dc))
        out.append(remote(grad.at[rng, 0, :, :, x, 1 - c], raw.at[q, 0, 0], raw_s.at[q, 0, 0], raw_r.at[q, 0, 0], partner))
        out.append(remote(grad.at[rng, 1, :, y, :, 1 - c], raw.at[q, 1, 0], raw_s.at[q, 1, 0], raw_r.at[q, 1, 0], partner))
        return out

    def raw_arrival(q, s, i):
        return pltpu.make_async_copy(raw.at[q, s, i], raw.at[q, s, i], raw_r.at[q, s, i])

    def own_copy(k, s):
        src = grad.at[k, 0, :, :, x, c] if s == 0 else grad.at[k, 1, :, y, :, c]
        return pltpu.make_async_copy(src, inbuf.at[s, 0], in_sem.at[s, 0])

    def raw_load(k, s, i):
        return pltpu.make_async_copy(raw.at[k // PAIR, s, i, k % PAIR], inbuf.at[s, 1 + i], in_sem.at[s, 1 + i])

    def part_copy(k, s):
        slot = k % SLOTS
        return remote(part.at[slot, s], mom_out.at[pl.ds(k * CHUNK + s * HALF, HALF)],
                      part_s.at[slot, s], part_r.at[k, s], (y_nbr if s == 0 else x_nbr) + c)

    def mom_load(k):
        return pltpu.make_async_copy(mom.at[pl.ds(k * CHUNK, CHUNK)], momb.at[k % SLOTS], mom_in.at[k % SLOTS])

    def w_load(k):
        rng = pl.ds(k * CHUNK, CHUNK)
        return pltpu.make_async_copy(w.at[rng], w_out.at[rng], w_in.at[k])

    def own_send(g, r):
        slot = g % GSLOTS
        return remote(stage.at[slot, peers[r]], owned.at[g % OSLOTS, :, pl.ds(me * rows, rows)],
                      own_s.at[slot, r], own_r.at[g, r], peers[r])

    def nrm_send(g, r):
        slot = g % GSLOTS
        return remote(nstage.at[slot, peers[r]], owned_n.at[g, me], nrm_s.at[slot, r], nrm_r.at[g, r], peers[r])

    def back_send(g, r):
        slot = g % XSLOTS
        return remote(xbuf.at[slot, :, pl.ds(peers[r] * rows, rows)], xin.at[g % RSLOTS, me],
                      back_s.at[slot, r], back_r.at[g, r], peers[r])

    def tail_send(g, i, r):
        slot = g % XSLOTS
        return remote(xbuf.at[slot, i, pl.ds(peers[r] * rows, rows)], xin.at[g % RSLOTS, me, i],
                      tail_s.at[i, r], tail_r.at[i, r], peers[r])

    def sum_chunk(k):
        slot = k % SLOTS
        @pl.when(k % PAIR == 0)
        def _():
            for s in range(2):
                for i in range(3):
                    raw_arrival(k // PAIR, s, i).wait()

        for s in range(2):
            for i in range(3):
                raw_load(k, s, i).start()

        @pl.when(k >= SLOTS)
        def _():
            for s in range(2):
                part_copy(k - SLOTS, s).wait_send()

        for s in range(2):
            own_copy(k, s).wait()
            for i in range(3):
                raw_load(k, s, i).wait()
            keep = y if s == 0 else x

            @pl.loop(0, HALF)
            def _(m):
                def total(e):
                    v = [inbuf[s, i, m, e].astype(jnp.float32) for i in range(4)]
                    return (v[0] + v[1]) + (v[2] + v[3])

                part[slot, s, m] = total(1 - keep)
                kept[k % 2, s * HALF + m] = total(keep)

            part_copy(k, s).start()

        @pl.when(k + 1 < steps)
        def _():
            for s in range(2):
                own_copy(k + 1, s).start()
        w_load(k).start()

    def finish_chunk(k):
        slot = k % SLOTS
        g, i = k // GROUP, k % GROUP
        gslot = g % GSLOTS
        mom_load(k).wait()
        for s in range(2):
            part_copy(k, s).wait_recv()

        @pl.when((i == 0) & (g >= GSLOTS))
        def _():
            for r in range(NDEV - 1):
                own_send(g - GSLOTS, r).wait_send()
                nrm_send(g - GSLOTS, r).wait_send()

        @pl.loop(0, CHUNK)
        def _(j):
            new = MOMENTUM_COEF * momb[slot, j] + (kept[k % 2, j] + mom_out[k * CHUNK + j])
            mom_out[k * CHUNK + j] = new
            stage[gslot, j, i] = new.astype(jnp.bfloat16)
            sq = jnp.sum(new * new, axis=0, keepdims=True)
            nstage[gslot, j, i] = (sq[:, :128] + sq[:, 128:256]) + (sq[:, 256:384] + sq[:, 384:])

        @pl.when(i == GROUP - 1)
        def _():
            for r in range(NDEV - 1):
                own_send(g, r).start()
                nrm_send(g, r).start()

        owned[g % OSLOTS, i, pl.ds(pl.multiple_of(me * rows, rows), rows)] = stage[gslot, me, i]
        owned_n[g, me, i] = nstage[gslot, me, i]

        @pl.when(k + 1 < steps)
        def _():
            mom_load(k + 1).start()

    def owned_arrival(g):
        @pl.when(g >= XSLOTS)
        def _():
            for r in range(NDEV - 1):
                back_send(g - XSLOTS, r).wait_send()

        for r in range(NDEV - 1):
            own_send(g, r).wait_recv()
            nrm_send(g, r).wait_recv()

    def orthogonalize(g, i):
        slot = g % XSLOTS
        sq = owned_n[g, 0, i]
        for j in range(1, NDEV):
            sq = sq + owned_n[g, j, i]
        den = jnp.sqrt(jnp.sum(sq, axis=1, keepdims=True)) + NORM_EPS

        @pl.loop(0, NDEV)
        def _(j):
            blk = pl.ds(pl.multiple_of(j * rows, rows), rows)
            xbuf[slot, i, blk] = (owned[g % OSLOTS, i, blk].astype(jnp.float32) / den).astype(jnp.bfloat16)

        @pl.loop(0, NS_ITERS)
        def _(_):
            cur = xbuf[slot, i]
            gram[...] = lax.dot_general(cur, cur, (((1,), (1,)), ((), ())),
                                        preferred_element_type=jnp.float32).astype(jnp.bfloat16)
            gm = gram[...]
            sqr = jnp.dot(gm, gm, preferred_element_type=jnp.float32)
            poly[...] = (COEF_B * gm.astype(jnp.float32) + COEF_C * sqr).astype(jnp.bfloat16)
            px = jnp.dot(poly[...], cur, preferred_element_type=jnp.float32)
            xbuf[slot, i] = (COEF_A * cur.astype(jnp.float32) + px).astype(jnp.bfloat16)

        xin[g % RSLOTS, me, i] = xbuf[slot, i, pl.ds(pl.multiple_of(me * rows, rows), rows)]

    def send_back(g):
        for r in range(NDEV - 1):
            back_send(g, r).start()

    def update_rows(g, i, j):
        m = (g * GROUP + i) * CHUNK + j
        old = w_out[m]
        step = xin[g % RSLOTS, j, i].astype(jnp.float32) * rms_scale
        w_out[m] = old - LEARN_RATE * (step + WEIGHT_DECAY * old)

    def update_weights(g):
        for i in range(GROUP):
            w_load(g * GROUP + i).wait()
        for r in range(NDEV):
            j = peers[r] if r < NDEV - 1 else me
            if r < NDEV - 1:
                pltpu.make_async_copy(xin.at[g % RSLOTS, j], xin.at[g % RSLOTS, j], back_r.at[g, r]).wait()

            @pl.loop(0, GROUP)
            def _(i):
                update_rows(g, i, j)

    def update_last(g):
        @pl.loop(0, GROUP)
        def _(i):
            w_load(g * GROUP + i).wait()
            update_rows(g, i, me)
            for r in range(NDEV - 1):
                pltpu.make_async_copy(xin.at[g % RSLOTS, peers[r], i], xin.at[g % RSLOTS, peers[r], i],
                                      tail_r.at[i, r]).wait()
                update_rows(g, i, peers[r])

    for q in range(AHEAD // PAIR):
        for copy in raw_copies(q):
            copy.start()
    for s in range(2):
        own_copy(0, s).start()
    mom_load(0).start()

    @pl.loop(0, steps)
    def _(t):
        @pl.when((t % PAIR == 0) & (t + AHEAD < steps))
        def _():
            for copy in raw_copies((t + AHEAD) // PAIR):
                copy.start()

        sum_chunk(t)

        def at(lag, work):
            @pl.when(((t - lag) % GROUP == 0) & (t >= lag + GROUP))
            def _():
                work((t - lag) // GROUP - 1)

        at(1 + GROUP, send_back)

        @pl.when(t >= 1)
        def _():
            finish_chunk(t - 1)

        at(1, owned_arrival)

        @pl.when(t >= 1 + GROUP)
        def _():
            orthogonalize((t - 1) // GROUP - 1, (t - 1) % GROUP)

        at(3 + GROUP, update_weights)

    groups = steps // GROUP
    last = groups - 1
    finish_chunk(steps - 1)

    @pl.loop(GROUP - 1, 2 * GROUP)
    def _(n):
        @pl.when(n == GROUP)
        def _():
            send_back(last - 1)
            owned_arrival(last)

        orthogonalize(last - 1 + n // GROUP, n % GROUP)

        @pl.when(n >= GROUP)
        def _():
            for r in range(NDEV - 1):
                tail_send(last, n - GROUP, r).start()

    @pl.loop(0, steps // PAIR)
    def _(q):
        for copy in raw_copies(q):
            copy.wait_send()

    @pl.loop(steps - SLOTS, steps)
    def _(k):
        for s in range(2):
            part_copy(k, s).wait_send()

    @pl.loop(groups - GSLOTS, groups)
    def _(g):
        for r in range(NDEV - 1):
            own_send(g, r).wait_send()
            nrm_send(g, r).wait_send()

    @pl.loop((steps - 4 - GROUP) // GROUP, last)
    def _(g):
        update_weights(g)

    update_last(last)

    for r in range(NDEV - 1):
        for g in range(groups - XSLOTS, last):
            back_send(g, r).wait_send()
        for i in range(GROUP):
            tail_send(last, i, r).wait_send()


def write_kernel(results, w_out, mom_out, sems):
    n = w_out.shape[0] // PIECES
    copies = []
    for i in range(PIECES):
        rng = pl.ds(i * n, n)
        copies.append(pltpu.make_async_copy(results.at[0, rng], w_out.at[rng], sems.at[0, i]))
        copies.append(pltpu.make_async_copy(results.at[1, rng], mom_out.at[rng], sems.at[1, i]))
    for copy in copies:
        copy.start()
    for copy in copies:
        copy.wait()


def solution(mesh):
    row_spec = P('stage', 'data', None)
    grad_spec = P(('stage', 'data'), None, None, None)

    def local_step(w_rows, mom_rows, grad_full):
        n_mats, rows, n_cols = w_rows.shape
        n_rows = rows * NDEV
        steps = n_mats // CHUNK
        groups = steps // GROUP
        grad_view = grad_full.reshape(steps, 2, HALF, 2, 2, 2, rows, n_cols)
        f32, bf16 = jnp.float32, jnp.bfloat16
        dma = pltpu.SemaphoreType.DMA
        hbm = pl.BlockSpec(memory_space=pltpu.HBM)
        vmem = pl.BlockSpec(memory_space=pltpu.VMEM)
        results, _ = pl.pallas_call(
            muon_kernel,
            name="muon_step",
            out_shape=(
                pltpu.VMEM((2, n_mats, rows, n_cols), f32),
                jax.ShapeDtypeStruct((steps // PAIR, 2, 3, PAIR, HALF, 2, rows, n_cols), bf16),
            ),
            in_specs=[hbm] * 3,
            out_specs=(vmem, hbm),
            scratch_shapes=[
                pltpu.VMEM((2, 4, HALF, 2, rows, n_cols), bf16),
                pltpu.VMEM((2, CHUNK, rows, n_cols), f32),
                pltpu.VMEM((SLOTS, 2, HALF, rows, n_cols), f32),
                pltpu.VMEM((SLOTS, CHUNK, rows, n_cols), f32),
                pltpu.VMEM((GSLOTS, NDEV, GROUP, rows, n_cols), bf16),
                pltpu.VMEM((OSLOTS, GROUP, n_rows, n_cols), bf16),
                pltpu.VMEM((GSLOTS, NDEV, GROUP, 1, 128), f32),
                pltpu.VMEM((groups, NDEV, GROUP, 1, 128), f32),
                pltpu.VMEM((XSLOTS, GROUP, n_rows, n_cols), bf16),
                pltpu.VMEM((RSLOTS, NDEV, GROUP, rows, n_cols), bf16),
                pltpu.VMEM((n_rows, n_rows), bf16),
                pltpu.VMEM((n_rows, n_rows), bf16),
                dma((steps // PAIR, 2, 3)), dma((steps // PAIR, 2, 3)),
                dma((SLOTS, 2)), dma((steps, 2)),
                dma((GSLOTS, NDEV)), dma((groups, NDEV)),
                dma((GSLOTS, NDEV)), dma((groups, NDEV)),
                dma((XSLOTS, NDEV)), dma((groups, NDEV)),
                dma((GROUP, NDEV)), dma((GROUP, NDEV)),
                dma((2, 4)), dma((SLOTS,)), dma((steps,)),
            ],
            compiler_params=pltpu.CompilerParams(
                collective_id=0, has_side_effects=True, vmem_limit_bytes=31 * 2 ** 20),
        )(grad_view, mom_rows, w_rows)
        return pl.pallas_call(
            write_kernel,
            name="write_results",
            out_shape=(jax.ShapeDtypeStruct(w_rows.shape, f32), jax.ShapeDtypeStruct(w_rows.shape, f32)),
            in_specs=[vmem],
            out_specs=(hbm, hbm),
            scratch_shapes=[dma((2, PIECES))],
            compiler_params=pltpu.CompilerParams(vmem_limit_bytes=2 ** 20),
        )(results)

    return jax.shard_map(local_step, mesh=mesh, in_specs=(row_spec, row_spec, grad_spec),
                         out_specs=(row_spec, row_spec), check_vma=False)
```

```python
import functools
import math

import jax
import jax.numpy as jnp
from jax import lax
from jax.experimental import pallas as pl
from jax.experimental.pallas import tpu as pltpu
from jax.sharding import PartitionSpec as P

MOMENTUM_COEF = 0.95
LEARN_RATE = 0.05
WEIGHT_DECAY = 0.2
NORM_EPS = 1e-7
COEF_A = 3.4445
COEF_B = -4.7750
COEF_C = 2.0315
NS_ITERS = 5

NDEV = 8
CHUNK = 8
HALF = 4
PAIR = 2
AHEAD = 2
SLOTS = 3
GROUP = 2
GSLOTS = 2
OSLOTS = 3
XSLOTS = 3
RSLOTS = 3
PIECES = 4
MESH = pl.DeviceIdType.MESH


def muon_kernel(
    grad, mom, w, results, raw,
    inbuf, kept, part, momb, stage, swap, owned, nstage, nswap, owned_n, xbuf, xin, gram, poly,
    raw_s, raw_r, part_s, part_r, swap_s, swap_r, own_s, own_r, nrm_s, nrm_r, back_s, back_r, tail_s, tail_r,
    in_sem, mom_in, w_in,
):
    n_mats, rows, cols = mom.shape
    rms_scale = 0.2 * math.sqrt(max(rows * NDEV, cols))
    w_out, mom_out = results.at[0], results.at[1]
    steps = n_mats // CHUNK
    me = lax.axis_index("data")
    y, x, c = me // 4, (me // 2) % 2, me % 2
    partner = y * 4 + x * 2 + (1 - c)
    x_nbr = y * 4 + (1 - x) * 2
    y_nbr = (1 - y) * 4 + x * 2
    diagonal = (1 - y) * 4 + (1 - x) * 2
    peers = [base + core for base in (diagonal, x_nbr, y_nbr) for core in (c, 1 - c)] + [partner]

    chip = me // 2
    chips = [base // 2 for base in (diagonal, x_nbr, y_nbr)]

    def remote(src, dst, send, recv, dev):
        return pltpu.make_async_remote_copy(
            src_ref=src, dst_ref=dst, send_sem=send, recv_sem=recv,
            device_id={"data": dev}, device_id_type=MESH)

    barrier = pltpu.get_barrier_semaphore()
    for peer in peers:
        pl.semaphore_signal(barrier, inc=1, device_id={"data": peer}, device_id_type=MESH)
    pl.semaphore_wait(barrier, NDEV - 1)

    def raw_copies(q):
        rng = pl.ds(q * PAIR, PAIR)
        out = []
        for dc in range(2):
            out.append(remote(grad.at[rng, 0, :, :, 1 - x, dc], raw.at[q, 0, 1 + c],
                              raw_s.at[q, 0, 1 + dc], raw_r.at[q, 0, 1 + c], x_nbr + dc))
            out.append(remote(grad.at[rng, 1, :, 1 - y, :, dc], raw.at[q, 1, 1 + c],
                              raw_s.at[q, 1, 1 + dc], raw_r.at[q, 1, 1 + c], y_nbr + dc))
        out.append(remote(grad.at[rng, 0, :, :, x, 1 - c], raw.at[q, 0, 0], raw_s.at[q, 0, 0], raw_r.at[q, 0, 0], partner))
        out.append(remote(grad.at[rng, 1, :, y, :, 1 - c], raw.at[q, 1, 0], raw_s.at[q, 1, 0], raw_r.at[q, 1, 0], partner))
        return out

    def raw_arrival(q, s, i):
        return pltpu.make_async_copy(raw.at[q, s, i], raw.at[q, s, i], raw_r.at[q, s, i])

    def own_copy(k, s):
        src = grad.at[k, 0, :, :, x, c] if s == 0 else grad.at[k, 1, :, y, :, c]
        return pltpu.make_async_copy(src, inbuf.at[s, 0], in_sem.at[s, 0])

    def raw_load(k, s, i):
        return pltpu.make_async_copy(raw.at[k // PAIR, s, i, k % PAIR], inbuf.at[s, 1 + i], in_sem.at[s, 1 + i])

    def part_copy(k, s):
        slot = k % SLOTS
        return remote(part.at[slot, s], mom_out.at[pl.ds(k * CHUNK + s * HALF, HALF)],
                      part_s.at[slot, s], part_r.at[k, s], (y_nbr if s == 0 else x_nbr) + c)

    def mom_load(k):
        return pltpu.make_async_copy(mom.at[pl.ds(k * CHUNK, CHUNK)], momb.at[k % SLOTS], mom_in.at[k % SLOTS])

    def w_load(k):
        rng = pl.ds(k * CHUNK, CHUNK)
        return pltpu.make_async_copy(w.at[rng], w_out.at[rng], w_in.at[k])

    def swap_copies(g):
        slot = g % GSLOTS
        return [remote(swap, stage.at[slot, :, c], swap_s.at[0], swap_r.at[g, 0], partner),
                remote(nswap, nstage.at[slot, :, c], swap_s.at[1], swap_r.at[g, 1], partner)]

    def own_send(g, r):
        slot = g % GSLOTS
        return remote(stage.at[slot, chips[r]], owned.at[g % OSLOTS, pl.ds(chip * 2, 2)],
                      own_s.at[slot, r], own_r.at[g, r], chips[r] * 2 + c)

    def nrm_send(g, r):
        slot = g % GSLOTS
        return remote(nstage.at[slot, chips[r]], owned_n.at[g, pl.ds(chip * 2, 2)],
                      nrm_s.at[slot, r], nrm_r.at[g, r], chips[r] * 2 + c)

    def back_send(g, r):
        slot = g % XSLOTS
        return remote(xbuf.at[slot, :, pl.ds(peers[r] * rows, rows)], xin.at[g % RSLOTS, me],
                      back_s.at[slot, r], back_r.at[g, r], peers[r])

    def tail_send(g, i, r):
        slot = g % XSLOTS
        return remote(xbuf.at[slot, i, pl.ds(peers[r] * rows, rows)], xin.at[g % RSLOTS, me, i],
                      tail_s.at[i, r], tail_r.at[i, r], peers[r])

    def sum_chunk(k):
        slot = k % SLOTS
        @pl.when(k % PAIR == 0)
        def _():
            for s in range(2):
                for i in range(3):
                    raw_arrival(k // PAIR, s, i).wait()

        for s in range(2):
            for i in range(3):
                raw_load(k, s, i).start()

        @pl.when(k >= SLOTS)
        def _():
            for s in range(2):
                part_copy(k - SLOTS, s).wait_send()

        for s in range(2):
            own_copy(k, s).wait()
            for i in range(3):
                raw_load(k, s, i).wait()
            keep = y if s == 0 else x

            @pl.loop(0, HALF)
            def _(m):
                def total(e):
                    v = [inbuf[s, i, m, e].astype(jnp.float32) for i in range(4)]
                    return (v[0] + v[1]) + (v[2] + v[3])

                part[slot, s, m] = total(1 - keep)
                kept[k % 2, s * HALF + m] = total(keep)

            part_copy(k, s).start()

        @pl.when(k + 1 < steps)
        def _():
            for s in range(2):
                own_copy(k + 1, s).start()
        w_load(k).start()

    def finish_chunk(k):
        slot = k % SLOTS
        g, i = k // GROUP, k % GROUP
        gslot = g % GSLOTS
        mom_load(k).wait()
        for s in range(2):
            part_copy(k, s).wait_recv()

        def momentum(j):
            new = MOMENTUM_COEF * momb[slot, j] + (kept[k % 2, j] + mom_out[k * CHUNK + j])
            mom_out[k * CHUNK + j] = new
            sq = jnp.sum(new * new, axis=0, keepdims=True)
            return new.astype(jnp.bfloat16), (sq[:, :128] + sq[:, 128:256]) + (sq[:, 256:384] + sq[:, 384:])

        @pl.loop(0, NDEV // 2)
        def _(q):
            stage[gslot, q, c, i], nstage[gslot, q, c, i] = momentum(2 * q + c)
            swap[q, i], nswap[q, i] = momentum(2 * q + 1 - c)

        @pl.when(i == GROUP - 1)
        def _():
            @pl.when(g >= 1)
            def _():
                for r in range(3):
                    own_send(g - 1, r).wait_send()
                    nrm_send(g - 1, r).wait_send()

            for copy in swap_copies(g):
                copy.start()
            for copy in swap_copies(g):
                copy.wait()
            for r in range(3):
                own_send(g, r).start()
                nrm_send(g, r).start()

            @pl.loop(0, GROUP)
            def _(n):
                for core in range(2):
                    owned[g % OSLOTS, chip * 2 + core, n] = stage[gslot, chip, core, n]
                    owned_n[g, chip * 2 + core, n] = nstage[gslot, chip, core, n]

        @pl.when(k + 1 < steps)
        def _():
            mom_load(k + 1).start()

    def owned_arrival(g):
        @pl.when(g >= XSLOTS)
        def _():
            for r in range(NDEV - 1):
                back_send(g - XSLOTS, r).wait_send()

        for r in range(3):
            own_send(g, r).wait_recv()
            nrm_send(g, r).wait_recv()

    def orthogonalize(g, i):
        slot = g % XSLOTS
        sq = owned_n[g, 0, i]
        for j in range(1, NDEV):
            sq = sq + owned_n[g, j, i]
        den = jnp.sqrt(jnp.sum(sq, axis=1, keepdims=True)) + NORM_EPS

        @pl.loop(0, NDEV)
        def _(j):
            blk = pl.ds(pl.multiple_of(j * rows, rows), rows)
            xbuf[slot, i, blk] = (owned[g % OSLOTS, j, i].astype(jnp.float32) / den).astype(jnp.bfloat16)

        @pl.loop(0, NS_ITERS)
        def _(_):
            cur = xbuf[slot, i]
            gram[...] = lax.dot_general(cur, cur, (((1,), (1,)), ((), ())),
                                        preferred_element_type=jnp.float32).astype(jnp.bfloat16)
            gm = gram[...]
            sqr = jnp.dot(gm, gm, preferred_element_type=jnp.float32)
            poly[...] = (COEF_B * gm.astype(jnp.float32) + COEF_C * sqr).astype(jnp.bfloat16)
            px = jnp.dot(poly[...], cur, preferred_element_type=jnp.float32)
            xbuf[slot, i] = (COEF_A * cur.astype(jnp.float32) + px).astype(jnp.bfloat16)

        xin[g % RSLOTS, me, i] = xbuf[slot, i, pl.ds(pl.multiple_of(me * rows, rows), rows)]

    def send_back(g):
        for r in range(NDEV - 1):
            back_send(g, r).start()

    def update_rows(g, i, j):
        m = (g * GROUP + i) * CHUNK + j
        old = w_out[m]
        step = xin[g % RSLOTS, j, i].astype(jnp.float32) * rms_scale
        w_out[m] = old - LEARN_RATE * (step + WEIGHT_DECAY * old)

    def update_weights(g):
        for i in range(GROUP):
            w_load(g * GROUP + i).wait()
        for r in range(NDEV):
            j = peers[r] if r < NDEV - 1 else me
            if r < NDEV - 1:
                pltpu.make_async_copy(xin.at[g % RSLOTS, j], xin.at[g % RSLOTS, j], back_r.at[g, r]).wait()

            @pl.loop(0, GROUP)
            def _(i):
                update_rows(g, i, j)

    def update_last(g):
        @pl.loop(0, GROUP)
        def _(i):
            w_load(g * GROUP + i).wait()
            update_rows(g, i, me)
            for r in range(NDEV - 1):
                pltpu.make_async_copy(xin.at[g % RSLOTS, peers[r], i], xin.at[g % RSLOTS, peers[r], i],
                                      tail_r.at[i, r]).wait()
                update_rows(g, i, peers[r])

    for q in range(AHEAD // PAIR):
        for copy in raw_copies(q):
            copy.start()
    for s in range(2):
        own_copy(0, s).start()
    mom_load(0).start()

    @pl.loop(0, steps)
    def _(t):
        @pl.when((t % PAIR == 0) & (t + AHEAD < steps))
        def _():
            for copy in raw_copies((t + AHEAD) // PAIR):
                copy.start()

        sum_chunk(t)

        def at(lag, work):
            @pl.when(((t - lag) % GROUP == 0) & (t >= lag + GROUP))
            def _():
                work((t - lag) // GROUP - 1)

        at(1 + GROUP, send_back)

        @pl.when(t >= 1)
        def _():
            finish_chunk(t - 1)

        at(1, owned_arrival)

        @pl.when(t >= 1 + GROUP)
        def _():
            orthogonalize((t - 1) // GROUP - 1, (t - 1) % GROUP)

        at(3 + GROUP, update_weights)

    groups = steps // GROUP
    last = groups - 1
    finish_chunk(steps - 1)

    @pl.loop(GROUP - 1, 2 * GROUP)
    def _(n):
        @pl.when(n == GROUP)
        def _():
            send_back(last - 1)
            owned_arrival(last)

        orthogonalize(last - 1 + n // GROUP, n % GROUP)

        @pl.when(n >= GROUP)
        def _():
            for r in range(NDEV - 1):
                tail_send(last, n - GROUP, r).start()

    @pl.loop(0, steps // PAIR)
    def _(q):
        for copy in raw_copies(q):
            copy.wait_send()

    @pl.loop(steps - SLOTS, steps)
    def _(k):
        for s in range(2):
            part_copy(k, s).wait_send()

    for r in range(3):
        own_send(last, r).wait_send()
        nrm_send(last, r).wait_send()

    @pl.loop((steps - 4 - GROUP) // GROUP, last)
    def _(g):
        update_weights(g)

    update_last(last)

    for r in range(NDEV - 1):
        for g in range(groups - XSLOTS, last):
            back_send(g, r).wait_send()
        for i in range(GROUP):
            tail_send(last, i, r).wait_send()


def write_kernel(results, w_out, mom_out, sems):
    n = w_out.shape[0] // PIECES
    copies = []
    for i in range(PIECES):
        rng = pl.ds(i * n, n)
        copies.append(pltpu.make_async_copy(results.at[0, rng], w_out.at[rng], sems.at[0, i]))
        copies.append(pltpu.make_async_copy(results.at[1, rng], mom_out.at[rng], sems.at[1, i]))
    for copy in copies:
        copy.start()
    for copy in copies:
        copy.wait()


def solution(mesh):
    row_spec = P('stage', 'data', None)
    grad_spec = P(('stage', 'data'), None, None, None)

    def local_step(w_rows, mom_rows, grad_full):
        n_mats, rows, n_cols = w_rows.shape
        n_rows = rows * NDEV
        steps = n_mats // CHUNK
        groups = steps // GROUP
        grad_view = grad_full.reshape(steps, 2, HALF, 2, 2, 2, rows, n_cols)
        f32, bf16 = jnp.float32, jnp.bfloat16
        dma = pltpu.SemaphoreType.DMA
        hbm = pl.BlockSpec(memory_space=pltpu.HBM)
        vmem = pl.BlockSpec(memory_space=pltpu.VMEM)
        results, _ = pl.pallas_call(
            muon_kernel,
            name="muon_step",
            out_shape=(
                pltpu.VMEM((2, n_mats, rows, n_cols), f32),
                jax.ShapeDtypeStruct((steps // PAIR, 2, 3, PAIR, HALF, 2, rows, n_cols), bf16),
            ),
            in_specs=[hbm] * 3,
            out_specs=(vmem, hbm),
            scratch_shapes=[
                pltpu.VMEM((2, 4, HALF, 2, rows, n_cols), bf16),
                pltpu.VMEM((2, CHUNK, rows, n_cols), f32),
                pltpu.VMEM((SLOTS, 2, HALF, rows, n_cols), f32),
                pltpu.VMEM((SLOTS, CHUNK, rows, n_cols), f32),
                pltpu.VMEM((GSLOTS, NDEV // 2, 2, GROUP, rows, n_cols), bf16),
                pltpu.VMEM((NDEV // 2, GROUP, rows, n_cols), bf16),
                pltpu.VMEM((OSLOTS, NDEV, GROUP, rows, n_cols), bf16),
                pltpu.VMEM((GSLOTS, NDEV // 2, 2, GROUP, 1, 128), f32),
                pltpu.VMEM((NDEV // 2, GROUP, 1, 128), f32),
                pltpu.VMEM((groups, NDEV, GROUP, 1, 128), f32),
                pltpu.VMEM((XSLOTS, GROUP, n_rows, n_cols), bf16),
                pltpu.VMEM((RSLOTS, NDEV, GROUP, rows, n_cols), bf16),
                pltpu.VMEM((n_rows, n_rows), bf16),
                pltpu.VMEM((n_rows, n_rows), bf16),
                dma((steps // PAIR, 2, 3)), dma((steps // PAIR, 2, 3)),
                dma((SLOTS, 2)), dma((steps, 2)),
                dma((2,)), dma((groups, 2)),
                dma((GSLOTS, 3)), dma((groups, 3)),
                dma((GSLOTS, 3)), dma((groups, 3)),
                dma((XSLOTS, NDEV)), dma((groups, NDEV)),
                dma((GROUP, NDEV)), dma((GROUP, NDEV)),
                dma((2, 4)), dma((SLOTS,)), dma((steps,)),
            ],
            compiler_params=pltpu.CompilerParams(
                collective_id=0, has_side_effects=True, vmem_limit_bytes=31 * 2 ** 20),
        )(grad_view, mom_rows, w_rows)
        return pl.pallas_call(
            write_kernel,
            name="write_results",
            out_shape=(jax.ShapeDtypeStruct(w_rows.shape, f32), jax.ShapeDtypeStruct(w_rows.shape, f32)),
            in_specs=[vmem],
            out_specs=(hbm, hbm),
            scratch_shapes=[dma((2, PIECES))],
            compiler_params=pltpu.CompilerParams(vmem_limit_bytes=2 ** 20),
        )(results)

    return jax.shard_map(local_step, mesh=mesh, in_specs=(row_spec, row_spec, grad_spec),
                         out_specs=(row_spec, row_spec), check_vma=False)
```

```python
import functools
import math

import jax
import jax.numpy as jnp
from jax import lax
from jax.experimental import pallas as pl
from jax.experimental.pallas import tpu as pltpu
from jax.sharding import PartitionSpec as P

MOMENTUM_COEF = 0.95
LEARN_RATE = 0.05
WEIGHT_DECAY = 0.2
NORM_EPS = 1e-7
COEF_A = 3.4445
COEF_B = -4.7750
COEF_C = 2.0315
NS_ITERS = 5

NDEV = 8
CHUNK = 8
HALF = 4
PAIR = 2
AHEAD = 2
SLOTS = 3
GROUP = 2
GSLOTS = 2
OSLOTS = 3
XSLOTS = 3
RSLOTS = 3
PIECES = 4
MESH = pl.DeviceIdType.MESH


def muon_kernel(
    grad, mom, w, results, raw,
    inbuf, kept, part, momb, stage, swap, owned, nstage, nswap, owned_n, xbuf, xswap, xstage, xin, gram, poly,
    raw_s, raw_r, part_s, part_r, swap_s, swap_r, own_s, own_r, nrm_s, nrm_r, xswap_s, xswap_r, back_s, back_r, tswap_s, tswap_r, tail_s, tail_r,
    in_sem, mom_in, w_in,
):
    n_mats, rows, cols = mom.shape
    rms_scale = 0.2 * math.sqrt(max(rows * NDEV, cols))
    w_out, mom_out = results.at[0], results.at[1]
    steps = n_mats // CHUNK
    me = lax.axis_index("data")
    y, x, c = me // 4, (me // 2) % 2, me % 2
    partner = y * 4 + x * 2 + (1 - c)
    x_nbr = y * 4 + (1 - x) * 2
    y_nbr = (1 - y) * 4 + x * 2
    diagonal = (1 - y) * 4 + (1 - x) * 2
    peers = [base + core for base in (diagonal, x_nbr, y_nbr) for core in (c, 1 - c)] + [partner]

    chip = me // 2
    chips = [base // 2 for base in (diagonal, x_nbr, y_nbr)]

    def remote(src, dst, send, recv, dev):
        return pltpu.make_async_remote_copy(
            src_ref=src, dst_ref=dst, send_sem=send, recv_sem=recv,
            device_id={"data": dev}, device_id_type=MESH)

    barrier = pltpu.get_barrier_semaphore()
    for peer in peers:
        pl.semaphore_signal(barrier, inc=1, device_id={"data": peer}, device_id_type=MESH)
    pl.semaphore_wait(barrier, NDEV - 1)

    def raw_copies(q):
        rng = pl.ds(q * PAIR, PAIR)
        out = []
        for dc in range(2):
            out.append(remote(grad.at[rng, 0, :, :, 1 - x, dc], raw.at[q, 0, 1 + c],
                              raw_s.at[q, 0, 1 + dc], raw_r.at[q, 0, 1 + c], x_nbr + dc))
            out.append(remote(grad.at[rng, 1, :, 1 - y, :, dc], raw.at[q, 1, 1 + c],
                              raw_s.at[q, 1, 1 + dc], raw_r.at[q, 1, 1 + c], y_nbr + dc))
        out.append(remote(grad.at[rng, 0, :, :, x, 1 - c], raw.at[q, 0, 0], raw_s.at[q, 0, 0], raw_r.at[q, 0, 0], partner))
        out.append(remote(grad.at[rng, 1, :, y, :, 1 - c], raw.at[q, 1, 0], raw_s.at[q, 1, 0], raw_r.at[q, 1, 0], partner))
        return out

    def raw_arrival(q, s, i):
        return pltpu.make_async_copy(raw.at[q, s, i], raw.at[q, s, i], raw_r.at[q, s, i])

    def own_copy(k, s):
        src = grad.at[k, 0, :, :, x, c] if s == 0 else grad.at[k, 1, :, y, :, c]
        return pltpu.make_async_copy(src, inbuf.at[s, 0], in_sem.at[s, 0])

    def raw_load(k, s, i):
        return pltpu.make_async_copy(raw.at[k // PAIR, s, i, k % PAIR], inbuf.at[s, 1 + i], in_sem.at[s, 1 + i])

    def part_copy(k, s):
        slot = k % SLOTS
        return remote(part.at[slot, s], mom_out.at[pl.ds(k * CHUNK + s * HALF, HALF)],
                      part_s.at[slot, s], part_r.at[k, s], (y_nbr if s == 0 else x_nbr) + c)

    def mom_load(k):
        return pltpu.make_async_copy(mom.at[pl.ds(k * CHUNK, CHUNK)], momb.at[k % SLOTS], mom_in.at[k % SLOTS])

    def w_load(k):
        rng = pl.ds(k * CHUNK, CHUNK)
        return pltpu.make_async_copy(w.at[rng], w_out.at[rng], w_in.at[k])

    def swap_copies(g):
        slot = g % GSLOTS
        return [remote(swap, stage.at[slot, :, c], swap_s.at[0], swap_r.at[g, 0], partner),
                remote(nswap, nstage.at[slot, :, c], swap_s.at[1], swap_r.at[g, 1], partner)]

    def own_send(g, r):
        slot = g % GSLOTS
        return remote(stage.at[slot, chips[r]], owned.at[g % OSLOTS, pl.ds(chip * 2, 2)],
                      own_s.at[slot, r], own_r.at[g, r], chips[r] * 2 + c)

    def nrm_send(g, r):
        slot = g % GSLOTS
        return remote(nstage.at[slot, chips[r]], owned_n.at[g, pl.ds(chip * 2, 2)],
                      nrm_s.at[slot, r], nrm_r.at[g, r], chips[r] * 2 + c)

    def xswap_copy(g):
        return remote(xswap, xstage.at[g % XSLOTS, :, c], xswap_s.at[0], xswap_r.at[g], partner)

    def back_send(g, r):
        slot = g % XSLOTS
        return remote(xstage.at[slot, chips[r]], xin.at[g % RSLOTS, pl.ds(chip * 2, 2)],
                      back_s.at[slot, r], back_r.at[g, r], chips[r] * 2 + c)

    def tail_swap(g, i):
        return remote(xswap.at[:, i], xstage.at[g % XSLOTS, :, c, i], tswap_s.at[i], tswap_r.at[i], partner)

    def tail_send(g, i, r):
        return remote(xstage.at[g % XSLOTS, chips[r], :, i], xin.at[g % RSLOTS, pl.ds(chip * 2, 2), i],
                      tail_s.at[i, r], tail_r.at[i, r], chips[r] * 2 + c)

    def keep_rows(g, i):
        for core in range(2):
            xin[g % RSLOTS, chip * 2 + core, i] = xstage[g % XSLOTS, chip, core, i]

    def sum_chunk(k):
        slot = k % SLOTS
        @pl.when(k % PAIR == 0)
        def _():
            for s in range(2):
                for i in range(3):
                    raw_arrival(k // PAIR, s, i).wait()

        for s in range(2):
            for i in range(3):
                raw_load(k, s, i).start()

        @pl.when(k >= SLOTS)
        def _():
            for s in range(2):
                part_copy(k - SLOTS, s).wait_send()

        for s in range(2):
            own_copy(k, s).wait()
            for i in range(3):
                raw_load(k, s, i).wait()
            keep = y if s == 0 else x

            @pl.loop(0, HALF)
            def _(m):
                def total(e):
                    v = [inbuf[s, i, m, e].astype(jnp.float32) for i in range(4)]
                    return (v[0] + v[1]) + (v[2] + v[3])

                part[slot, s, m] = total(1 - keep)
                kept[k % 2, s * HALF + m] = total(keep)

            part_copy(k, s).start()

        @pl.when(k + 1 < steps)
        def _():
            for s in range(2):
                own_copy(k + 1, s).start()
        w_load(k).start()

    def finish_chunk(k):
        slot = k % SLOTS
        g, i = k // GROUP, k % GROUP
        gslot = g % GSLOTS
        mom_load(k).wait()
        for s in range(2):
            part_copy(k, s).wait_recv()

        def momentum(j):
            new = MOMENTUM_COEF * momb[slot, j] + (kept[k % 2, j] + mom_out[k * CHUNK + j])
            mom_out[k * CHUNK + j] = new
            sq = jnp.sum(new * new, axis=0, keepdims=True)
            return new.astype(jnp.bfloat16), (sq[:, :128] + sq[:, 128:256]) + (sq[:, 256:384] + sq[:, 384:])

        @pl.loop(0, NDEV // 2)
        def _(q):
            stage[gslot, q, c, i], nstage[gslot, q, c, i] = momentum(2 * q + c)
            swap[q, i], nswap[q, i] = momentum(2 * q + 1 - c)

        @pl.when(i == GROUP - 1)
        def _():
            @pl.when(g >= 1)
            def _():
                for r in range(3):
                    own_send(g - 1, r).wait_send()
                    nrm_send(g - 1, r).wait_send()

            @pl.when(g >= XSLOTS)
            def _():
                for r in range(3):
                    back_send(g - XSLOTS, r).wait_send()

            for copy in swap_copies(g):
                copy.start()
            for copy in swap_copies(g):
                copy.wait()
            for r in range(3):
                own_send(g, r).start()
                nrm_send(g, r).start()

            @pl.loop(0, GROUP)
            def _(n):
                for core in range(2):
                    owned[g % OSLOTS, chip * 2 + core, n] = stage[gslot, chip, core, n]
                    owned_n[g, chip * 2 + core, n] = nstage[gslot, chip, core, n]

        @pl.when(k + 1 < steps)
        def _():
            mom_load(k + 1).start()

    def owned_arrival(g):
        for r in range(3):
            own_send(g, r).wait_recv()
            nrm_send(g, r).wait_recv()

    def orthogonalize(g, i):
        sq = owned_n[g, 0, i]
        for j in range(1, NDEV):
            sq = sq + owned_n[g, j, i]
        den = jnp.sqrt(jnp.sum(sq, axis=1, keepdims=True)) + NORM_EPS

        @pl.loop(0, NDEV)
        def _(j):
            blk = pl.ds(pl.multiple_of(j * rows, rows), rows)
            xbuf[blk] = (owned[g % OSLOTS, j, i].astype(jnp.float32) / den).astype(jnp.bfloat16)

        @pl.loop(0, NS_ITERS)
        def _(_):
            cur = xbuf[...]
            gram[...] = lax.dot_general(cur, cur, (((1,), (1,)), ((), ())),
                                        preferred_element_type=jnp.float32).astype(jnp.bfloat16)
            gm = gram[...]
            sqr = jnp.dot(gm, gm, preferred_element_type=jnp.float32)
            poly[...] = (COEF_B * gm.astype(jnp.float32) + COEF_C * sqr).astype(jnp.bfloat16)
            px = jnp.dot(poly[...], cur, preferred_element_type=jnp.float32)
            xbuf[...] = (COEF_A * cur.astype(jnp.float32) + px).astype(jnp.bfloat16)

        @pl.loop(0, NDEV // 2)
        def _(q):
            xstage[g % XSLOTS, q, c, i] = xbuf[pl.ds(pl.multiple_of((2 * q + c) * rows, rows), rows)]
            xswap[q, i] = xbuf[pl.ds(pl.multiple_of((2 * q + 1 - c) * rows, rows), rows)]

    def send_back(g):
        xswap_copy(g).wait()
        for r in range(3):
            back_send(g, r).start()

        @pl.loop(0, GROUP)
        def _(i):
            keep_rows(g, i)

    def update_rows(g, i, j):
        m = (g * GROUP + i) * CHUNK + j
        old = w_out[m]
        step = xin[g % RSLOTS, j, i].astype(jnp.float32) * rms_scale
        w_out[m] = old - LEARN_RATE * (step + WEIGHT_DECAY * old)

    def update_weights(g):
        for i in range(GROUP):
            w_load(g * GROUP + i).wait()
        for r in range(4):
            if r < 3:
                back_send(g, r).wait_recv()

            @pl.loop(0, GROUP)
            def _(i):
                for core in range(2):
                    update_rows(g, i, (chips + [chip])[r] * 2 + core)

    def update_last(g):
        @pl.loop(0, GROUP)
        def _(i):
            w_load(g * GROUP + i).wait()
            for r in range(-1, 3):
                if r >= 0:
                    tail_send(g, i, r).wait_recv()
                for core in range(2):
                    update_rows(g, i, (chips[r] if r >= 0 else chip) * 2 + core)

    for q in range(AHEAD // PAIR):
        for copy in raw_copies(q):
            copy.start()
    for s in range(2):
        own_copy(0, s).start()
    mom_load(0).start()

    @pl.loop(0, steps)
    def _(t):
        @pl.when((t % PAIR == 0) & (t + AHEAD < steps))
        def _():
            for copy in raw_copies((t + AHEAD) // PAIR):
                copy.start()

        sum_chunk(t)

        def at(lag, work):
            @pl.when(((t - lag) % GROUP == 0) & (t >= lag + GROUP))
            def _():
                work((t - lag) // GROUP - 1)

        at(1 + GROUP, send_back)

        @pl.when(t >= 1)
        def _():
            finish_chunk(t - 1)

        at(1, owned_arrival)

        @pl.when(t >= 1 + GROUP)
        def _():
            g, i = (t - 1) // GROUP - 1, (t - 1) % GROUP
            orthogonalize(g, i)

            @pl.when(i == GROUP - 1)
            def _():
                xswap_copy(g).start()

        at(3 + GROUP, update_weights)

    groups = steps // GROUP
    last = groups - 1
    finish_chunk(steps - 1)

    @pl.loop(GROUP - 1, 2 * GROUP)
    def _(n):
        @pl.when(n == GROUP)
        def _():
            send_back(last - 1)
            owned_arrival(last)

        orthogonalize(last - 1 + n // GROUP, n % GROUP)

        @pl.when(n == GROUP - 1)
        def _():
            xswap_copy(last - 1).start()

        @pl.when(n >= GROUP)
        def _():
            i = n - GROUP
            tail_swap(last, i).start()
            tail_swap(last, i).wait()
            for r in range(3):
                tail_send(last, i, r).start()
            keep_rows(last, i)

    @pl.loop(0, steps // PAIR)
    def _(q):
        for copy in raw_copies(q):
            copy.wait_send()

    @pl.loop(steps - SLOTS, steps)
    def _(k):
        for s in range(2):
            part_copy(k, s).wait_send()

    for r in range(3):
        own_send(last, r).wait_send()
        nrm_send(last, r).wait_send()

    @pl.loop((steps - 4 - GROUP) // GROUP, last)
    def _(g):
        update_weights(g)

    update_last(last)

    for r in range(3):
        for g in range(groups - XSLOTS, last):
            back_send(g, r).wait_send()
        for i in range(GROUP):
            tail_send(last, i, r).wait_send()


def write_kernel(results, w_out, mom_out, sems):
    n = w_out.shape[0] // PIECES
    copies = []
    for i in range(PIECES):
        rng = pl.ds(i * n, n)
        copies.append(pltpu.make_async_copy(results.at[0, rng], w_out.at[rng], sems.at[0, i]))
        copies.append(pltpu.make_async_copy(results.at[1, rng], mom_out.at[rng], sems.at[1, i]))
    for copy in copies:
        copy.start()
    for copy in copies:
        copy.wait()


def solution(mesh):
    row_spec = P('stage', 'data', None)
    grad_spec = P(('stage', 'data'), None, None, None)

    def local_step(w_rows, mom_rows, grad_full):
        n_mats, rows, n_cols = w_rows.shape
        n_rows = rows * NDEV
        steps = n_mats // CHUNK
        groups = steps // GROUP
        grad_view = grad_full.reshape(steps, 2, HALF, 2, 2, 2, rows, n_cols)
        f32, bf16 = jnp.float32, jnp.bfloat16
        dma = pltpu.SemaphoreType.DMA
        hbm = pl.BlockSpec(memory_space=pltpu.HBM)
        vmem = pl.BlockSpec(memory_space=pltpu.VMEM)
        results, _ = pl.pallas_call(
            muon_kernel,
            name="muon_step",
            out_shape=(
                pltpu.VMEM((2, n_mats, rows, n_cols), f32),
                jax.ShapeDtypeStruct((steps // PAIR, 2, 3, PAIR, HALF, 2, rows, n_cols), bf16),
            ),
            in_specs=[hbm] * 3,
            out_specs=(vmem, hbm),
            scratch_shapes=[
                pltpu.VMEM((2, 4, HALF, 2, rows, n_cols), bf16),
                pltpu.VMEM((2, CHUNK, rows, n_cols), f32),
                pltpu.VMEM((SLOTS, 2, HALF, rows, n_cols), f32),
                pltpu.VMEM((SLOTS, CHUNK, rows, n_cols), f32),
                pltpu.VMEM((GSLOTS, NDEV // 2, 2, GROUP, rows, n_cols), bf16),
                pltpu.VMEM((NDEV // 2, GROUP, rows, n_cols), bf16),
                pltpu.VMEM((OSLOTS, NDEV, GROUP, rows, n_cols), bf16),
                pltpu.VMEM((GSLOTS, NDEV // 2, 2, GROUP, 1, 128), f32),
                pltpu.VMEM((NDEV // 2, GROUP, 1, 128), f32),
                pltpu.VMEM((groups, NDEV, GROUP, 1, 128), f32),
                pltpu.VMEM((n_rows, n_cols), bf16),
                pltpu.VMEM((NDEV // 2, GROUP, rows, n_cols), bf16),
                pltpu.VMEM((XSLOTS, NDEV // 2, 2, GROUP, rows, n_cols), bf16),
                pltpu.VMEM((RSLOTS, NDEV, GROUP, rows, n_cols), bf16),
                pltpu.VMEM((n_rows, n_rows), bf16),
                pltpu.VMEM((n_rows, n_rows), bf16),
                dma((steps // PAIR, 2, 3)), dma((steps // PAIR, 2, 3)),
                dma((SLOTS, 2)), dma((steps, 2)),
                dma((2,)), dma((groups, 2)),
                dma((GSLOTS, 3)), dma((groups, 3)),
                dma((GSLOTS, 3)), dma((groups, 3)),
                dma((1,)), dma((groups,)),
                dma((XSLOTS, 3)), dma((groups, 3)),
                dma((GROUP,)), dma((GROUP,)),
                dma((GROUP, 3)), dma((GROUP, 3)),
                dma((2, 4)), dma((SLOTS,)), dma((steps,)),
            ],
            compiler_params=pltpu.CompilerParams(
                collective_id=0, has_side_effects=True, vmem_limit_bytes=31 * 2 ** 20),
        )(grad_view, mom_rows, w_rows)
        return pl.pallas_call(
            write_kernel,
            name="write_results",
            out_shape=(jax.ShapeDtypeStruct(w_rows.shape, f32), jax.ShapeDtypeStruct(w_rows.shape, f32)),
            in_specs=[vmem],
            out_specs=(hbm, hbm),
            scratch_shapes=[dma((2, PIECES))],
            compiler_params=pltpu.CompilerParams(vmem_limit_bytes=2 ** 20),
        )(results)

    return jax.shard_map(local_step, mesh=mesh, in_specs=(row_spec, row_spec, grad_spec),
                         out_specs=(row_spec, row_spec), check_vma=False)
```

```python
import functools
import math

import jax
import jax.numpy as jnp
from jax import lax
from jax.experimental import pallas as pl
from jax.experimental.pallas import tpu as pltpu
from jax.sharding import PartitionSpec as P

MOMENTUM_COEF = 0.95
LEARN_RATE = 0.05
WEIGHT_DECAY = 0.2
NORM_EPS = 1e-7
COEF_A = 3.4445
COEF_B = -4.7750
COEF_C = 2.0315
NS_ITERS = 5

NDEV = 8
CHUNK = 8
HALF = 4
PAIR = 2
AHEAD = 2
SLOTS = 3
GROUP = 2
GSLOTS = 2
OSLOTS = 3
XSLOTS = 3
RSLOTS = 3
PIECES = 4
MESH = pl.DeviceIdType.MESH


def muon_kernel(
    grad, mom, w, results, raw,
    inbuf, kept, part, momb, stage, swap, owned, nstage, nswap, owned_n, xbuf, xswap, xstage, xin, gram, poly,
    raw_s, raw_r, part_s, part_r, swap_s, swap_r, own_s, own_r, nrm_s, nrm_r, xswap_s, xswap_r, back_s, back_r, tail_s, tail_r,
    in_sem, mom_in, w_in,
):
    n_mats, rows, cols = mom.shape
    rms_scale = 0.2 * math.sqrt(max(rows * NDEV, cols))
    w_out, mom_out = results.at[0], results.at[1]
    steps = n_mats // CHUNK
    me = lax.axis_index("data")
    y, x, c = me // 4, (me // 2) % 2, me % 2
    partner = y * 4 + x * 2 + (1 - c)
    x_nbr = y * 4 + (1 - x) * 2
    y_nbr = (1 - y) * 4 + x * 2
    diagonal = (1 - y) * 4 + (1 - x) * 2
    peers = [base + core for base in (diagonal, x_nbr, y_nbr) for core in (c, 1 - c)] + [partner]

    chip = me // 2
    chips = [base // 2 for base in (diagonal, x_nbr, y_nbr)]

    def remote(src, dst, send, recv, dev):
        return pltpu.make_async_remote_copy(
            src_ref=src, dst_ref=dst, send_sem=send, recv_sem=recv,
            device_id={"data": dev}, device_id_type=MESH)

    barrier = pltpu.get_barrier_semaphore()
    for peer in peers:
        pl.semaphore_signal(barrier, inc=1, device_id={"data": peer}, device_id_type=MESH)
    pl.semaphore_wait(barrier, NDEV - 1)

    def raw_copies(q):
        rng = pl.ds(q * PAIR, PAIR)
        out = []
        for dc in range(2):
            out.append(remote(grad.at[rng, 0, :, :, 1 - x, dc], raw.at[q, 0, 1 + c],
                              raw_s.at[q, 0, 1 + dc], raw_r.at[q, 0, 1 + c], x_nbr + dc))
            out.append(remote(grad.at[rng, 1, :, 1 - y, :, dc], raw.at[q, 1, 1 + c],
                              raw_s.at[q, 1, 1 + dc], raw_r.at[q, 1, 1 + c], y_nbr + dc))
        out.append(remote(grad.at[rng, 0, :, :, x, 1 - c], raw.at[q, 0, 0], raw_s.at[q, 0, 0], raw_r.at[q, 0, 0], partner))
        out.append(remote(grad.at[rng, 1, :, y, :, 1 - c], raw.at[q, 1, 0], raw_s.at[q, 1, 0], raw_r.at[q, 1, 0], partner))
        return out

    def raw_arrival(q, s, i):
        return pltpu.make_async_copy(raw.at[q, s, i], raw.at[q, s, i], raw_r.at[q, s, i])

    def own_copy(k, s):
        src = grad.at[k, 0, :, :, x, c] if s == 0 else grad.at[k, 1, :, y, :, c]
        return pltpu.make_async_copy(src, inbuf.at[s, 0], in_sem.at[s, 0])

    def raw_load(k, s, i):
        return pltpu.make_async_copy(raw.at[k // PAIR, s, i, k % PAIR], inbuf.at[s, 1 + i], in_sem.at[s, 1 + i])

    def part_copy(k, s):
        slot = k % SLOTS
        return remote(part.at[slot, s], mom_out.at[pl.ds(k * CHUNK + s * HALF, HALF)],
                      part_s.at[slot, s], part_r.at[k, s], (y_nbr if s == 0 else x_nbr) + c)

    def mom_load(k):
        return pltpu.make_async_copy(mom.at[pl.ds(k * CHUNK, CHUNK)], momb.at[k % SLOTS], mom_in.at[k % SLOTS])

    def w_load(k):
        rng = pl.ds(k * CHUNK, CHUNK)
        return pltpu.make_async_copy(w.at[rng], w_out.at[rng], w_in.at[k])

    def swap_copies(g):
        slot = g % GSLOTS
        return [remote(swap, stage.at[slot, :, c], swap_s.at[0], swap_r.at[g, 0], partner),
                remote(nswap, nstage.at[slot, :, c], swap_s.at[1], swap_r.at[g, 1], partner)]

    def own_send(g, r):
        slot = g % GSLOTS
        return remote(stage.at[slot, chips[r]], owned.at[g % OSLOTS, pl.ds(chip * 2, 2)],
                      own_s.at[slot, r], own_r.at[g, r], chips[r] * 2 + c)

    def nrm_send(g, r):
        slot = g % GSLOTS
        return remote(nstage.at[slot, chips[r]], owned_n.at[g, pl.ds(chip * 2, 2)],
                      nrm_s.at[slot, r], nrm_r.at[g, r], chips[r] * 2 + c)

    def xswap_copy(g):
        return remote(xswap, xstage.at[g % XSLOTS, :, c], xswap_s.at[0], xswap_r.at[g], partner)

    def back_send(g, r):
        slot = g % XSLOTS
        return remote(xstage.at[slot, chips[r]], xin.at[g % RSLOTS, pl.ds(chip * 2, 2)],
                      back_s.at[slot, r], back_r.at[g, r], chips[r] * 2 + c)

    def tail_send(g, i, r):
        return remote(xbuf.at[i, pl.ds(peers[r] * rows, rows)], xin.at[g % RSLOTS, me, i],
                      tail_s.at[i, r], tail_r.at[i, r], peers[r])

    def sum_chunk(k):
        slot = k % SLOTS
        @pl.when(k % PAIR == 0)
        def _():
            for s in range(2):
                for i in range(3):
                    raw_arrival(k // PAIR, s, i).wait()

        for s in range(2):
            for i in range(3):
                raw_load(k, s, i).start()

        @pl.when(k >= SLOTS)
        def _():
            for s in range(2):
                part_copy(k - SLOTS, s).wait_send()

        for s in range(2):
            own_copy(k, s).wait()
            for i in range(3):
                raw_load(k, s, i).wait()
            keep = y if s == 0 else x

            @pl.loop(0, HALF)
            def _(m):
                def total(e):
                    v = [inbuf[s, i, m, e].astype(jnp.float32) for i in range(4)]
                    return (v[0] + v[1]) + (v[2] + v[3])

                part[slot, s, m] = total(1 - keep)
                kept[k % 2, s * HALF + m] = total(keep)

            part_copy(k, s).start()

        @pl.when(k + 1 < steps)
        def _():
            for s in range(2):
                own_copy(k + 1, s).start()
        w_load(k).start()

    def finish_chunk(k):
        slot = k % SLOTS
        g, i = k // GROUP, k % GROUP
        gslot = g % GSLOTS
        mom_load(k).wait()
        for s in range(2):
            part_copy(k, s).wait_recv()

        def momentum(j):
            new = MOMENTUM_COEF * momb[slot, j] + (kept[k % 2, j] + mom_out[k * CHUNK + j])
            mom_out[k * CHUNK + j] = new
            sq = jnp.sum(new * new, axis=0, keepdims=True)
            return new.astype(jnp.bfloat16), (sq[:, :128] + sq[:, 128:256]) + (sq[:, 256:384] + sq[:, 384:])

        @pl.loop(0, NDEV // 2)
        def _(q):
            stage[gslot, q, c, i], nstage[gslot, q, c, i] = momentum(2 * q + c)
            swap[q, i], nswap[q, i] = momentum(2 * q + 1 - c)

        @pl.when(i == GROUP - 1)
        def _():
            @pl.when(g >= 1)
            def _():
                for r in range(3):
                    own_send(g - 1, r).wait_send()
                    nrm_send(g - 1, r).wait_send()

            @pl.when(g >= XSLOTS)
            def _():
                for r in range(3):
                    back_send(g - XSLOTS, r).wait_send()

            for copy in swap_copies(g):
                copy.start()
            for copy in swap_copies(g):
                copy.wait()
            for r in range(3):
                own_send(g, r).start()
                nrm_send(g, r).start()

            @pl.loop(0, GROUP)
            def _(n):
                for core in range(2):
                    owned[g % OSLOTS, chip * 2 + core, n] = stage[gslot, chip, core, n]
                    owned_n[g, chip * 2 + core, n] = nstage[gslot, chip, core, n]

        @pl.when(k + 1 < steps)
        def _():
            mom_load(k + 1).start()

    def owned_arrival(g):
        for r in range(3):
            own_send(g, r).wait_recv()
            nrm_send(g, r).wait_recv()

    def orthogonalize(g, i):
        sq = owned_n[g, 0, i]
        for j in range(1, NDEV):
            sq = sq + owned_n[g, j, i]
        den = jnp.sqrt(jnp.sum(sq, axis=1, keepdims=True)) + NORM_EPS

        @pl.loop(0, NDEV)
        def _(j):
            blk = pl.ds(pl.multiple_of(j * rows, rows), rows)
            xbuf[i, blk] = (owned[g % OSLOTS, j, i].astype(jnp.float32) / den).astype(jnp.bfloat16)

        @pl.loop(0, NS_ITERS)
        def _(_):
            cur = xbuf[i]
            gram[...] = lax.dot_general(cur, cur, (((1,), (1,)), ((), ())),
                                        preferred_element_type=jnp.float32).astype(jnp.bfloat16)
            gm = gram[...]
            sqr = jnp.dot(gm, gm, preferred_element_type=jnp.float32)
            poly[...] = (COEF_B * gm.astype(jnp.float32) + COEF_C * sqr).astype(jnp.bfloat16)
            px = jnp.dot(poly[...], cur, preferred_element_type=jnp.float32)
            xbuf[i] = (COEF_A * cur.astype(jnp.float32) + px).astype(jnp.bfloat16)

    def split_rows(g, i):
        @pl.loop(0, NDEV // 2)
        def _(q):
            xstage[g % XSLOTS, q, c, i] = xbuf[i, pl.ds(pl.multiple_of((2 * q + c) * rows, rows), rows)]
            xswap[q, i] = xbuf[i, pl.ds(pl.multiple_of((2 * q + 1 - c) * rows, rows), rows)]

        @pl.when(i == GROUP - 1)
        def _():
            xswap_copy(g).start()

    def send_back(g):
        xswap_copy(g).wait()
        for r in range(3):
            back_send(g, r).start()

        @pl.loop(0, GROUP)
        def _(i):
            for core in range(2):
                xin[g % RSLOTS, chip * 2 + core, i] = xstage[g % XSLOTS, chip, core, i]

    def update_rows(g, i, j):
        m = (g * GROUP + i) * CHUNK + j
        old = w_out[m]
        step = xin[g % RSLOTS, j, i].astype(jnp.float32) * rms_scale
        w_out[m] = old - LEARN_RATE * (step + WEIGHT_DECAY * old)

    def update_weights(g):
        for i in range(GROUP):
            w_load(g * GROUP + i).wait()
        for r in range(4):
            if r < 3:
                back_send(g, r).wait_recv()

            @pl.loop(0, GROUP)
            def _(i):
                for core in range(2):
                    update_rows(g, i, (chips + [chip])[r] * 2 + core)

    def update_last(g):
        @pl.loop(0, GROUP)
        def _(i):
            w_load(g * GROUP + i).wait()
            update_rows(g, i, me)
            for r in range(NDEV - 1):
                pltpu.make_async_copy(xin.at[g % RSLOTS, peers[r], i], xin.at[g % RSLOTS, peers[r], i],
                                      tail_r.at[i, r]).wait()
                update_rows(g, i, peers[r])

    for q in range(AHEAD // PAIR):
        for copy in raw_copies(q):
            copy.start()
    for s in range(2):
        own_copy(0, s).start()
    mom_load(0).start()

    @pl.loop(0, steps)
    def _(t):
        @pl.when((t % PAIR == 0) & (t + AHEAD < steps))
        def _():
            for copy in raw_copies((t + AHEAD) // PAIR):
                copy.start()

        sum_chunk(t)

        def at(lag, work):
            @pl.when(((t - lag) % GROUP == 0) & (t >= lag + GROUP))
            def _():
                work((t - lag) // GROUP - 1)

        at(1 + GROUP, send_back)

        @pl.when(t >= 1)
        def _():
            finish_chunk(t - 1)

        at(1, owned_arrival)

        @pl.when(t >= 1 + GROUP)
        def _():
            g, i = (t - 1) // GROUP - 1, (t - 1) % GROUP
            orthogonalize(g, i)
            split_rows(g, i)

        at(3 + GROUP, update_weights)

    groups = steps // GROUP
    last = groups - 1
    finish_chunk(steps - 1)

    @pl.loop(GROUP - 1, 2 * GROUP)
    def _(n):
        @pl.when(n == GROUP)
        def _():
            send_back(last - 1)
            owned_arrival(last)

        orthogonalize(last - 1 + n // GROUP, n % GROUP)

        @pl.when(n == GROUP - 1)
        def _():
            split_rows(last - 1, n)

        @pl.when(n >= GROUP)
        def _():
            i = n - GROUP
            for r in range(NDEV - 1):
                tail_send(last, i, r).start()
            xin[last % RSLOTS, me, i] = xbuf[i, pl.ds(pl.multiple_of(me * rows, rows), rows)]

    @pl.loop(0, steps // PAIR)
    def _(q):
        for copy in raw_copies(q):
            copy.wait_send()

    @pl.loop(steps - SLOTS, steps)
    def _(k):
        for s in range(2):
            part_copy(k, s).wait_send()

    for r in range(3):
        own_send(last, r).wait_send()
        nrm_send(last, r).wait_send()

    @pl.loop((steps - 4 - GROUP) // GROUP, last)
    def _(g):
        update_weights(g)

    update_last(last)

    for g in range(groups - XSLOTS, last):
        for r in range(3):
            back_send(g, r).wait_send()
    for i in range(GROUP):
        for r in range(NDEV - 1):
            tail_send(last, i, r).wait_send()


def write_kernel(results, w_out, mom_out, sems):
    n = w_out.shape[0] // PIECES
    copies = []
    for i in range(PIECES):
        rng = pl.ds(i * n, n)
        copies.append(pltpu.make_async_copy(results.at[0, rng], w_out.at[rng], sems.at[0, i]))
        copies.append(pltpu.make_async_copy(results.at[1, rng], mom_out.at[rng], sems.at[1, i]))
    for copy in copies:
        copy.start()
    for copy in copies:
        copy.wait()


def solution(mesh):
    row_spec = P('stage', 'data', None)
    grad_spec = P(('stage', 'data'), None, None, None)

    def local_step(w_rows, mom_rows, grad_full):
        n_mats, rows, n_cols = w_rows.shape
        n_rows = rows * NDEV
        steps = n_mats // CHUNK
        groups = steps // GROUP
        grad_view = grad_full.reshape(steps, 2, HALF, 2, 2, 2, rows, n_cols)
        f32, bf16 = jnp.float32, jnp.bfloat16
        dma = pltpu.SemaphoreType.DMA
        hbm = pl.BlockSpec(memory_space=pltpu.HBM)
        vmem = pl.BlockSpec(memory_space=pltpu.VMEM)
        results, _ = pl.pallas_call(
            muon_kernel,
            name="muon_step",
            out_shape=(
                pltpu.VMEM((2, n_mats, rows, n_cols), f32),
                jax.ShapeDtypeStruct((steps // PAIR, 2, 3, PAIR, HALF, 2, rows, n_cols), bf16),
            ),
            in_specs=[hbm] * 3,
            out_specs=(vmem, hbm),
            scratch_shapes=[
                pltpu.VMEM((2, 4, HALF, 2, rows, n_cols), bf16),
                pltpu.VMEM((2, CHUNK, rows, n_cols), f32),
                pltpu.VMEM((SLOTS, 2, HALF, rows, n_cols), f32),
                pltpu.VMEM((SLOTS, CHUNK, rows, n_cols), f32),
                pltpu.VMEM((GSLOTS, NDEV // 2, 2, GROUP, rows, n_cols), bf16),
                pltpu.VMEM((NDEV // 2, GROUP, rows, n_cols), bf16),
                pltpu.VMEM((OSLOTS, NDEV, GROUP, rows, n_cols), bf16),
                pltpu.VMEM((GSLOTS, NDEV // 2, 2, GROUP, 1, 128), f32),
                pltpu.VMEM((NDEV // 2, GROUP, 1, 128), f32),
                pltpu.VMEM((groups, NDEV, GROUP, 1, 128), f32),
                pltpu.VMEM((GROUP, n_rows, n_cols), bf16),
                pltpu.VMEM((NDEV // 2, GROUP, rows, n_cols), bf16),
                pltpu.VMEM((XSLOTS, NDEV // 2, 2, GROUP, rows, n_cols), bf16),
                pltpu.VMEM((RSLOTS, NDEV, GROUP, rows, n_cols), bf16),
                pltpu.VMEM((n_rows, n_rows), bf16),
                pltpu.VMEM((n_rows, n_rows), bf16),
                dma((steps // PAIR, 2, 3)), dma((steps // PAIR, 2, 3)),
                dma((SLOTS, 2)), dma((steps, 2)),
                dma((2,)), dma((groups, 2)),
                dma((GSLOTS, 3)), dma((groups, 3)),
                dma((GSLOTS, 3)), dma((groups, 3)),
                dma((1,)), dma((groups,)),
                dma((XSLOTS, 3)), dma((groups, 3)),
                dma((GROUP, NDEV)), dma((GROUP, NDEV)),
                dma((2, 4)), dma((SLOTS,)), dma((steps,)),
            ],
            compiler_params=pltpu.CompilerParams(
                collective_id=0, has_side_effects=True, vmem_limit_bytes=31 * 2 ** 20),
        )(grad_view, mom_rows, w_rows)
        return pl.pallas_call(
            write_kernel,
            name="write_results",
            out_shape=(jax.ShapeDtypeStruct(w_rows.shape, f32), jax.ShapeDtypeStruct(w_rows.shape, f32)),
            in_specs=[vmem],
            out_specs=(hbm, hbm),
            scratch_shapes=[dma((2, PIECES))],
            compiler_params=pltpu.CompilerParams(vmem_limit_bytes=2 ** 20),
        )(results)

    return jax.shard_map(local_step, mesh=mesh, in_specs=(row_spec, row_spec, grad_spec),
                         out_specs=(row_spec, row_spec), check_vma=False)
```

```python
import functools
import math

import jax
import jax.numpy as jnp
from jax import lax
from jax.experimental import pallas as pl
from jax.experimental.pallas import tpu as pltpu
from jax.sharding import PartitionSpec as P

MOMENTUM_COEF = 0.95
LEARN_RATE = 0.05
WEIGHT_DECAY = 0.2
NORM_EPS = 1e-7
COEF_A = 3.4445
COEF_B = -4.7750
COEF_C = 2.0315
NS_ITERS = 5

NDEV = 8
CHUNK = 8
HALF = 4
PAIR = 4
AHEAD = 4
SLOTS = 3
GROUP = 2
GSLOTS = 2
OSLOTS = 3
XSLOTS = 3
RSLOTS = 3
PIECES = 4
MESH = pl.DeviceIdType.MESH


def muon_kernel(
    grad, mom, w, results, raw,
    inbuf, kept, part, momb, stage, swap, owned, nstage, nswap, owned_n, xbuf, xswap, xstage, xin, gram, poly,
    raw_s, raw_r, part_s, part_r, swap_s, swap_r, own_s, own_r, nrm_s, nrm_r, xswap_s, xswap_r, back_s, back_r, tail_s, tail_r,
    in_sem, mom_in, w_in,
):
    n_mats, rows, cols = mom.shape
    rms_scale = 0.2 * math.sqrt(max(rows * NDEV, cols))
    w_out, mom_out = results.at[0], results.at[1]
    steps = n_mats // CHUNK
    me = lax.axis_index("data")
    y, x, c = me // 4, (me // 2) % 2, me % 2
    partner = y * 4 + x * 2 + (1 - c)
    x_nbr = y * 4 + (1 - x) * 2
    y_nbr = (1 - y) * 4 + x * 2
    diagonal = (1 - y) * 4 + (1 - x) * 2
    peers = [base + core for base in (diagonal, x_nbr, y_nbr) for core in (c, 1 - c)] + [partner]

    chip = me // 2
    chips = [base // 2 for base in (diagonal, x_nbr, y_nbr)]

    def remote(src, dst, send, recv, dev):
        return pltpu.make_async_remote_copy(
            src_ref=src, dst_ref=dst, send_sem=send, recv_sem=recv,
            device_id={"data": dev}, device_id_type=MESH)

    barrier = pltpu.get_barrier_semaphore()
    for peer in peers:
        pl.semaphore_signal(barrier, inc=1, device_id={"data": peer}, device_id_type=MESH)
    pl.semaphore_wait(barrier, NDEV - 1)

    def raw_copies(q):
        rng = pl.ds(q * PAIR, PAIR)
        out = []
        for dc in range(2):
            out.append(remote(grad.at[rng, 0, :, :, 1 - x, dc], raw.at[q, 0, 1 + c],
                              raw_s.at[q, 0, 1 + dc], raw_r.at[q, 0, 1 + c], x_nbr + dc))
            out.append(remote(grad.at[rng, 1, :, 1 - y, :, dc], raw.at[q, 1, 1 + c],
                              raw_s.at[q, 1, 1 + dc], raw_r.at[q, 1, 1 + c], y_nbr + dc))
        out.append(remote(grad.at[rng, 0, :, :, x, 1 - c], raw.at[q, 0, 0], raw_s.at[q, 0, 0], raw_r.at[q, 0, 0], partner))
        out.append(remote(grad.at[rng, 1, :, y, :, 1 - c], raw.at[q, 1, 0], raw_s.at[q, 1, 0], raw_r.at[q, 1, 0], partner))
        return out

    def raw_arrival(q, s, i):
        return pltpu.make_async_copy(raw.at[q, s, i], raw.at[q, s, i], raw_r.at[q, s, i])

    def own_copy(k, s):
        src = grad.at[k, 0, :, :, x, c] if s == 0 else grad.at[k, 1, :, y, :, c]
        return pltpu.make_async_copy(src, inbuf.at[s, 0], in_sem.at[s, 0])

    def raw_load(k, s, i):
        return pltpu.make_async_copy(raw.at[k // PAIR, s, i, k % PAIR], inbuf.at[s, 1 + i], in_sem.at[s, 1 + i])

    def part_copy(k, s):
        slot = k % SLOTS
        return remote(part.at[slot, s], mom_out.at[pl.ds(k * CHUNK + s * HALF, HALF)],
                      part_s.at[slot, s], part_r.at[k, s], (y_nbr if s == 0 else x_nbr) + c)

    def mom_load(k):
        return pltpu.make_async_copy(mom.at[pl.ds(k * CHUNK, CHUNK)], momb.at[k % SLOTS], mom_in.at[k % SLOTS])

    def w_load(k):
        rng = pl.ds(k * CHUNK, CHUNK)
        return pltpu.make_async_copy(w.at[rng], w_out.at[rng], w_in.at[k])

    def swap_copies(g):
        slot = g % GSLOTS
        return [remote(swap, stage.at[slot, :, c], swap_s.at[0], swap_r.at[g, 0], partner),
                remote(nswap, nstage.at[slot, :, c], swap_s.at[1], swap_r.at[g, 1], partner)]

    def own_send(g, r):
        slot = g % GSLOTS
        return remote(stage.at[slot, chips[r]], owned.at[g % OSLOTS, pl.ds(chip * 2, 2)],
                      own_s.at[slot, r], own_r.at[g, r], chips[r] * 2 + c)

    def nrm_send(g, r):
        slot = g % GSLOTS
        return remote(nstage.at[slot, chips[r]], owned_n.at[g, pl.ds(chip * 2, 2)],
                      nrm_s.at[slot, r], nrm_r.at[g, r], chips[r] * 2 + c)

    def xswap_copy(g):
        return remote(xswap, xstage.at[g % XSLOTS, :, c], xswap_s.at[0], xswap_r.at[g], partner)

    def back_send(g, r):
        slot = g % XSLOTS
        return remote(xstage.at[slot, chips[r]], xin.at[g % RSLOTS, pl.ds(chip * 2, 2)],
                      back_s.at[slot, r], back_r.at[g, r], chips[r] * 2 + c)

    def tail_send(g, i, r):
        return remote(xbuf.at[i, pl.ds(peers[r] * rows, rows)], xin.at[g % RSLOTS, me, i],
                      tail_s.at[i, r], tail_r.at[i, r], peers[r])

    def sum_chunk(k):
        slot = k % SLOTS
        @pl.when(k % PAIR == 0)
        def _():
            for s in range(2):
                for i in range(3):
                    raw_arrival(k // PAIR, s, i).wait()

        for s in range(2):
            for i in range(3):
                raw_load(k, s, i).start()

        @pl.when(k >= SLOTS)
        def _():
            for s in range(2):
                part_copy(k - SLOTS, s).wait_send()

        for s in range(2):
            own_copy(k, s).wait()
            for i in range(3):
                raw_load(k, s, i).wait()
            keep = y if s == 0 else x

            @pl.loop(0, HALF)
            def _(m):
                def total(e):
                    v = [inbuf[s, i, m, e].astype(jnp.float32) for i in range(4)]
                    return (v[0] + v[1]) + (v[2] + v[3])

                part[slot, s, m] = total(1 - keep)
                kept[k % 2, s * HALF + m] = total(keep)

            part_copy(k, s).start()

        @pl.when(k + 1 < steps)
        def _():
            for s in range(2):
                own_copy(k + 1, s).start()
        w_load(k).start()

    def finish_chunk(k):
        slot = k % SLOTS
        g, i = k // GROUP, k % GROUP
        gslot = g % GSLOTS
        mom_load(k).wait()
        for s in range(2):
            part_copy(k, s).wait_recv()

        def momentum(j):
            new = MOMENTUM_COEF * momb[slot, j] + (kept[k % 2, j] + mom_out[k * CHUNK + j])
            mom_out[k * CHUNK + j] = new
            sq = jnp.sum(new * new, axis=0, keepdims=True)
            return new.astype(jnp.bfloat16), (sq[:, :128] + sq[:, 128:256]) + (sq[:, 256:384] + sq[:, 384:])

        @pl.loop(0, NDEV // 2)
        def _(q):
            stage[gslot, q, c, i], nstage[gslot, q, c, i] = momentum(2 * q + c)
            swap[q, i], nswap[q, i] = momentum(2 * q + 1 - c)

        @pl.when(i == GROUP - 1)
        def _():
            @pl.when(g >= 1)
            def _():
                for r in range(3):
                    own_send(g - 1, r).wait_send()
                    nrm_send(g - 1, r).wait_send()

            @pl.when(g >= XSLOTS)
            def _():
                for r in range(3):
                    back_send(g - XSLOTS, r).wait_send()

            for copy in swap_copies(g):
                copy.start()
            for copy in swap_copies(g):
                copy.wait()
            for r in range(3):
                own_send(g, r).start()
                nrm_send(g, r).start()

            @pl.loop(0, GROUP)
            def _(n):
                for core in range(2):
                    owned[g % OSLOTS, chip * 2 + core, n] = stage[gslot, chip, core, n]
                    owned_n[g, chip * 2 + core, n] = nstage[gslot, chip, core, n]

        @pl.when(k + 1 < steps)
        def _():
            mom_load(k + 1).start()

    def owned_arrival(g):
        for r in range(3):
            own_send(g, r).wait_recv()
            nrm_send(g, r).wait_recv()

    def orthogonalize(g, i):
        sq = owned_n[g, 0, i]
        for j in range(1, NDEV):
            sq = sq + owned_n[g, j, i]
        den = jnp.sqrt(jnp.sum(sq, axis=1, keepdims=True)) + NORM_EPS

        @pl.loop(0, NDEV)
        def _(j):
            blk = pl.ds(pl.multiple_of(j * rows, rows), rows)
            xbuf[i, blk] = (owned[g % OSLOTS, j, i].astype(jnp.float32) / den).astype(jnp.bfloat16)

        @pl.loop(0, NS_ITERS)
        def _(_):
            cur = xbuf[i]
            gram[...] = lax.dot_general(cur, cur, (((1,), (1,)), ((), ())),
                                        preferred_element_type=jnp.float32).astype(jnp.bfloat16)
            gm = gram[...]
            sqr = jnp.dot(gm, gm, preferred_element_type=jnp.float32)
            poly[...] = (COEF_B * gm.astype(jnp.float32) + COEF_C * sqr).astype(jnp.bfloat16)
            px = jnp.dot(poly[...], cur, preferred_element_type=jnp.float32)
            xbuf[i] = (COEF_A * cur.astype(jnp.float32) + px).astype(jnp.bfloat16)

    def split_rows(g, i):
        @pl.loop(0, NDEV // 2)
        def _(q):
            xstage[g % XSLOTS, q, c, i] = xbuf[i, pl.ds(pl.multiple_of((2 * q + c) * rows, rows), rows)]
            xswap[q, i] = xbuf[i, pl.ds(pl.multiple_of((2 * q + 1 - c) * rows, rows), rows)]

        @pl.when(i == GROUP - 1)
        def _():
            xswap_copy(g).start()

    def send_back(g):
        xswap_copy(g).wait()
        for r in range(3):
            back_send(g, r).start()

        @pl.loop(0, GROUP)
        def _(i):
            for core in range(2):
                xin[g % RSLOTS, chip * 2 + core, i] = xstage[g % XSLOTS, chip, core, i]

    def update_rows(g, i, j):
        m = (g * GROUP + i) * CHUNK + j
        old = w_out[m]
        step = xin[g % RSLOTS, j, i].astype(jnp.float32) * rms_scale
        w_out[m] = old - LEARN_RATE * (step + WEIGHT_DECAY * old)

    def update_weights(g):
        for i in range(GROUP):
            w_load(g * GROUP + i).wait()
        for r in range(4):
            if r < 3:
                back_send(g, r).wait_recv()

            @pl.loop(0, GROUP)
            def _(i):
                for core in range(2):
                    update_rows(g, i, (chips + [chip])[r] * 2 + core)

    def update_last(g):
        @pl.loop(0, GROUP)
        def _(i):
            w_load(g * GROUP + i).wait()
            update_rows(g, i, me)
            for r in range(NDEV - 1):
                pltpu.make_async_copy(xin.at[g % RSLOTS, peers[r], i], xin.at[g % RSLOTS, peers[r], i],
                                      tail_r.at[i, r]).wait()
                update_rows(g, i, peers[r])

    for q in range(AHEAD // PAIR):
        for copy in raw_copies(q):
            copy.start()
    for s in range(2):
        own_copy(0, s).start()
    mom_load(0).start()

    @pl.loop(0, steps)
    def _(t):
        @pl.when((t % PAIR == 0) & (t + AHEAD < steps))
        def _():
            for copy in raw_copies((t + AHEAD) // PAIR):
                copy.start()

        sum_chunk(t)

        def at(lag, work):
            @pl.when(((t - lag) % GROUP == 0) & (t >= lag + GROUP))
            def _():
                work((t - lag) // GROUP - 1)

        at(1 + GROUP, send_back)

        @pl.when(t >= 1)
        def _():
            finish_chunk(t - 1)

        at(1, owned_arrival)

        @pl.when(t >= 1 + GROUP)
        def _():
            g, i = (t - 1) // GROUP - 1, (t - 1) % GROUP
            orthogonalize(g, i)
            split_rows(g, i)

        at(3 + GROUP, update_weights)

    groups = steps // GROUP
    last = groups - 1
    finish_chunk(steps - 1)

    @pl.loop(GROUP - 1, 2 * GROUP)
    def _(n):
        @pl.when(n == GROUP)
        def _():
            send_back(last - 1)
            owned_arrival(last)

        orthogonalize(last - 1 + n // GROUP, n % GROUP)

        @pl.when(n == GROUP - 1)
        def _():
            split_rows(last - 1, n)

        @pl.when(n >= GROUP)
        def _():
            i = n - GROUP
            for r in range(NDEV - 1):
                tail_send(last, i, r).start()
            xin[last % RSLOTS, me, i] = xbuf[i, pl.ds(pl.multiple_of(me * rows, rows), rows)]

    @pl.loop(0, steps // PAIR)
    def _(q):
        for copy in raw_copies(q):
            copy.wait_send()

    @pl.loop(steps - SLOTS, steps)
    def _(k):
        for s in range(2):
            part_copy(k, s).wait_send()

    for r in range(3):
        own_send(last, r).wait_send()
        nrm_send(last, r).wait_send()

    @pl.loop((steps - 4 - GROUP) // GROUP, last)
    def _(g):
        update_weights(g)

    update_last(last)

    for g in range(groups - XSLOTS, last):
        for r in range(3):
            back_send(g, r).wait_send()
    for i in range(GROUP):
        for r in range(NDEV - 1):
            tail_send(last, i, r).wait_send()


def write_kernel(results, w_out, mom_out, sems):
    n = w_out.shape[0] // PIECES
    copies = []
    for i in range(PIECES):
        rng = pl.ds(i * n, n)
        copies.append(pltpu.make_async_copy(results.at[0, rng], w_out.at[rng], sems.at[0, i]))
        copies.append(pltpu.make_async_copy(results.at[1, rng], mom_out.at[rng], sems.at[1, i]))
    for copy in copies:
        copy.start()
    for copy in copies:
        copy.wait()


def solution(mesh):
    row_spec = P('stage', 'data', None)
    grad_spec = P(('stage', 'data'), None, None, None)

    def local_step(w_rows, mom_rows, grad_full):
        n_mats, rows, n_cols = w_rows.shape
        n_rows = rows * NDEV
        steps = n_mats // CHUNK
        groups = steps // GROUP
        grad_view = grad_full.reshape(steps, 2, HALF, 2, 2, 2, rows, n_cols)
        f32, bf16 = jnp.float32, jnp.bfloat16
        dma = pltpu.SemaphoreType.DMA
        hbm = pl.BlockSpec(memory_space=pltpu.HBM)
        vmem = pl.BlockSpec(memory_space=pltpu.VMEM)
        results, _ = pl.pallas_call(
            muon_kernel,
            name="muon_step",
            out_shape=(
                pltpu.VMEM((2, n_mats, rows, n_cols), f32),
                jax.ShapeDtypeStruct((steps // PAIR, 2, 3, PAIR, HALF, 2, rows, n_cols), bf16),
            ),
            in_specs=[hbm] * 3,
            out_specs=(vmem, hbm),
            scratch_shapes=[
                pltpu.VMEM((2, 4, HALF, 2, rows, n_cols), bf16),
                pltpu.VMEM((2, CHUNK, rows, n_cols), f32),
                pltpu.VMEM((SLOTS, 2, HALF, rows, n_cols), f32),
                pltpu.VMEM((SLOTS, CHUNK, rows, n_cols), f32),
                pltpu.VMEM((GSLOTS, NDEV // 2, 2, GROUP, rows, n_cols), bf16),
                pltpu.VMEM((NDEV // 2, GROUP, rows, n_cols), bf16),
                pltpu.VMEM((OSLOTS, NDEV, GROUP, rows, n_cols), bf16),
                pltpu.VMEM((GSLOTS, NDEV // 2, 2, GROUP, 1, 128), f32),
                pltpu.VMEM((NDEV // 2, GROUP, 1, 128), f32),
                pltpu.VMEM((groups, NDEV, GROUP, 1, 128), f32),
                pltpu.VMEM((GROUP, n_rows, n_cols), bf16),
                pltpu.VMEM((NDEV // 2, GROUP, rows, n_cols), bf16),
                pltpu.VMEM((XSLOTS, NDEV // 2, 2, GROUP, rows, n_cols), bf16),
                pltpu.VMEM((RSLOTS, NDEV, GROUP, rows, n_cols), bf16),
                pltpu.VMEM((n_rows, n_rows), bf16),
                pltpu.VMEM((n_rows, n_rows), bf16),
                dma((steps // PAIR, 2, 3)), dma((steps // PAIR, 2, 3)),
                dma((SLOTS, 2)), dma((steps, 2)),
                dma((2,)), dma((groups, 2)),
                dma((GSLOTS, 3)), dma((groups, 3)),
                dma((GSLOTS, 3)), dma((groups, 3)),
                dma((1,)), dma((groups,)),
                dma((XSLOTS, 3)), dma((groups, 3)),
                dma((GROUP, NDEV)), dma((GROUP, NDEV)),
                dma((2, 4)), dma((SLOTS,)), dma((steps,)),
            ],
            compiler_params=pltpu.CompilerParams(
                collective_id=0, has_side_effects=True, vmem_limit_bytes=31 * 2 ** 20),
        )(grad_view, mom_rows, w_rows)
        return pl.pallas_call(
            write_kernel,
            name="write_results",
            out_shape=(jax.ShapeDtypeStruct(w_rows.shape, f32), jax.ShapeDtypeStruct(w_rows.shape, f32)),
            in_specs=[vmem],
            out_specs=(hbm, hbm),
            scratch_shapes=[dma((2, PIECES))],
            compiler_params=pltpu.CompilerParams(vmem_limit_bytes=2 ** 20),
        )(results)

    return jax.shard_map(local_step, mesh=mesh, in_specs=(row_spec, row_spec, grad_spec),
                         out_specs=(row_spec, row_spec), check_vma=False)
```

```python
import functools
import math

import jax
import jax.numpy as jnp
from jax import lax
from jax.experimental import pallas as pl
from jax.experimental.pallas import tpu as pltpu
from jax.sharding import PartitionSpec as P

MOMENTUM_COEF = 0.95
LEARN_RATE = 0.05
WEIGHT_DECAY = 0.2
NORM_EPS = 1e-7
COEF_A = 3.4445
COEF_B = -4.7750
COEF_C = 2.0315
NS_ITERS = 5

NDEV = 8
CHUNK = 8
HALF = 4
PAIR = 4
AHEAD = 4
SLOTS = 3
GROUP = 2
GSLOTS = 2
OSLOTS = 4
XSLOTS = 3
RSLOTS = 4
PIECES = 4
MESH = pl.DeviceIdType.MESH


def muon_kernel(
    grad, mom, w, results, raw,
    inbuf, kept, part, momb, stage, swap, owned, nstage, nswap, owned_n, xbuf, xswap, xstage, xin, gram, poly,
    raw_s, raw_r, part_s, part_r, swap_s, swap_r, own_s, own_r, nrm_s, nrm_r, xswap_s, xswap_r, back_s, back_r, tail_s, tail_r, lswap_s, lswap_r, lown_s, lown_r, lnrm_s, lnrm_r,
    in_sem, mom_in, w_in,
):
    n_mats, rows, cols = mom.shape
    rms_scale = 0.2 * math.sqrt(max(rows * NDEV, cols))
    w_out, mom_out = results.at[0], results.at[1]
    steps = n_mats // CHUNK
    me = lax.axis_index("data")
    y, x, c = me // 4, (me // 2) % 2, me % 2
    partner = y * 4 + x * 2 + (1 - c)
    x_nbr = y * 4 + (1 - x) * 2
    y_nbr = (1 - y) * 4 + x * 2
    diagonal = (1 - y) * 4 + (1 - x) * 2
    peers = [base + core for base in (diagonal, x_nbr, y_nbr) for core in (c, 1 - c)] + [partner]

    chip = me // 2
    chips = [base // 2 for base in (diagonal, x_nbr, y_nbr)]

    def remote(src, dst, send, recv, dev):
        return pltpu.make_async_remote_copy(
            src_ref=src, dst_ref=dst, send_sem=send, recv_sem=recv,
            device_id={"data": dev}, device_id_type=MESH)

    barrier = pltpu.get_barrier_semaphore()
    for peer in peers:
        pl.semaphore_signal(barrier, inc=1, device_id={"data": peer}, device_id_type=MESH)
    pl.semaphore_wait(barrier, NDEV - 1)

    def raw_copies(q):
        rng = pl.ds(q * PAIR, PAIR)
        out = []
        for dc in range(2):
            out.append(remote(grad.at[rng, 0, :, :, 1 - x, dc], raw.at[q, 0, 1 + c],
                              raw_s.at[q, 0, 1 + dc], raw_r.at[q, 0, 1 + c], x_nbr + dc))
            out.append(remote(grad.at[rng, 1, :, 1 - y, :, dc], raw.at[q, 1, 1 + c],
                              raw_s.at[q, 1, 1 + dc], raw_r.at[q, 1, 1 + c], y_nbr + dc))
        out.append(remote(grad.at[rng, 0, :, :, x, 1 - c], raw.at[q, 0, 0], raw_s.at[q, 0, 0], raw_r.at[q, 0, 0], partner))
        out.append(remote(grad.at[rng, 1, :, y, :, 1 - c], raw.at[q, 1, 0], raw_s.at[q, 1, 0], raw_r.at[q, 1, 0], partner))
        return out

    def raw_arrival(q, s, i):
        return pltpu.make_async_copy(raw.at[q, s, i], raw.at[q, s, i], raw_r.at[q, s, i])

    def own_copy(k, s):
        src = grad.at[k, 0, :, :, x, c] if s == 0 else grad.at[k, 1, :, y, :, c]
        return pltpu.make_async_copy(src, inbuf.at[s, 0], in_sem.at[s, 0])

    def raw_load(k, s, i):
        return pltpu.make_async_copy(raw.at[k // PAIR, s, i, k % PAIR], inbuf.at[s, 1 + i], in_sem.at[s, 1 + i])

    def part_copy(k, s):
        slot = k % SLOTS
        return remote(part.at[slot, s], mom_out.at[pl.ds(k * CHUNK + s * HALF, HALF)],
                      part_s.at[slot, s], part_r.at[k, s], (y_nbr if s == 0 else x_nbr) + c)

    def mom_load(k):
        return pltpu.make_async_copy(mom.at[pl.ds(k * CHUNK, CHUNK)], momb.at[k % SLOTS], mom_in.at[k % SLOTS])

    def w_load(k):
        rng = pl.ds(k * CHUNK, CHUNK)
        return pltpu.make_async_copy(w.at[rng], w_out.at[rng], w_in.at[k])

    def swap_copies(g):
        slot = g % GSLOTS
        return [remote(swap, stage.at[slot, :, c], swap_s.at[0], swap_r.at[g, 0], partner),
                remote(nswap, nstage.at[slot, :, c], swap_s.at[1], swap_r.at[g, 1], partner)]

    def own_send(g, r):
        slot = g % GSLOTS
        return remote(stage.at[slot, chips[r]], owned.at[g % OSLOTS, pl.ds(chip * 2, 2)],
                      own_s.at[slot, r], own_r.at[g, r], chips[r] * 2 + c)

    def nrm_send(g, r):
        slot = g % GSLOTS
        return remote(nstage.at[slot, chips[r]], owned_n.at[g, pl.ds(chip * 2, 2)],
                      nrm_s.at[slot, r], nrm_r.at[g, r], chips[r] * 2 + c)

    final = steps // GROUP - 1
    fslot = final % GSLOTS

    def last_swap(i):
        return [remote(swap.at[:, i], stage.at[fslot, :, c, i], lswap_s.at[i, 0], lswap_r.at[i, 0], partner),
                remote(nswap.at[:, i], nstage.at[fslot, :, c, i], lswap_s.at[i, 1], lswap_r.at[i, 1], partner)]

    def last_send(i, r):
        dev = chips[r] * 2 + c
        return [remote(stage.at[fslot, chips[r], :, i], owned.at[final % OSLOTS, pl.ds(chip * 2, 2), i],
                       lown_s.at[i, r], lown_r.at[i, r], dev),
                remote(nstage.at[fslot, chips[r], :, i], owned_n.at[final, pl.ds(chip * 2, 2), i],
                       lnrm_s.at[i, r], lnrm_r.at[i, r], dev)]

    def xswap_copy(g):
        return remote(xswap, xstage.at[g % XSLOTS, :, c], xswap_s.at[0], xswap_r.at[g], partner)

    def back_send(g, r):
        slot = g % XSLOTS
        return remote(xstage.at[slot, chips[r]], xin.at[g % RSLOTS, pl.ds(chip * 2, 2)],
                      back_s.at[slot, r], back_r.at[g, r], chips[r] * 2 + c)

    def tail_send(g, i, r):
        return remote(xbuf.at[i, pl.ds(peers[r] * rows, rows)], xin.at[g % RSLOTS, me, i],
                      tail_s.at[i, r], tail_r.at[i, r], peers[r])

    def sum_chunk(k):
        slot = k % SLOTS
        @pl.when(k % PAIR == 0)
        def _():
            for s in range(2):
                for i in range(3):
                    raw_arrival(k // PAIR, s, i).wait()

        for s in range(2):
            for i in range(3):
                raw_load(k, s, i).start()

        @pl.when(k >= SLOTS)
        def _():
            for s in range(2):
                part_copy(k - SLOTS, s).wait_send()

        for s in range(2):
            own_copy(k, s).wait()
            for i in range(3):
                raw_load(k, s, i).wait()
            keep = y if s == 0 else x

            @pl.loop(0, HALF)
            def _(m):
                def total(e):
                    v = [inbuf[s, i, m, e].astype(jnp.float32) for i in range(4)]
                    return (v[0] + v[1]) + (v[2] + v[3])

                part[slot, s, m] = total(1 - keep)
                kept[k % 2, s * HALF + m] = total(keep)

            part_copy(k, s).start()

        @pl.when(k + 1 < steps)
        def _():
            for s in range(2):
                own_copy(k + 1, s).start()
        w_load(k).start()

    def finish_chunk(k):
        slot = k % SLOTS
        g, i = k // GROUP, k % GROUP
        gslot = g % GSLOTS
        mom_load(k).wait()
        for s in range(2):
            part_copy(k, s).wait_recv()

        def momentum(j):
            new = MOMENTUM_COEF * momb[slot, j] + (kept[k % 2, j] + mom_out[k * CHUNK + j])
            mom_out[k * CHUNK + j] = new
            sq = jnp.sum(new * new, axis=0, keepdims=True)
            return new.astype(jnp.bfloat16), (sq[:, :128] + sq[:, 128:256]) + (sq[:, 256:384] + sq[:, 384:])

        @pl.loop(0, NDEV // 2)
        def _(q):
            stage[gslot, q, c, i], nstage[gslot, q, c, i] = momentum(2 * q + c)
            swap[q, i], nswap[q, i] = momentum(2 * q + 1 - c)

        def keep_rows(n):
            for core in range(2):
                owned[g % OSLOTS, chip * 2 + core, n] = stage[gslot, chip, core, n]
                owned_n[g, chip * 2 + core, n] = nstage[gslot, chip, core, n]

        @pl.when(g == final)
        def _():
            for copy in last_swap(i):
                copy.start()
            for copy in last_swap(i):
                copy.wait()
            for r in range(3):
                for copy in last_send(i, r):
                    copy.start()
            keep_rows(i)

        @pl.when((i == GROUP - 1) & (g < final))
        def _():
            @pl.when(g >= 1)
            def _():
                for r in range(3):
                    own_send(g - 1, r).wait_send()
                    nrm_send(g - 1, r).wait_send()

            @pl.when(g >= XSLOTS)
            def _():
                for r in range(3):
                    back_send(g - XSLOTS, r).wait_send()

            for copy in swap_copies(g):
                copy.start()
            for copy in swap_copies(g):
                copy.wait()
            for r in range(3):
                own_send(g, r).start()
                nrm_send(g, r).start()

            @pl.loop(0, GROUP)
            def _(n):
                keep_rows(n)

        @pl.when(k + 1 < steps)
        def _():
            mom_load(k + 1).start()

    def owned_arrival(g):
        for r in range(3):
            own_send(g, r).wait_recv()
            nrm_send(g, r).wait_recv()

    def orthogonalize(g, i):
        sq = owned_n[g, 0, i]
        for j in range(1, NDEV):
            sq = sq + owned_n[g, j, i]
        den = jnp.sqrt(jnp.sum(sq, axis=1, keepdims=True)) + NORM_EPS

        @pl.loop(0, NDEV)
        def _(j):
            blk = pl.ds(pl.multiple_of(j * rows, rows), rows)
            xbuf[i, blk] = (owned[g % OSLOTS, j, i].astype(jnp.float32) / den).astype(jnp.bfloat16)

        @pl.loop(0, NS_ITERS)
        def _(_):
            cur = xbuf[i]
            gram[...] = lax.dot_general(cur, cur, (((1,), (1,)), ((), ())),
                                        preferred_element_type=jnp.float32).astype(jnp.bfloat16)
            gm = gram[...]
            sqr = jnp.dot(gm, gm, preferred_element_type=jnp.float32)
            poly[...] = (COEF_B * gm.astype(jnp.float32) + COEF_C * sqr).astype(jnp.bfloat16)
            px = jnp.dot(poly[...], cur, preferred_element_type=jnp.float32)
            xbuf[i] = (COEF_A * cur.astype(jnp.float32) + px).astype(jnp.bfloat16)

    def split_rows(g, i):
        @pl.loop(0, NDEV // 2)
        def _(q):
            xstage[g % XSLOTS, q, c, i] = xbuf[i, pl.ds(pl.multiple_of((2 * q + c) * rows, rows), rows)]
            xswap[q, i] = xbuf[i, pl.ds(pl.multiple_of((2 * q + 1 - c) * rows, rows), rows)]

        @pl.when(i == GROUP - 1)
        def _():
            xswap_copy(g).start()

    def send_back(g):
        xswap_copy(g).wait()
        for r in range(3):
            back_send(g, r).start()

        @pl.loop(0, GROUP)
        def _(i):
            for core in range(2):
                xin[g % RSLOTS, chip * 2 + core, i] = xstage[g % XSLOTS, chip, core, i]

    def update_rows(g, i, j):
        m = (g * GROUP + i) * CHUNK + j
        old = w_out[m]
        step = xin[g % RSLOTS, j, i].astype(jnp.float32) * rms_scale
        w_out[m] = old - LEARN_RATE * (step + WEIGHT_DECAY * old)

    def update_weights(g):
        for i in range(GROUP):
            w_load(g * GROUP + i).wait()
        for r in range(4):
            if r < 3:
                back_send(g, r).wait_recv()

            @pl.loop(0, GROUP)
            def _(i):
                for core in range(2):
                    update_rows(g, i, (chips + [chip])[r] * 2 + core)

    def update_last(g):
        @pl.loop(0, GROUP)
        def _(i):
            w_load(g * GROUP + i).wait()
            update_rows(g, i, me)
            for r in range(NDEV - 1):
                pltpu.make_async_copy(xin.at[g % RSLOTS, peers[r], i], xin.at[g % RSLOTS, peers[r], i],
                                      tail_r.at[i, r]).wait()
                update_rows(g, i, peers[r])

    for q in range(AHEAD // PAIR):
        for copy in raw_copies(q):
            copy.start()
    for s in range(2):
        own_copy(0, s).start()
    mom_load(0).start()

    @pl.loop(0, steps)
    def _(t):
        @pl.when((t % PAIR == 0) & (t + AHEAD < steps))
        def _():
            for copy in raw_copies((t + AHEAD) // PAIR):
                copy.start()

        sum_chunk(t)

        def at(lag, work):
            @pl.when(((t - lag) % GROUP == 0) & (t >= lag + GROUP))
            def _():
                work((t - lag) // GROUP - 1)

        at(1 + GROUP, send_back)

        @pl.when(t >= 1)
        def _():
            finish_chunk(t - 1)

        at(1, owned_arrival)

        @pl.when(t >= 1 + GROUP)
        def _():
            g, i = (t - 1) // GROUP - 1, (t - 1) % GROUP
            orthogonalize(g, i)
            split_rows(g, i)

        at(3 + GROUP, update_weights)

    groups = steps // GROUP
    last = groups - 1
    finish_chunk(steps - 1)

    @pl.loop(GROUP - 1, 2 * GROUP)
    def _(n):
        @pl.when(n == GROUP)
        def _():
            send_back(last - 1)

        @pl.when(n >= GROUP)
        def _():
            for r in range(3):
                for copy in last_send(n - GROUP, r):
                    copy.wait_recv()

        orthogonalize(last - 1 + n // GROUP, n % GROUP)

        @pl.when(n == GROUP - 1)
        def _():
            split_rows(last - 1, n)

        @pl.when(n >= GROUP)
        def _():
            i = n - GROUP
            for r in range(NDEV - 1):
                tail_send(last, i, r).start()
            xin[last % RSLOTS, me, i] = xbuf[i, pl.ds(pl.multiple_of(me * rows, rows), rows)]

    @pl.loop(0, steps // PAIR)
    def _(q):
        for copy in raw_copies(q):
            copy.wait_send()

    @pl.loop(steps - SLOTS, steps)
    def _(k):
        for s in range(2):
            part_copy(k, s).wait_send()

    for r in range(3):
        own_send(last - 1, r).wait_send()
        nrm_send(last - 1, r).wait_send()
        for i in range(GROUP):
            for copy in last_send(i, r):
                copy.wait_send()

    @pl.loop((steps - 4 - GROUP) // GROUP, last)
    def _(g):
        update_weights(g)

    update_last(last)

    for g in range(last - XSLOTS, last):
        for r in range(3):
            back_send(g, r).wait_send()
    for i in range(GROUP):
        for r in range(NDEV - 1):
            tail_send(last, i, r).wait_send()


def write_kernel(results, w_out, mom_out, sems):
    n = w_out.shape[0] // PIECES
    copies = []
    for i in range(PIECES):
        rng = pl.ds(i * n, n)
        copies.append(pltpu.make_async_copy(results.at[0, rng], w_out.at[rng], sems.at[0, i]))
        copies.append(pltpu.make_async_copy(results.at[1, rng], mom_out.at[rng], sems.at[1, i]))
    for copy in copies:
        copy.start()
    for copy in copies:
        copy.wait()


def solution(mesh):
    row_spec = P('stage', 'data', None)
    grad_spec = P(('stage', 'data'), None, None, None)

    def local_step(w_rows, mom_rows, grad_full):
        n_mats, rows, n_cols = w_rows.shape
        n_rows = rows * NDEV
        steps = n_mats // CHUNK
        groups = steps // GROUP
        grad_view = grad_full.reshape(steps, 2, HALF, 2, 2, 2, rows, n_cols)
        f32, bf16 = jnp.float32, jnp.bfloat16
        dma = pltpu.SemaphoreType.DMA
        hbm = pl.BlockSpec(memory_space=pltpu.HBM)
        vmem = pl.BlockSpec(memory_space=pltpu.VMEM)
        results, _ = pl.pallas_call(
            muon_kernel,
            name="muon_step",
            out_shape=(
                pltpu.VMEM((2, n_mats, rows, n_cols), f32),
                jax.ShapeDtypeStruct((steps // PAIR, 2, 3, PAIR, HALF, 2, rows, n_cols), bf16),
            ),
            in_specs=[hbm] * 3,
            out_specs=(vmem, hbm),
            scratch_shapes=[
                pltpu.VMEM((2, 4, HALF, 2, rows, n_cols), bf16),
                pltpu.VMEM((2, CHUNK, rows, n_cols), f32),
                pltpu.VMEM((SLOTS, 2, HALF, rows, n_cols), f32),
                pltpu.VMEM((SLOTS, CHUNK, rows, n_cols), f32),
                pltpu.VMEM((GSLOTS, NDEV // 2, 2, GROUP, rows, n_cols), bf16),
                pltpu.VMEM((NDEV // 2, GROUP, rows, n_cols), bf16),
                pltpu.VMEM((OSLOTS, NDEV, GROUP, rows, n_cols), bf16),
                pltpu.VMEM((GSLOTS, NDEV // 2, 2, GROUP, 1, 128), f32),
                pltpu.VMEM((NDEV // 2, GROUP, 1, 128), f32),
                pltpu.VMEM((groups, NDEV, GROUP, 1, 128), f32),
                pltpu.VMEM((GROUP, n_rows, n_cols), bf16),
                pltpu.VMEM((NDEV // 2, GROUP, rows, n_cols), bf16),
                pltpu.VMEM((XSLOTS, NDEV // 2, 2, GROUP, rows, n_cols), bf16),
                pltpu.VMEM((RSLOTS, NDEV, GROUP, rows, n_cols), bf16),
                pltpu.VMEM((n_rows, n_rows), bf16),
                pltpu.VMEM((n_rows, n_rows), bf16),
                dma((steps // PAIR, 2, 3)), dma((steps // PAIR, 2, 3)),
                dma((SLOTS, 2)), dma((steps, 2)),
                dma((2,)), dma((groups, 2)),
                dma((GSLOTS, 3)), dma((groups, 3)),
                dma((GSLOTS, 3)), dma((groups, 3)),
                dma((1,)), dma((groups,)),
                dma((XSLOTS, 3)), dma((groups, 3)),
                dma((GROUP, NDEV)), dma((GROUP, NDEV)),
                *[dma((GROUP, 3))] * 6,
                dma((2, 4)), dma((SLOTS,)), dma((steps,)),
            ],
            compiler_params=pltpu.CompilerParams(
                collective_id=0, has_side_effects=True, vmem_limit_bytes=31 * 2 ** 20),
        )(grad_view, mom_rows, w_rows)
        return pl.pallas_call(
            write_kernel,
            name="write_results",
            out_shape=(jax.ShapeDtypeStruct(w_rows.shape, f32), jax.ShapeDtypeStruct(w_rows.shape, f32)),
            in_specs=[vmem],
            out_specs=(hbm, hbm),
            scratch_shapes=[dma((2, PIECES))],
            compiler_params=pltpu.CompilerParams(vmem_limit_bytes=2 ** 20),
        )(results)

    return jax.shard_map(local_step, mesh=mesh, in_specs=(row_spec, row_spec, grad_spec),
                         out_specs=(row_spec, row_spec), check_vma=False)
```

```python
import functools
import math

import jax
import jax.numpy as jnp
from jax import lax
from jax.experimental import pallas as pl
from jax.experimental.pallas import tpu as pltpu
from jax.sharding import PartitionSpec as P

MOMENTUM_COEF = 0.95
LEARN_RATE = 0.05
WEIGHT_DECAY = 0.2
NORM_EPS = 1e-7
COEF_A = 3.4445
COEF_B = -4.7750
COEF_C = 2.0315
NS_ITERS = 5

NDEV = 8
CHUNK = 8
HALF = 4
PAIR = 4
AHEAD = 4
SLOTS = 3
GROUP = 2
GSLOTS = 2
OSLOTS = 3
XSLOTS = 3
RSLOTS = 3
PIECES = 4
MESH = pl.DeviceIdType.MESH


def muon_kernel(
    grad, mom, w, results, raw,
    inbuf, kept, part, momb, stage, swap, owned, nstage, nswap, owned_n, xbuf, xswap, xstage, xin, gram, poly,
    raw_s, raw_r, part_s, part_r, swap_s, swap_r, own_s, own_r, nrm_s, nrm_r, xswap_s, xswap_r, back_s, back_r, tail_s, tail_r,
    in_sem, mom_in, w_in,
):
    n_mats, rows, cols = mom.shape
    rms_scale = 0.2 * math.sqrt(max(rows * NDEV, cols))
    w_out, mom_out = results.at[0], results.at[1]
    steps = n_mats // CHUNK
    me = lax.axis_index("data")
    y, x, c = me // 4, (me // 2) % 2, me % 2
    partner = y * 4 + x * 2 + (1 - c)
    x_nbr = y * 4 + (1 - x) * 2
    y_nbr = (1 - y) * 4 + x * 2
    diagonal = (1 - y) * 4 + (1 - x) * 2
    peers = [base + core for base in (diagonal, x_nbr, y_nbr) for core in (c, 1 - c)] + [partner]

    chip = me // 2
    chips = [base // 2 for base in (diagonal, x_nbr, y_nbr)]

    def remote(src, dst, send, recv, dev):
        return pltpu.make_async_remote_copy(
            src_ref=src, dst_ref=dst, send_sem=send, recv_sem=recv,
            device_id={"data": dev}, device_id_type=MESH)

    barrier = pltpu.get_barrier_semaphore()
    for peer in peers:
        pl.semaphore_signal(barrier, inc=1, device_id={"data": peer}, device_id_type=MESH)
    pl.semaphore_wait(barrier, NDEV - 1)

    def raw_copies(q):
        rng = pl.ds(q * PAIR, PAIR)
        out = []
        for dc in range(2):
            out.append(remote(grad.at[rng, 0, :, :, 1 - x, dc], raw.at[q, 0, 1 + c],
                              raw_s.at[q, 0, 1 + dc], raw_r.at[q, 0, 1 + c], x_nbr + dc))
            out.append(remote(grad.at[rng, 1, :, 1 - y, :, dc], raw.at[q, 1, 1 + c],
                              raw_s.at[q, 1, 1 + dc], raw_r.at[q, 1, 1 + c], y_nbr + dc))
        out.append(remote(grad.at[rng, 0, :, :, x, 1 - c], raw.at[q, 0, 0], raw_s.at[q, 0, 0], raw_r.at[q, 0, 0], partner))
        out.append(remote(grad.at[rng, 1, :, y, :, 1 - c], raw.at[q, 1, 0], raw_s.at[q, 1, 0], raw_r.at[q, 1, 0], partner))
        return out

    def raw_arrival(q, s, i):
        return pltpu.make_async_copy(raw.at[q, s, i], raw.at[q, s, i], raw_r.at[q, s, i])

    def own_copy(k, s):
        src = grad.at[k, 0, :, :, x, c] if s == 0 else grad.at[k, 1, :, y, :, c]
        return pltpu.make_async_copy(src, inbuf.at[s, 0], in_sem.at[s, 0])

    def raw_load(k, s, i):
        return pltpu.make_async_copy(raw.at[k // PAIR, s, i, k % PAIR], inbuf.at[s, 1 + i], in_sem.at[s, 1 + i])

    def part_copy(k, s):
        slot = k % SLOTS
        return remote(part.at[slot, s], mom_out.at[pl.ds(k * CHUNK + s * HALF, HALF)],
                      part_s.at[slot, s], part_r.at[k, s], (y_nbr if s == 0 else x_nbr) + c)

    def mom_load(k):
        return pltpu.make_async_copy(mom.at[pl.ds(k * CHUNK, CHUNK)], momb.at[k % SLOTS], mom_in.at[k % SLOTS])

    def w_load(k):
        rng = pl.ds(k * CHUNK, CHUNK)
        return pltpu.make_async_copy(w.at[rng], w_out.at[rng], w_in.at[k])

    def swap_copies(g):
        slot = g % GSLOTS
        return [remote(swap, stage.at[slot, :, c], swap_s.at[0], swap_r.at[g, 0], partner),
                remote(nswap, nstage.at[slot, :, c], swap_s.at[1], swap_r.at[g, 1], partner)]

    def own_send(g, r):
        slot = g % GSLOTS
        return remote(stage.at[slot, chips[r]], owned.at[g % OSLOTS, pl.ds(chip * 2, 2)],
                      own_s.at[slot, r], own_r.at[g, r], chips[r] * 2 + c)

    def nrm_send(g, r):
        slot = g % GSLOTS
        return remote(nstage.at[slot, chips[r]], owned_n.at[g, pl.ds(chip * 2, 2)],
                      nrm_s.at[slot, r], nrm_r.at[g, r], chips[r] * 2 + c)

    def xswap_copy(g):
        return remote(xswap, xstage.at[g % XSLOTS, :, c], xswap_s.at[0], xswap_r.at[g], partner)

    def back_send(g, r):
        slot = g % XSLOTS
        return remote(xstage.at[slot, chips[r]], xin.at[g % RSLOTS, pl.ds(chip * 2, 2)],
                      back_s.at[slot, r], back_r.at[g, r], chips[r] * 2 + c)

    def tail_send(g, i, r):
        return remote(xbuf.at[i, pl.ds(peers[r] * rows, rows)], xin.at[g % RSLOTS, me, i],
                      tail_s.at[i, r], tail_r.at[i, r], peers[r])

    def sum_chunk(k):
        slot = k % SLOTS
        @pl.when(k % PAIR == 0)
        def _():
            for s in range(2):
                for i in range(3):
                    raw_arrival(k // PAIR, s, i).wait()

        for s in range(2):
            for i in range(3):
                raw_load(k, s, i).start()

        @pl.when(k >= SLOTS)
        def _():
            for s in range(2):
                part_copy(k - SLOTS, s).wait_send()

        for s in range(2):
            own_copy(k, s).wait()
            for i in range(3):
                raw_load(k, s, i).wait()
            keep = y if s == 0 else x

            @pl.loop(0, HALF)
            def _(m):
                def total(e):
                    v = [inbuf[s, i, m, e].astype(jnp.float32) for i in range(4)]
                    return (v[0] + v[1]) + (v[2] + v[3])

                part[slot, s, m] = total(1 - keep)
                kept[k % 2, s * HALF + m] = total(keep)

            part_copy(k, s).start()

        @pl.when(k + 1 < steps)
        def _():
            for s in range(2):
                own_copy(k + 1, s).start()
        w_load(k).start()

    def finish_chunk(k):
        slot = k % SLOTS
        g, i = k // GROUP, k % GROUP
        gslot = g % GSLOTS
        mom_load(k).wait()
        for s in range(2):
            part_copy(k, s).wait_recv()

        def momentum(j):
            new = MOMENTUM_COEF * momb[slot, j] + (kept[k % 2, j] + mom_out[k * CHUNK + j])
            mom_out[k * CHUNK + j] = new
            sq = jnp.sum(new * new, axis=0, keepdims=True)
            return new.astype(jnp.bfloat16), (sq[:, :128] + sq[:, 128:256]) + (sq[:, 256:384] + sq[:, 384:])

        @pl.loop(0, NDEV // 2)
        def _(q):
            stage[gslot, q, c, i], nstage[gslot, q, c, i] = momentum(2 * q + c)
            swap[q, i], nswap[q, i] = momentum(2 * q + 1 - c)

        @pl.when(i == GROUP - 1)
        def _():
            @pl.when(g >= 1)
            def _():
                for r in range(3):
                    own_send(g - 1, r).wait_send()
                    nrm_send(g - 1, r).wait_send()

            @pl.when(g >= XSLOTS)
            def _():
                for r in range(3):
                    back_send(g - XSLOTS, r).wait_send()

            for copy in swap_copies(g):
                copy.start()
            for copy in swap_copies(g):
                copy.wait()
            for r in range(3):
                own_send(g, r).start()
                nrm_send(g, r).start()

            @pl.loop(0, GROUP)
            def _(n):
                for core in range(2):
                    owned[g % OSLOTS, chip * 2 + core, n] = stage[gslot, chip, core, n]
                    owned_n[g, chip * 2 + core, n] = nstage[gslot, chip, core, n]

        @pl.when(k + 1 < steps)
        def _():
            mom_load(k + 1).start()

    def owned_arrival(g):
        for r in range(3):
            own_send(g, r).wait_recv()
            nrm_send(g, r).wait_recv()

    def orthogonalize(g, i):
        sq = owned_n[g, 0, i]
        for j in range(1, NDEV):
            sq = sq + owned_n[g, j, i]
        den = jnp.sqrt(jnp.sum(sq, axis=1, keepdims=True)) + NORM_EPS

        @pl.loop(0, NDEV)
        def _(j):
            blk = pl.ds(pl.multiple_of(j * rows, rows), rows)
            xbuf[i, blk] = (owned[g % OSLOTS, j, i].astype(jnp.float32) / den).astype(jnp.bfloat16)

        @pl.loop(0, NS_ITERS)
        def _(_):
            cur = xbuf[i]
            gram[...] = lax.dot_general(cur, cur, (((1,), (1,)), ((), ())),
                                        preferred_element_type=jnp.float32).astype(jnp.bfloat16)
            gm = gram[...]
            sqr = jnp.dot(gm, gm, preferred_element_type=jnp.float32)
            poly[...] = (COEF_B * gm.astype(jnp.float32) + COEF_C * sqr).astype(jnp.bfloat16)
            px = jnp.dot(poly[...], cur, preferred_element_type=jnp.float32)
            xbuf[i] = (COEF_A * cur.astype(jnp.float32) + px).astype(jnp.bfloat16)

    def split_rows(g, i):
        @pl.loop(0, NDEV // 2)
        def _(q):
            xstage[g % XSLOTS, q, c, i] = xbuf[i, pl.ds(pl.multiple_of((2 * q + c) * rows, rows), rows)]
            xswap[q, i] = xbuf[i, pl.ds(pl.multiple_of((2 * q + 1 - c) * rows, rows), rows)]

        @pl.when(i == GROUP - 1)
        def _():
            xswap_copy(g).start()

    def send_back(g):
        xswap_copy(g).wait()
        for r in range(3):
            back_send(g, r).start()

        @pl.loop(0, GROUP)
        def _(i):
            for core in range(2):
                xin[g % RSLOTS, chip * 2 + core, i] = xstage[g % XSLOTS, chip, core, i]

    def update_rows(g, i, j):
        m = (g * GROUP + i) * CHUNK + j
        old = w_out[m]
        step = xin[g % RSLOTS, j, i].astype(jnp.float32) * rms_scale
        w_out[m] = old - LEARN_RATE * (step + WEIGHT_DECAY * old)

    def update_weights(g):
        for i in range(GROUP):
            w_load(g * GROUP + i).wait()
        for r in range(4):
            if r < 3:
                back_send(g, r).wait_recv()

            @pl.loop(0, GROUP)
            def _(i):
                for core in range(2):
                    update_rows(g, i, (chips + [chip])[r] * 2 + core)

    def update_last(g):
        @pl.loop(0, GROUP)
        def _(i):
            w_load(g * GROUP + i).wait()
            update_rows(g, i, me)
            for r in range(NDEV - 1):
                pltpu.make_async_copy(xin.at[g % RSLOTS, peers[r], i], xin.at[g % RSLOTS, peers[r], i],
                                      tail_r.at[i, r]).wait()
                update_rows(g, i, peers[r])

    for q in range(AHEAD // PAIR):
        for copy in raw_copies(q):
            copy.start()
    for s in range(2):
        own_copy(0, s).start()
    mom_load(0).start()

    @pl.loop(0, steps)
    def _(t):
        def next_raw(core):
            @pl.when((t % PAIR == 0) & (t + AHEAD < steps) & (c == core))
            def _():
                for copy in raw_copies((t + AHEAD) // PAIR):
                    copy.start()

        next_raw(0)
        sum_chunk(t)
        next_raw(1)

        def at(lag, work):
            @pl.when(((t - lag) % GROUP == 0) & (t >= lag + GROUP))
            def _():
                work((t - lag) // GROUP - 1)

        at(1 + GROUP, send_back)

        @pl.when(t >= 1)
        def _():
            finish_chunk(t - 1)

        at(1, owned_arrival)

        @pl.when(t >= 1 + GROUP)
        def _():
            g, i = (t - 1) // GROUP - 1, (t - 1) % GROUP
            orthogonalize(g, i)
            split_rows(g, i)

        at(3 + GROUP, update_weights)

    groups = steps // GROUP
    last = groups - 1
    finish_chunk(steps - 1)

    @pl.loop(GROUP - 1, 2 * GROUP)
    def _(n):
        @pl.when(n == GROUP)
        def _():
            send_back(last - 1)
            owned_arrival(last)

        orthogonalize(last - 1 + n // GROUP, n % GROUP)

        @pl.when(n == GROUP - 1)
        def _():
            split_rows(last - 1, n)

        @pl.when(n >= GROUP)
        def _():
            i = n - GROUP
            for r in range(NDEV - 1):
                tail_send(last, i, r).start()
            xin[last % RSLOTS, me, i] = xbuf[i, pl.ds(pl.multiple_of(me * rows, rows), rows)]

    @pl.loop(0, steps // PAIR)
    def _(q):
        for copy in raw_copies(q):
            copy.wait_send()

    @pl.loop(steps - SLOTS, steps)
    def _(k):
        for s in range(2):
            part_copy(k, s).wait_send()

    for r in range(3):
        own_send(last, r).wait_send()
        nrm_send(last, r).wait_send()

    @pl.loop((steps - 4 - GROUP) // GROUP, last)
    def _(g):
        update_weights(g)

    update_last(last)

    for g in range(groups - XSLOTS, last):
        for r in range(3):
            back_send(g, r).wait_send()
    for i in range(GROUP):
        for r in range(NDEV - 1):
            tail_send(last, i, r).wait_send()


def write_kernel(results, w_out, mom_out, sems):
    n = w_out.shape[0] // PIECES
    copies = []
    for i in range(PIECES):
        rng = pl.ds(i * n, n)
        copies.append(pltpu.make_async_copy(results.at[0, rng], w_out.at[rng], sems.at[0, i]))
        copies.append(pltpu.make_async_copy(results.at[1, rng], mom_out.at[rng], sems.at[1, i]))
    for copy in copies:
        copy.start()
    for copy in copies:
        copy.wait()


def solution(mesh):
    row_spec = P('stage', 'data', None)
    grad_spec = P(('stage', 'data'), None, None, None)

    def local_step(w_rows, mom_rows, grad_full):
        n_mats, rows, n_cols = w_rows.shape
        n_rows = rows * NDEV
        steps = n_mats // CHUNK
        groups = steps // GROUP
        grad_view = grad_full.reshape(steps, 2, HALF, 2, 2, 2, rows, n_cols)
        f32, bf16 = jnp.float32, jnp.bfloat16
        dma = pltpu.SemaphoreType.DMA
        hbm = pl.BlockSpec(memory_space=pltpu.HBM)
        vmem = pl.BlockSpec(memory_space=pltpu.VMEM)
        results, _ = pl.pallas_call(
            muon_kernel,
            name="muon_step",
            out_shape=(
                pltpu.VMEM((2, n_mats, rows, n_cols), f32),
                jax.ShapeDtypeStruct((steps // PAIR, 2, 3, PAIR, HALF, 2, rows, n_cols), bf16),
            ),
            in_specs=[hbm] * 3,
            out_specs=(vmem, hbm),
            scratch_shapes=[
                pltpu.VMEM((2, 4, HALF, 2, rows, n_cols), bf16),
                pltpu.VMEM((2, CHUNK, rows, n_cols), f32),
                pltpu.VMEM((SLOTS, 2, HALF, rows, n_cols), f32),
                pltpu.VMEM((SLOTS, CHUNK, rows, n_cols), f32),
                pltpu.VMEM((GSLOTS, NDEV // 2, 2, GROUP, rows, n_cols), bf16),
                pltpu.VMEM((NDEV // 2, GROUP, rows, n_cols), bf16),
                pltpu.VMEM((OSLOTS, NDEV, GROUP, rows, n_cols), bf16),
                pltpu.VMEM((GSLOTS, NDEV // 2, 2, GROUP, 1, 128), f32),
                pltpu.VMEM((NDEV // 2, GROUP, 1, 128), f32),
                pltpu.VMEM((groups, NDEV, GROUP, 1, 128), f32),
                pltpu.VMEM((GROUP, n_rows, n_cols), bf16),
                pltpu.VMEM((NDEV // 2, GROUP, rows, n_cols), bf16),
                pltpu.VMEM((XSLOTS, NDEV // 2, 2, GROUP, rows, n_cols), bf16),
                pltpu.VMEM((RSLOTS, NDEV, GROUP, rows, n_cols), bf16),
                pltpu.VMEM((n_rows, n_rows), bf16),
                pltpu.VMEM((n_rows, n_rows), bf16),
                dma((steps // PAIR, 2, 3)), dma((steps // PAIR, 2, 3)),
                dma((SLOTS, 2)), dma((steps, 2)),
                dma((2,)), dma((groups, 2)),
                dma((GSLOTS, 3)), dma((groups, 3)),
                dma((GSLOTS, 3)), dma((groups, 3)),
                dma((1,)), dma((groups,)),
                dma((XSLOTS, 3)), dma((groups, 3)),
                dma((GROUP, NDEV)), dma((GROUP, NDEV)),
                dma((2, 4)), dma((SLOTS,)), dma((steps,)),
            ],
            compiler_params=pltpu.CompilerParams(
                collective_id=0, has_side_effects=True, vmem_limit_bytes=31 * 2 ** 20),
        )(grad_view, mom_rows, w_rows)
        return pl.pallas_call(
            write_kernel,
            name="write_results",
            out_shape=(jax.ShapeDtypeStruct(w_rows.shape, f32), jax.ShapeDtypeStruct(w_rows.shape, f32)),
            in_specs=[vmem],
            out_specs=(hbm, hbm),
            scratch_shapes=[dma((2, PIECES))],
            compiler_params=pltpu.CompilerParams(vmem_limit_bytes=2 ** 20),
        )(results)

    return jax.shard_map(local_step, mesh=mesh, in_specs=(row_spec, row_spec, grad_spec),
                         out_specs=(row_spec, row_spec), check_vma=False)
```

```python
import functools
import math

import jax
import jax.numpy as jnp
from jax import lax
from jax.experimental import pallas as pl
from jax.experimental.pallas import tpu as pltpu
from jax.sharding import PartitionSpec as P

MOMENTUM_COEF = 0.95
LEARN_RATE = 0.05
WEIGHT_DECAY = 0.2
NORM_EPS = 1e-7
COEF_A = 3.4445
COEF_B = -4.7750
COEF_C = 2.0315
NS_ITERS = 5

NDEV = 8
CHUNK = 8
HALF = 4
PAIR = 4
AHEAD = 4
SLOTS = 3
GROUP = 2
GSLOTS = 2
OSLOTS = 3
XSLOTS = 3
RSLOTS = 3
PIECES = 2
MESH = pl.DeviceIdType.MESH


def muon_kernel(
    grad, mom, w, results, raw,
    inbuf, kept, part, momb, stage, swap, owned, nstage, nswap, owned_n, xbuf, xswap, xstage, xin, gram, poly,
    raw_s, raw_r, part_s, part_r, swap_s, swap_r, own_s, own_r, nrm_s, nrm_r, xswap_s, xswap_r, back_s, back_r, tail_s, tail_r,
    in_sem, mom_in, w_in,
):
    n_mats, rows, cols = mom.shape
    rms_scale = 0.2 * math.sqrt(max(rows * NDEV, cols))
    w_out, mom_out = results.at[0], results.at[1]
    steps = n_mats // CHUNK
    me = lax.axis_index("data")
    y, x, c = me // 4, (me // 2) % 2, me % 2
    partner = y * 4 + x * 2 + (1 - c)
    x_nbr = y * 4 + (1 - x) * 2
    y_nbr = (1 - y) * 4 + x * 2
    diagonal = (1 - y) * 4 + (1 - x) * 2
    peers = [base + core for base in (diagonal, x_nbr, y_nbr) for core in (c, 1 - c)] + [partner]

    chip = me // 2
    chips = [base // 2 for base in (diagonal, x_nbr, y_nbr)]

    def remote(src, dst, send, recv, dev):
        return pltpu.make_async_remote_copy(
            src_ref=src, dst_ref=dst, send_sem=send, recv_sem=recv,
            device_id={"data": dev}, device_id_type=MESH)

    barrier = pltpu.get_barrier_semaphore()
    for peer in peers:
        pl.semaphore_signal(barrier, inc=1, device_id={"data": peer}, device_id_type=MESH)
    pl.semaphore_wait(barrier, NDEV - 1)

    def raw_copies(q):
        rng = pl.ds(q * PAIR, PAIR)
        out = []
        for dc in range(2):
            out.append(remote(grad.at[rng, 0, :, :, 1 - x, dc], raw.at[q, 0, 1 + c],
                              raw_s.at[q, 0, 1 + dc], raw_r.at[q, 0, 1 + c], x_nbr + dc))
            out.append(remote(grad.at[rng, 1, :, 1 - y, :, dc], raw.at[q, 1, 1 + c],
                              raw_s.at[q, 1, 1 + dc], raw_r.at[q, 1, 1 + c], y_nbr + dc))
        out.append(remote(grad.at[rng, 0, :, :, x, 1 - c], raw.at[q, 0, 0], raw_s.at[q, 0, 0], raw_r.at[q, 0, 0], partner))
        out.append(remote(grad.at[rng, 1, :, y, :, 1 - c], raw.at[q, 1, 0], raw_s.at[q, 1, 0], raw_r.at[q, 1, 0], partner))
        return out

    def raw_arrival(q, s, i):
        return pltpu.make_async_copy(raw.at[q, s, i], raw.at[q, s, i], raw_r.at[q, s, i])

    def own_copy(k, s):
        src = grad.at[k, 0, :, :, x, c] if s == 0 else grad.at[k, 1, :, y, :, c]
        return pltpu.make_async_copy(src, inbuf.at[s, 0], in_sem.at[s, 0])

    def raw_load(k, s, i):
        return pltpu.make_async_copy(raw.at[k // PAIR, s, i, k % PAIR], inbuf.at[s, 1 + i], in_sem.at[s, 1 + i])

    def part_copy(k, s):
        slot = k % SLOTS
        return remote(part.at[slot, s], mom_out.at[pl.ds(k * CHUNK + s * HALF, HALF)],
                      part_s.at[slot, s], part_r.at[k, s], (y_nbr if s == 0 else x_nbr) + c)

    def mom_load(k):
        return pltpu.make_async_copy(mom.at[pl.ds(k * CHUNK, CHUNK)], momb.at[k % SLOTS], mom_in.at[k % SLOTS])

    def w_load(k):
        rng = pl.ds(k * CHUNK, CHUNK)
        return pltpu.make_async_copy(w.at[rng], w_out.at[rng], w_in.at[k])

    def swap_copies(g):
        slot = g % GSLOTS
        return [remote(swap, stage.at[slot, :, c], swap_s.at[0], swap_r.at[g, 0], partner),
                remote(nswap, nstage.at[slot, :, c], swap_s.at[1], swap_r.at[g, 1], partner)]

    def own_send(g, r):
        slot = g % GSLOTS
        return remote(stage.at[slot, chips[r]], owned.at[g % OSLOTS, pl.ds(chip * 2, 2)],
                      own_s.at[slot, r], own_r.at[g, r], chips[r] * 2 + c)

    def nrm_send(g, r):
        slot = g % GSLOTS
        return remote(nstage.at[slot, chips[r]], owned_n.at[g, pl.ds(chip * 2, 2)],
                      nrm_s.at[slot, r], nrm_r.at[g, r], chips[r] * 2 + c)

    def xswap_copy(g):
        return remote(xswap, xstage.at[g % XSLOTS, :, c], xswap_s.at[0], xswap_r.at[g], partner)

    def back_send(g, r):
        slot = g % XSLOTS
        return remote(xstage.at[slot, chips[r]], xin.at[g % RSLOTS, pl.ds(chip * 2, 2)],
                      back_s.at[slot, r], back_r.at[g, r], chips[r] * 2 + c)

    def tail_send(g, i, r):
        return remote(xbuf.at[i, pl.ds(peers[r] * rows, rows)], xin.at[g % RSLOTS, me, i],
                      tail_s.at[i, r], tail_r.at[i, r], peers[r])

    def sum_chunk(k):
        slot = k % SLOTS
        @pl.when(k % PAIR == 0)
        def _():
            for s in range(2):
                for i in range(3):
                    raw_arrival(k // PAIR, s, i).wait()

        for s in range(2):
            for i in range(3):
                raw_load(k, s, i).start()

        @pl.when(k >= SLOTS)
        def _():
            for s in range(2):
                part_copy(k - SLOTS, s).wait_send()

        for s in range(2):
            own_copy(k, s).wait()
            for i in range(3):
                raw_load(k, s, i).wait()
            keep = y if s == 0 else x

            @pl.loop(0, HALF)
            def _(m):
                def total(e):
                    v = [inbuf[s, i, m, e].astype(jnp.float32) for i in range(4)]
                    return (v[0] + v[1]) + (v[2] + v[3])

                part[slot, s, m] = total(1 - keep)
                kept[k % 2, s * HALF + m] = total(keep)

            part_copy(k, s).start()

        @pl.when(k + 1 < steps)
        def _():
            for s in range(2):
                own_copy(k + 1, s).start()
        w_load(k).start()

    def finish_chunk(k):
        slot = k % SLOTS
        g, i = k // GROUP, k % GROUP
        gslot = g % GSLOTS
        mom_load(k).wait()
        for s in range(2):
            part_copy(k, s).wait_recv()

        def momentum(j):
            new = MOMENTUM_COEF * momb[slot, j] + (kept[k % 2, j] + mom_out[k * CHUNK + j])
            mom_out[k * CHUNK + j] = new
            sq = jnp.sum(new * new, axis=0, keepdims=True)
            return new.astype(jnp.bfloat16), (sq[:, :128] + sq[:, 128:256]) + (sq[:, 256:384] + sq[:, 384:])

        @pl.loop(0, NDEV // 2)
        def _(q):
            stage[gslot, q, c, i], nstage[gslot, q, c, i] = momentum(2 * q + c)
            swap[q, i], nswap[q, i] = momentum(2 * q + 1 - c)

        @pl.when(i == GROUP - 1)
        def _():
            @pl.when(g >= 1)
            def _():
                for r in range(3):
                    own_send(g - 1, r).wait_send()
                    nrm_send(g - 1, r).wait_send()

            @pl.when(g >= XSLOTS)
            def _():
                for r in range(3):
                    back_send(g - XSLOTS, r).wait_send()

            for copy in swap_copies(g):
                copy.start()
            for copy in swap_copies(g):
                copy.wait()
            for r in range(3):
                own_send(g, r).start()
                nrm_send(g, r).start()

            @pl.loop(0, GROUP)
            def _(n):
                for core in range(2):
                    owned[g % OSLOTS, chip * 2 + core, n] = stage[gslot, chip, core, n]
                    owned_n[g, chip * 2 + core, n] = nstage[gslot, chip, core, n]

        @pl.when(k + 1 < steps)
        def _():
            mom_load(k + 1).start()

    def owned_arrival(g):
        for r in range(3):
            own_send(g, r).wait_recv()
            nrm_send(g, r).wait_recv()

    def orthogonalize(g, i):
        sq = owned_n[g, 0, i]
        for j in range(1, NDEV):
            sq = sq + owned_n[g, j, i]
        den = jnp.sqrt(jnp.sum(sq, axis=1, keepdims=True)) + NORM_EPS

        @pl.loop(0, NDEV)
        def _(j):
            blk = pl.ds(pl.multiple_of(j * rows, rows), rows)
            xbuf[i, blk] = (owned[g % OSLOTS, j, i].astype(jnp.float32) / den).astype(jnp.bfloat16)

        @pl.loop(0, NS_ITERS)
        def _(_):
            cur = xbuf[i]
            gram[...] = lax.dot_general(cur, cur, (((1,), (1,)), ((), ())),
                                        preferred_element_type=jnp.float32).astype(jnp.bfloat16)
            gm = gram[...]
            sqr = jnp.dot(gm, gm, preferred_element_type=jnp.float32)
            poly[...] = (COEF_B * gm.astype(jnp.float32) + COEF_C * sqr).astype(jnp.bfloat16)
            px = jnp.dot(poly[...], cur, preferred_element_type=jnp.float32)
            xbuf[i] = (COEF_A * cur.astype(jnp.float32) + px).astype(jnp.bfloat16)

    def split_rows(g, i):
        @pl.loop(0, NDEV // 2)
        def _(q):
            xstage[g % XSLOTS, q, c, i] = xbuf[i, pl.ds(pl.multiple_of((2 * q + c) * rows, rows), rows)]
            xswap[q, i] = xbuf[i, pl.ds(pl.multiple_of((2 * q + 1 - c) * rows, rows), rows)]

        @pl.when(i == GROUP - 1)
        def _():
            xswap_copy(g).start()

    def send_back(g):
        xswap_copy(g).wait()
        for r in range(3):
            back_send(g, r).start()

        @pl.loop(0, GROUP)
        def _(i):
            for core in range(2):
                xin[g % RSLOTS, chip * 2 + core, i] = xstage[g % XSLOTS, chip, core, i]

    def update_rows(g, i, j):
        m = (g * GROUP + i) * CHUNK + j
        old = w_out[m]
        step = xin[g % RSLOTS, j, i].astype(jnp.float32) * rms_scale
        w_out[m] = old - LEARN_RATE * (step + WEIGHT_DECAY * old)

    def update_weights(g):
        for i in range(GROUP):
            w_load(g * GROUP + i).wait()
        for r in range(4):
            if r < 3:
                back_send(g, r).wait_recv()

            @pl.loop(0, GROUP)
            def _(i):
                for core in range(2):
                    update_rows(g, i, (chips + [chip])[r] * 2 + core)

    def update_last(g):
        @pl.loop(0, GROUP)
        def _(i):
            w_load(g * GROUP + i).wait()
            update_rows(g, i, me)
            for r in range(NDEV - 1):
                pltpu.make_async_copy(xin.at[g % RSLOTS, peers[r], i], xin.at[g % RSLOTS, peers[r], i],
                                      tail_r.at[i, r]).wait()
                update_rows(g, i, peers[r])

    for q in range(AHEAD // PAIR):
        for copy in raw_copies(q):
            copy.start()
    for s in range(2):
        own_copy(0, s).start()
    mom_load(0).start()

    @pl.loop(0, steps)
    def _(t):
        @pl.when((t % PAIR == 0) & (t + AHEAD < steps))
        def _():
            for copy in raw_copies((t + AHEAD) // PAIR):
                copy.start()

        sum_chunk(t)

        def at(lag, work):
            @pl.when(((t - lag) % GROUP == 0) & (t >= lag + GROUP))
            def _():
                work((t - lag) // GROUP - 1)

        at(1 + GROUP, send_back)

        @pl.when(t >= 1)
        def _():
            finish_chunk(t - 1)

        at(1, owned_arrival)

        @pl.when(t >= 1 + GROUP)
        def _():
            g, i = (t - 1) // GROUP - 1, (t - 1) % GROUP
            orthogonalize(g, i)
            split_rows(g, i)

        at(3 + GROUP, update_weights)

    groups = steps // GROUP
    last = groups - 1
    finish_chunk(steps - 1)

    @pl.loop(GROUP - 1, 2 * GROUP)
    def _(n):
        @pl.when(n == GROUP)
        def _():
            send_back(last - 1)
            owned_arrival(last)

        orthogonalize(last - 1 + n // GROUP, n % GROUP)

        @pl.when(n == GROUP - 1)
        def _():
            split_rows(last - 1, n)

        @pl.when(n >= GROUP)
        def _():
            i = n - GROUP
            for r in range(NDEV - 1):
                tail_send(last, i, r).start()
            xin[last % RSLOTS, me, i] = xbuf[i, pl.ds(pl.multiple_of(me * rows, rows), rows)]

    @pl.loop(0, steps // PAIR)
    def _(q):
        for copy in raw_copies(q):
            copy.wait_send()

    @pl.loop(steps - SLOTS, steps)
    def _(k):
        for s in range(2):
            part_copy(k, s).wait_send()

    for r in range(3):
        own_send(last, r).wait_send()
        nrm_send(last, r).wait_send()

    @pl.loop((steps - 4 - GROUP) // GROUP, last)
    def _(g):
        update_weights(g)

    update_last(last)

    for g in range(groups - XSLOTS, last):
        for r in range(3):
            back_send(g, r).wait_send()
    for i in range(GROUP):
        for r in range(NDEV - 1):
            tail_send(last, i, r).wait_send()


def write_kernel(results, w_out, mom_out, sems):
    n = w_out.shape[0] // PIECES
    copies = []
    for i in range(PIECES):
        rng = pl.ds(i * n, n)
        copies.append(pltpu.make_async_copy(results.at[0, rng], w_out.at[rng], sems.at[0, i]))
        copies.append(pltpu.make_async_copy(results.at[1, rng], mom_out.at[rng], sems.at[1, i]))
    for copy in copies:
        copy.start()
    for copy in copies:
        copy.wait()


def solution(mesh):
    row_spec = P('stage', 'data', None)
    grad_spec = P(('stage', 'data'), None, None, None)

    def local_step(w_rows, mom_rows, grad_full):
        n_mats, rows, n_cols = w_rows.shape
        n_rows = rows * NDEV
        steps = n_mats // CHUNK
        groups = steps // GROUP
        grad_view = grad_full.reshape(steps, 2, HALF, 2, 2, 2, rows, n_cols)
        f32, bf16 = jnp.float32, jnp.bfloat16
        dma = pltpu.SemaphoreType.DMA
        hbm = pl.BlockSpec(memory_space=pltpu.HBM)
        vmem = pl.BlockSpec(memory_space=pltpu.VMEM)
        results, _ = pl.pallas_call(
            muon_kernel,
            name="muon_step",
            out_shape=(
                pltpu.VMEM((2, n_mats, rows, n_cols), f32),
                jax.ShapeDtypeStruct((steps // PAIR, 2, 3, PAIR, HALF, 2, rows, n_cols), bf16),
            ),
            in_specs=[hbm] * 3,
            out_specs=(vmem, hbm),
            scratch_shapes=[
                pltpu.VMEM((2, 4, HALF, 2, rows, n_cols), bf16),
                pltpu.VMEM((2, CHUNK, rows, n_cols), f32),
                pltpu.VMEM((SLOTS, 2, HALF, rows, n_cols), f32),
                pltpu.VMEM((SLOTS, CHUNK, rows, n_cols), f32),
                pltpu.VMEM((GSLOTS, NDEV // 2, 2, GROUP, rows, n_cols), bf16),
                pltpu.VMEM((NDEV // 2, GROUP, rows, n_cols), bf16),
                pltpu.VMEM((OSLOTS, NDEV, GROUP, rows, n_cols), bf16),
                pltpu.VMEM((GSLOTS, NDEV // 2, 2, GROUP, 1, 128), f32),
                pltpu.VMEM((NDEV // 2, GROUP, 1, 128), f32),
                pltpu.VMEM((groups, NDEV, GROUP, 1, 128), f32),
                pltpu.VMEM((GROUP, n_rows, n_cols), bf16),
                pltpu.VMEM((NDEV // 2, GROUP, rows, n_cols), bf16),
                pltpu.VMEM((XSLOTS, NDEV // 2, 2, GROUP, rows, n_cols), bf16),
                pltpu.VMEM((RSLOTS, NDEV, GROUP, rows, n_cols), bf16),
                pltpu.VMEM((n_rows, n_rows), bf16),
                pltpu.VMEM((n_rows, n_rows), bf16),
                dma((steps // PAIR, 2, 3)), dma((steps // PAIR, 2, 3)),
                dma((SLOTS, 2)), dma((steps, 2)),
                dma((2,)), dma((groups, 2)),
                dma((GSLOTS, 3)), dma((groups, 3)),
                dma((GSLOTS, 3)), dma((groups, 3)),
                dma((1,)), dma((groups,)),
                dma((XSLOTS, 3)), dma((groups, 3)),
                dma((GROUP, NDEV)), dma((GROUP, NDEV)),
                dma((2, 4)), dma((SLOTS,)), dma((steps,)),
            ],
            compiler_params=pltpu.CompilerParams(
                collective_id=0, has_side_effects=True, vmem_limit_bytes=31 * 2 ** 20),
        )(grad_view, mom_rows, w_rows)
        return pl.pallas_call(
            write_kernel,
            name="write_results",
            out_shape=(jax.ShapeDtypeStruct(w_rows.shape, f32), jax.ShapeDtypeStruct(w_rows.shape, f32)),
            in_specs=[vmem],
            out_specs=(hbm, hbm),
            scratch_shapes=[dma((2, PIECES))],
            compiler_params=pltpu.CompilerParams(vmem_limit_bytes=2 ** 20),
        )(results)

    return jax.shard_map(local_step, mesh=mesh, in_specs=(row_spec, row_spec, grad_spec),
                         out_specs=(row_spec, row_spec), check_vma=False)
```
